8 devices in a mesh: dp: 1 (over z), ep: 8 (over y, x, core).
Axes of the slice: x: 2, y: 2, z: 1, core: 2. Of those that a mesh axis runs over, the one named last changes fastest.
Arguments:
- x: bfloat16 [768, 2048], P(('dp', 'ep'))
- route_idx: int32 [768, 6], P(('dp', 'ep'))
- gates: float32 [768, 6], P(('dp', 'ep'))
- w_gate: bfloat16 [64, 2048, 1408], P('ep')
- w_up: bfloat16 [64, 2048, 1408], P('ep')
- w_down: bfloat16 [64, 1408, 2048], P('ep')
- shared_gate: bfloat16 [2048, 2816], replicated
- shared_up: bfloat16 [2048, 2816], replicated
- shared_down: bfloat16 [2816, 2048], replicated
Outputs:
- output: bfloat16 [768, 2048], P(('dp', 'ep'))
All inputs are finite; a program needn't handle non-finite values.
Results may differ from the reference program's by a relative error of at most 0.00804522.
Values are sent between devices in bfloat16 or wider.
A program may use at most 1 GiB of HBM per device.

```python
import jax
import jax.numpy as jnp
from jax import lax

D_MODEL = 2048
EXPERTS = 64
TOP_K = 6
EXPERT_FF = 1408
SHARED_FF = 2816
TOKENS_DEV = 96
GROUP_SIZE = 8
CAPACITY = 36
HOT_EXPERTS = 4
ROW_BLOCK = 64

TOKENS = GROUP_SIZE * TOKENS_DEV
PAIRS = TOKENS * TOP_K
NUM_BLOCKS = PAIRS // ROW_BLOCK + EXPERTS + 1
GATE_SCALE = (2.0 / TOP_K) ** 0.5


def cold_order(order_key):
    return jax.random.permutation(order_key, EXPERTS - HOT_EXPERTS).astype(jnp.int32)


def expert_counts(count_key):
    perm_key, weight_key, order_key = jax.random.split(count_key, 3)
    cold_num = EXPERTS - HOT_EXPERTS
    cold_total = TOKENS_DEV * TOP_K - HOT_EXPERTS * CAPACITY
    weights = jax.random.randint(weight_key, (GROUP_SIZE, cold_num), 1, 3, jnp.int32)
    cold = 1 + (cold_total - cold_num) * weights // jnp.sum(weights, axis=1, keepdims=True)
    leftover = cold_total - jnp.sum(cold, axis=1, keepdims=True)
    orders = jax.vmap(cold_order)(jax.random.split(order_key, GROUP_SIZE))
    cold = cold + (orders < leftover).astype(jnp.int32)
    hot = jnp.full((GROUP_SIZE, HOT_EXPERTS), CAPACITY, jnp.int32)
    by_rank = jnp.concatenate([hot, cold], axis=1).astype(jnp.int32)
    expert_perm = jax.random.permutation(perm_key, EXPERTS)
    return jnp.zeros((GROUP_SIZE, EXPERTS), jnp.int32).at[:, expert_perm].set(by_rank)


def device_routes(dev_key, dev_counts):
    tok_key, roll_key = jax.random.split(dev_key)
    count_ends = jnp.cumsum(dev_counts)
    slot_pos = jnp.arange(TOKENS_DEV * TOP_K, dtype=jnp.int32)
    labels = jnp.sum((count_ends[None, :] <= slot_pos[:, None]).astype(jnp.int32), axis=1)
    slot_table = labels.reshape(TOP_K, TOKENS_DEV).T
    slot_table = slot_table[jax.random.permutation(tok_key, TOKENS_DEV)]
    slot_shift = jax.random.randint(roll_key, (TOKENS_DEV, 1), 0, TOP_K, jnp.int32)
    slot_cols = (jnp.arange(TOP_K, dtype=jnp.int32)[None, :] + slot_shift) % TOP_K
    return jnp.take_along_axis(slot_table, slot_cols, axis=1)


def setup_inputs(seed: int = 0, part: int = 0) -> dict:
    shared_key, part_base = jax.random.split(jax.random.key(seed))
    part_key = jax.random.fold_in(part_base, part)
    count_key, dev_key, x_key, gate_key = jax.random.split(part_key, 4)
    counts = expert_counts(count_key)
    routes = jax.vmap(device_routes)(jax.random.split(dev_key, GROUP_SIZE), counts)
    route_idx = routes.reshape(TOKENS, TOP_K).astype(jnp.int32)
    x = jax.random.normal(x_key, (TOKENS, D_MODEL), jnp.float32).astype(jnp.bfloat16)
    gates = jax.random.uniform(gate_key, (TOKENS, TOP_K), jnp.float32, 0.3, 0.7) * GATE_SCALE
    weight_keys = jax.random.split(shared_key, 6)
    w_gate = (jax.random.normal(weight_keys[0], (EXPERTS, D_MODEL, EXPERT_FF), jnp.float32) * D_MODEL ** -0.5).astype(jnp.bfloat16)
    w_up = (jax.random.normal(weight_keys[1], (EXPERTS, D_MODEL, EXPERT_FF), jnp.float32) * D_MODEL ** -0.5).astype(jnp.bfloat16)
    w_down = (jax.random.normal(weight_keys[2], (EXPERTS, EXPERT_FF, D_MODEL), jnp.float32) * EXPERT_FF ** -0.5).astype(jnp.bfloat16)
    shared_gate = (jax.random.normal(weight_keys[3], (D_MODEL, SHARED_FF), jnp.float32) * D_MODEL ** -0.5).astype(jnp.bfloat16)
    shared_up = (jax.random.normal(weight_keys[4], (D_MODEL, SHARED_FF), jnp.float32) * D_MODEL ** -0.5).astype(jnp.bfloat16)
    shared_down = (jax.random.normal(weight_keys[5], (SHARED_FF, D_MODEL), jnp.float32) * SHARED_FF ** -0.5).astype(jnp.bfloat16)
    return {'x': x, 'route_idx': route_idx, 'gates': gates, 'w_gate': w_gate, 'w_up': w_up, 'w_down': w_down, 'shared_gate': shared_gate, 'shared_up': shared_up, 'shared_down': shared_down}


def swiglu(rows, gate_mat, up_mat, down_mat):
    act_a = jnp.dot(rows, gate_mat, preferred_element_type=jnp.float32)
    act_b = jnp.dot(rows, up_mat, preferred_element_type=jnp.float32)
    hidden = (jax.nn.silu(act_a) * act_b).astype(jnp.bfloat16)
    return jnp.dot(hidden, down_mat, preferred_element_type=jnp.float32).astype(jnp.bfloat16)


def reference(x, route_idx, gates, w_gate, w_up, w_down, shared_gate, shared_up, shared_down):
    flat_exp = route_idx.reshape(PAIRS)
    counts = jnp.zeros(EXPERTS, jnp.int32).at[flat_exp].add(1)
    padded = (counts + ROW_BLOCK - 1) // ROW_BLOCK * ROW_BLOCK
    pad_start = jnp.cumsum(padded) - padded
    raw_start = jnp.cumsum(counts) - counts
    sort_order = jnp.argsort(flat_exp, stable=True)
    sorted_exp = flat_exp[sort_order]
    dest_row = pad_start[sorted_exp] + jnp.arange(PAIRS) - raw_start[sorted_exp]
    row_tok = jnp.zeros(NUM_BLOCKS * ROW_BLOCK, jnp.int32).at[dest_row].set((sort_order // TOP_K).astype(jnp.int32))
    row_gate = jnp.zeros(NUM_BLOCKS * ROW_BLOCK, jnp.float32).at[dest_row].set(gates.reshape(PAIRS)[sort_order])
    pad_end = pad_start + padded
    block_first = jnp.arange(NUM_BLOCKS) * ROW_BLOCK
    block_exp = jnp.minimum(jnp.sum((pad_end[None, :] <= block_first[:, None]).astype(jnp.int32), axis=1), EXPERTS - 1)

    def block_step(running, block_data):
        tok_ids, gate_w, exp_id = block_data
        expert_out = swiglu(x[tok_ids], w_gate[exp_id], w_up[exp_id], w_down[exp_id])
        return running.at[tok_ids].add(gate_w[:, None] * expert_out.astype(jnp.float32)), None

    routed, _ = lax.scan(block_step, jnp.zeros((TOKENS, D_MODEL), jnp.float32), (row_tok.reshape(NUM_BLOCKS, ROW_BLOCK), row_gate.reshape(NUM_BLOCKS, ROW_BLOCK), block_exp))
    shared_out = swiglu(x, shared_gate, shared_up, shared_down)
    return (shared_out.astype(jnp.float32) + routed).astype(jnp.bfloat16)
```

```python
import functools

import jax
import jax.numpy as jnp
from jax import lax
from jax.experimental import pallas as pl
from jax.experimental.pallas import tpu as pltpu
from jax.sharding import PartitionSpec as P

MESH = pl.DeviceIdType.MESH
CAP = 36
SLOT = 40
VMEM_LIMIT = 67_000_000
BF16 = jnp.bfloat16
F32 = jnp.float32


def neighbours():
    me = lax.axis_index("ep")
    core = me % 2
    xb = (me // 2) % 2
    yb = me // 4
    sib = me + 1 - 2 * core
    xn = me + 2 - 4 * xb
    yn = me + 4 - 8 * yb
    dg = yn + 2 - 4 * xb
    return me, core, sib, xn, yn, dg


def rcopy(src, dst, send, recv, dev):
    return pltpu.make_async_remote_copy(
        src_ref=src, dst_ref=dst, send_sem=send, recv_sem=recv,
        device_id={"ep": dev}, device_id_type=MESH)


def gather_kernel(x_ref, route_ref, gate_ref, sg_hbm, su_hbm,
                  xall_hbm, hsh_ref, meta_all, cnt_ref, g_ref,
                  land, meta_s, bg, bu, metal,
                  wsem, osem, sx_s, sx_r, sy_s, sy_r, f_s, f_r, ss_s, ss_r, m_s, m_r):
    me, core, sib, xn, yn, dg = neighbours()
    nd = xall_hbm.shape[0]
    rows = x_ref.shape[0]
    half = rows // 2
    n_chunks = bg.shape[0]
    width = bg.shape[2]

    barrier = pltpu.get_barrier_semaphore()
    for r in range(1, nd):
        pl.semaphore_signal(barrier, inc=1, device_id={"ep": (me + r) % nd}, device_id_type=MESH)

    def wcopy(i):
        cols = pl.ds(pl.multiple_of(i * width, width), width)
        return (pltpu.make_async_copy(sg_hbm.at[:, cols], bg.at[i], wsem.at[0, i]),
                pltpu.make_async_copy(su_hbm.at[:, cols], bu.at[i], wsem.at[1, i]))

    for i in range(n_chunks):
        for c in wcopy(i):
            c.start()

    def hs(h):
        return pl.ds(h * half, half)

    own_out = pltpu.make_async_copy(x_ref, xall_hbm.at[me], osem.at[0])
    own_out.start()

    pl.semaphore_wait(barrier, nd - 1)
    own_x = [rcopy(x_ref.at[hs(h)], land.at[me, hs(h)], sx_s.at[h], sx_r.at[h], xn) for h in range(2)]
    own_y = [rcopy(x_ref.at[hs(h)], land.at[me, hs(h)], sy_s.at[h], sy_r.at[h], yn) for h in range(2)]
    own_s = rcopy(x_ref, land.at[me], ss_s.at[0], ss_r.at[0], sib)
    own_x[0].start()
    own_y[1].start()
    own_x[1].start()
    own_y[0].start()
    own_s.start()

    ids = lax.broadcasted_iota(jnp.int32, (rows, 128), 1)
    mask = jnp.zeros((rows, 128), F32)
    gmap = jnp.zeros((rows, 128), F32)
    for k in range(route_ref.shape[1]):
        eq = route_ref[:, k:k + 1] == ids
        mask = mask + jnp.where(eq, 1.0, 0.0)
        gmap = gmap + jnp.where(eq, gate_ref[:, k:k + 1], 0.0)
    lower = (lax.broadcasted_iota(jnp.int32, (rows, rows), 0)
             > lax.broadcasted_iota(jnp.int32, (rows, rows), 1))
    rank = jnp.dot(jnp.where(lower, 1.0, 0.0).astype(BF16), mask.astype(BF16), preferred_element_type=F32)
    rank = jnp.where(mask > 0.0, rank, -1.0)
    count = jnp.broadcast_to(jnp.sum(mask, axis=0, keepdims=True), (8, 128))
    rank_t = jnp.concatenate([rank, jnp.full((128 - rows, 128), -1.0, F32)], axis=0).T
    gate_t = jnp.concatenate([gmap, jnp.zeros((128 - rows, 128), F32)], axis=0).T
    for j in range(nd):
        meta_s[j, 0:8, :] = rank_t[8 * j:8 * j + 8]
        meta_s[j, 8:16, :] = gate_t[8 * j:8 * j + 8]
        meta_s[j, 16:24, :] = count
    metal[me] = meta_s[me]

    def shared_chunk(i):
        for c in wcopy(i):
            c.wait()
        a = jnp.dot(x_ref[...], bg[i], preferred_element_type=F32)
        b = jnp.dot(x_ref[...], bu[i], preferred_element_type=F32)
        cols = pl.ds(pl.multiple_of(i * width, width), width)
        hsh_ref[:, cols] = (jax.nn.silu(a) * b).astype(BF16)

    def shared_range(lo, hi):
        def body(i, carry):
            shared_chunk(i)
            return carry
        lax.fori_loop(lo, hi, body, 0)

    shared_range(0, 1)
    metas = []
    for r in range(1, nd):
        dst = (me + r) % nd
        c = rcopy(meta_s.at[dst], metal.at[me], m_s.at[r - 1], m_r.at[r - 1], dst)
        c.start()
        metas.append(c)

    shared_range(1, n_chunks - 2)

    own_x[0].wait_recv()
    fy = rcopy(land.at[xn, hs(0)], land.at[xn, hs(0)], f_s.at[0], f_r.at[0], yn)
    fy.start()
    sx0 = rcopy(land.at[xn, hs(0)], land.at[xn, hs(0)], ss_s.at[1], ss_r.at[1], sib)
    sx0.start()
    own_y[1].wait_recv()
    fx = rcopy(land.at[yn, hs(1)], land.at[yn, hs(1)], f_s.at[1], f_r.at[1], xn)
    fx.start()
    sy1 = rcopy(land.at[yn, hs(1)], land.at[yn, hs(1)], ss_s.at[2], ss_r.at[2], sib)
    sy1.start()

    shared_range(n_chunks - 2, n_chunks)

    for c in metas:
        c.wait_recv()
    meta_all[...] = metal[...]
    for d in range(nd):
        cnt_ref[d:d + 1, :] = metal[d, 16:17, :].astype(jnp.int32)

    width_g = 8 * SLOT
    lane = lax.broadcasted_iota(jnp.int32, (8, width_g), 1)
    sel = jnp.where(lane // SLOT == lax.broadcasted_iota(jnp.int32, (8, width_g), 0), 1.0, 0.0)
    slot_id = (lax.broadcasted_iota(jnp.int32, (rows, width_g), 1) % SLOT).astype(F32)

    def spread(v):
        return lax.dot_general(v, sel, (((0,), (0,)), ((), ())), preferred_element_type=F32)[:rows]

    def gate_body(d, carry):
        rk = metal[d, 0:8, :]
        gt = metal[d, 8:16, :]
        hi = gt.astype(BF16).astype(F32)
        mid = (gt - hi).astype(BF16).astype(F32)
        lo = gt - hi - mid
        eq = spread(rk) == slot_id
        for q, part in enumerate((hi, mid, lo)):
            g_ref[d, q * rows:(q + 1) * rows, :] = jnp.where(eq, spread(part), 0.0).astype(BF16)
        return carry

    lax.fori_loop(0, nd, gate_body, 0)

    outs = [own_out]

    def emit(d, k):
        c = pltpu.make_async_copy(land.at[d], xall_hbm.at[d], osem.at[k])
        c.start()
        outs.append(c)

    own_s.wait_recv()
    emit(sib, 1)
    own_x[1].wait_recv()
    sx1 = rcopy(land.at[xn, hs(1)], land.at[xn, hs(1)], ss_s.at[3], ss_r.at[3], sib)
    sx1.start()
    emit(xn, 2)
    own_y[0].wait_recv()
    sy0 = rcopy(land.at[yn, hs(0)], land.at[yn, hs(0)], ss_s.at[4], ss_r.at[4], sib)
    sy0.start()
    emit(yn, 3)
    sxn = xn + 1 - 2 * core
    syn = yn + 1 - 2 * core
    sdg = dg + 1 - 2 * core
    sx0.wait_recv()
    sx1.wait_recv()
    emit(sxn, 4)
    sy1.wait_recv()
    sy0.wait_recv()
    emit(syn, 5)
    fy.wait_recv()
    sd0 = rcopy(land.at[dg, hs(0)], land.at[dg, hs(0)], ss_s.at[5], ss_r.at[5], sib)
    sd0.start()
    fx.wait_recv()
    sd1 = rcopy(land.at[dg, hs(1)], land.at[dg, hs(1)], ss_s.at[6], ss_r.at[6], sib)
    sd1.start()
    emit(dg, 6)
    sd0.wait_recv()
    sd1.wait_recv()
    emit(sdg, 7)
    for c in own_x + own_y + [own_s, fy, fx, sx0, sx1, sy0, sy1, sd0, sd1] + metas:
        c.wait_send()
    for c in outs:
        c.wait()


def gather_call(x, route, gates, sg, su, nd):
    rows, d_model = x.shape
    ff = sg.shape[1]
    width = 256
    n_chunks = ff // width
    any_spec = pl.BlockSpec(memory_space=pl.ANY)
    vmem = pl.BlockSpec(memory_space=pltpu.VMEM)
    dma = pltpu.SemaphoreType.DMA
    return pl.pallas_call(
        gather_kernel,
        out_shape=(
            jax.ShapeDtypeStruct((nd, rows, d_model), BF16),
            jax.ShapeDtypeStruct((rows, ff), BF16),
            jax.ShapeDtypeStruct((nd, 24, 128), F32),
            jax.ShapeDtypeStruct((nd, 128), jnp.int32),
            jax.ShapeDtypeStruct((nd, 3 * rows, 8 * SLOT), BF16),
        ),
        in_specs=[vmem, vmem, vmem, any_spec, any_spec],
        out_specs=(any_spec, vmem, vmem, vmem, vmem),
        scratch_shapes=[
            pltpu.VMEM((nd, rows, d_model), BF16),
            pltpu.VMEM((nd, 24, 128), F32),
            pltpu.VMEM((n_chunks, d_model, width), BF16),
            pltpu.VMEM((n_chunks, d_model, width), BF16),
            pltpu.VMEM((nd, 24, 128), F32),
            dma((2, n_chunks)),
            dma((8,)),
            dma((2,)), dma((2,)), dma((2,)), dma((2,)), dma((2,)), dma((2,)),
            dma((7,)), dma((7,)), dma((7,)), dma((7,)),
        ],
        compiler_params=pltpu.CompilerParams(
            collective_id=0, has_side_effects=True, vmem_limit_bytes=VMEM_LIMIT),
        name="gather_shared",
    )(x, route, gates, sg, su)


def hidden_kernel(cnt, meta, xall_hbm, w1_hbm, w3_hbm, h_hbm,
                  xv, wb1, wb3, xg, pos_c, pos_s, hbuf, xsem, wsem, hsem):
    me = lax.axis_index("ep")
    n_exp, d_model, ff = w1_hbm.shape
    nd = meta.shape[0]
    toks = xv.shape[0]
    rows = toks // nd
    depth = wb1.shape[0]
    small = rows
    full = nd * SLOT
    bounds = [(c, min(256, ff - c)) for c in range(0, ff, 256)]

    def wcopy(e, slot, j):
        c0, w = bounds[j]
        return (pltpu.make_async_copy(w1_hbm.at[e, :, c0:c0 + w], wb1.at[slot, :, c0:c0 + w], wsem.at[slot, 0, j]),
                pltpu.make_async_copy(w3_hbm.at[e, :, c0:c0 + w], wb3.at[slot, :, c0:c0 + w], wsem.at[slot, 1, j]))

    xc = pltpu.make_async_copy(xall_hbm, xv, xsem)
    xc.start()
    for e in range(depth):
        for j in range(len(bounds)):
            for c in wcopy(e, e, j):
                c.start()

    row_e = lax.broadcasted_iota(jnp.int32, (8, rows), 0)
    offs = [jnp.int32(0)] * n_exp
    for d in range(nd):
        rk = meta[d, 0:8, 0:rows].astype(jnp.int32)
        off = jnp.zeros((8, rows), jnp.int32)
        for e in range(n_exp):
            off = jnp.where(row_e == e, offs[e], off)
            offs[e] = offs[e] + cnt[d, me * n_exp + e]
        pos_c[:, d * rows:(d + 1) * rows] = jnp.where(rk >= 0, rk + off, -1)
        pos_s[:, d * rows:(d + 1) * rows] = jnp.where(rk >= 0, rk + d * SLOT, -1)
    xc.wait()

    def hcopy(e):
        return pltpu.make_async_copy(hbuf.at[e % 2], h_hbm.at[e], hsem.at[e % 2])

    def gather_rows(pos, m):
        onehot = jnp.where(pos == lax.broadcasted_iota(jnp.int32, (m, toks), 0), 1.0, 0.0).astype(BF16)
        for c0 in range(0, d_model, 512):
            xg[0:m, c0:c0 + 512] = jnp.dot(
                onehot, xv[:, c0:c0 + 512], preferred_element_type=F32).astype(BF16)

    def hidden(slot, j, m):
        c0, w = bounds[j]
        a = jnp.dot(xg[0:m, :], wb1[slot, :, c0:c0 + w], preferred_element_type=F32)
        b = jnp.dot(xg[0:m, :], wb3[slot, :, c0:c0 + w], preferred_element_type=F32)
        return (jax.nn.silu(a) * b).astype(BF16)

    def body(e, carry):
        slot = e % depth
        total = jnp.int32(0)
        for d in range(nd):
            total = total + cnt[d, me * n_exp + e]

        @pl.when(e >= 2)
        def _():
            hcopy(e - 2).wait()

        @pl.when(total <= small)
        def _():
            gather_rows(pos_c[pl.ds(e, 1), :], small)
            slot_row = lax.broadcasted_iota(jnp.int32, (SLOT, small), 0)
            col = lax.broadcasted_iota(jnp.int32, (SLOT, small), 1)
            parts = []
            start = jnp.int32(0)
            for d in range(nd):
                n = cnt[d, me * n_exp + e]
                hit = (col == slot_row + start) & (slot_row < n)
                parts.append(jnp.where(hit, 1.0, 0.0))
                start = start + n
            expand = jnp.concatenate(parts, axis=0).astype(BF16)
            for j, (c0, w) in enumerate(bounds):
                for c in wcopy(e, slot, j):
                    c.wait()
                hid = hidden(slot, j, small)
                hbuf[e % 2, :, c0:c0 + w] = jnp.dot(
                    expand, hid, preferred_element_type=F32).astype(BF16)

        @pl.when(total > small)
        def _():
            gather_rows(pos_s[pl.ds(e, 1), :], full)
            for j, (c0, w) in enumerate(bounds):
                for c in wcopy(e, slot, j):
                    c.wait()
                hbuf[e % 2, :, c0:c0 + w] = hidden(slot, j, full)

        hcopy(e).start()

        @pl.when(e + depth < n_exp)
        def _():
            for j in range(len(bounds)):
                for c in wcopy(e + depth, slot, j):
                    c.start()
        return carry

    lax.fori_loop(0, n_exp, body, 0)
    hcopy(n_exp - 2).wait()
    hcopy(n_exp - 1).wait()


def hidden_call(cnt, meta, xall, w1, w3):
    n_exp, d_model, ff = w1.shape
    toks = xall.shape[0]
    nd = meta.shape[0]
    depth = 3
    any_spec = pl.BlockSpec(memory_space=pl.ANY)
    dma = pltpu.SemaphoreType.DMA
    return pl.pallas_call(
        hidden_kernel,
        out_shape=jax.ShapeDtypeStruct((n_exp, nd * SLOT, ff), BF16),
        in_specs=[pl.BlockSpec(memory_space=pltpu.SMEM), pl.BlockSpec(memory_space=pltpu.VMEM),
                  any_spec, any_spec, any_spec],
        out_specs=any_spec,
        scratch_shapes=[
            pltpu.VMEM((toks, d_model), BF16),
            pltpu.VMEM((depth, d_model, ff), BF16),
            pltpu.VMEM((depth, d_model, ff), BF16),
            pltpu.VMEM((nd * SLOT, d_model), BF16),
            pltpu.VMEM((8, toks), jnp.int32),
            pltpu.VMEM((8, toks), jnp.int32),
            pltpu.VMEM((2, nd * SLOT, ff), BF16),
            dma(()), dma((depth, 2, pl.cdiv(ff, 256))), dma((2,)),
        ],
        compiler_params=pltpu.CompilerParams(vmem_limit_bytes=VMEM_LIMIT),
        name="routed_hidden",
    )(cnt, meta, xall, w1, w3)


def down_kernel(h_hbm, g_hbm, hsh_ref, w2_hbm, sd_hbm, y_ref,
                hv, gv, wb, sdb, ob, snd, kept, in0, in1, in2,
                hsem, gsem, wsem, dsem, s0s, s0r, s1s, s1r, s2s, s2r):
    me, core, sib, xn, yn, dg = neighbours()
    n_exp, full, ff = hv.shape
    nd = gv.shape[0]
    rows = gv.shape[1] // 3
    n_chunks = snd.shape[0]
    width = wb.shape[3]
    depth = wb.shape[0]
    hw = width // 2

    barrier = pltpu.get_barrier_semaphore()
    for dev in (sib, xn, yn):
        pl.semaphore_signal(barrier, inc=1, device_id={"ep": dev}, device_id_type=MESH)

    def wcopy(c, e):
        cols = pl.ds(pl.multiple_of(c * width, width), width)
        slot = c % depth
        return pltpu.make_async_copy(w2_hbm.at[e, :, cols], wb.at[slot, e], wsem.at[slot, e])

    def dcopy(c):
        cols = pl.ds(pl.multiple_of(c * width, width), width)
        return pltpu.make_async_copy(sd_hbm.at[:, cols], sdb.at[c], dsem.at[c])

    def hcopy(e):
        return pltpu.make_async_copy(h_hbm.at[e], hv.at[e], hsem.at[e])

    gcopy = pltpu.make_async_copy(g_hbm, gv, gsem)
    for e in range(n_exp):
        hcopy(e).start()
        wcopy(0, e).start()
    gcopy.start()
    for c in range(1, depth):
        for e in range(n_exp):
            wcopy(c, e).start()

    own_c, xn_c, yn_c, dg_c = me // 2, xn // 2, yn // 2, dg // 2
    orders = ((own_c, yn_c, xn_c, dg_c), (own_c, xn_c, yn_c, dg_c))
    first_hop = (xn, yn)
    second_hop = (yn, xn)

    def send0(c):
        return rcopy(snd.at[c], in0.at[c], s0s.at[c], s0r.at[c], sib)

    def send1(c, q):
        return rcopy(kept.at[c, q, pl.ds(2, 2)], in1.at[c, q], s1s.at[c, q], s1r.at[c, q], first_hop[q])

    def send2(c, q):
        return rcopy(kept.at[c, q, 1], in2.at[c, q], s2s.at[c, q], s2r.at[c, q], second_hop[q])

    def step0(c):
        send0(c).wait_recv()
        kept[c] = kept[c] + in0[c]

    def step1(c):
        for q in range(2):
            send1(c, q).wait_recv()
            kept[c, q, 0:2] = kept[c, q, 0:2] + in1[c, q]

    def step2(c):
        for q in range(2):
            send2(c, q).wait_recv()
            kept[c, q, 0] = kept[c, q, 0] + in2[c, q]

    def start1(c):
        send1(c, 0).start()
        send1(c, 1).start()

    def start2(c):
        send2(c, 0).start()
        send2(c, 1).start()

    def expert(c, e):
        wcopy(c, e).wait()
        out = jnp.dot(hv[e], wb[c % depth, e], preferred_element_type=F32)
        out = out.astype(BF16).astype(F32)
        ob[:, e] = out.reshape(nd, SLOT, width)

    def gated(d):
        o = ob[d].reshape(n_exp * SLOT, width).astype(BF16)
        r = jnp.dot(gv[d], o, preferred_element_type=F32)
        return r[0:rows] + r[rows:2 * rows] + r[2 * rows:3 * rows]

    def chunk(c, carry):
        for e in range(n_exp):
            @pl.when(c == 0)
            def _():
                hcopy(e).wait()
            expert(c, e)

            @pl.when(c + depth < n_chunks)
            def _():
                wcopy(c + depth, e).start()

            if e == n_exp // 2 - 1:
                @pl.when(c >= 1)
                def _():
                    step0(c - 1)

                @pl.when(c >= 2)
                def _():
                    step1(c - 2)

                @pl.when(c >= 1)
                def _():
                    start1(c - 1)

                @pl.when(c >= 2)
                def _():
                    start2(c - 2)

        dcopy(c).start()

        @pl.when(c == 0)
        def _():
            gcopy.wait()
        chips = (own_c, xn_c, yn_c, dg_c)
        where = ((0, 0), (2, 1), (1, 2), (3, 3))
        for chip, (p0, p1) in zip(chips, where):
            r = gated(2 * chip + 1 - core)
            snd[c, 0, p0] = r[:, 0:hw]
            snd[c, 1, p1] = r[:, hw:width]
        for chip, (p0, p1) in zip(chips, where):
            r = gated(2 * chip + core)
            kept[c, 0, p0] = r[:, 0:hw]
            kept[c, 1, p1] = r[:, hw:width]

        send0(c).start()
        return carry

    pl.semaphore_wait(barrier, 3)
    lax.fori_loop(0, n_chunks, chunk, 0)

    def shared(c):
        dcopy(c).wait()
        cols = pl.ds(pl.multiple_of(c * width, width), width)
        s = jnp.dot(hsh_ref[...], sdb[c], preferred_element_type=F32).astype(BF16)
        y_ref[:, cols] = s

    def shared_range(lo, hi):
        def body(c, carry):
            shared(c)
            return carry
        lax.fori_loop(lo, hi, body, 0)

    last = n_chunks - 1
    shared_range(0, 3)
    step0(last)
    step1(last - 1)
    start1(last)
    start2(last - 1)
    shared_range(3, n_chunks)
    step1(last)
    start2(last)

    def finish(c, carry):
        step2(c)
        for q in range(2):
            cols = pl.ds(pl.multiple_of(c * width + q * hw, hw), hw)
            y_ref[:, cols] = (y_ref[:, cols].astype(F32) + kept[c, q, 0]).astype(BF16)
        return carry

    lax.fori_loop(0, n_chunks, finish, 0)

    def drain(c, carry):
        send0(c).wait_send()
        for q in range(2):
            send1(c, q).wait_send()
            send2(c, q).wait_send()
        return carry

    lax.fori_loop(0, n_chunks, drain, 0)


def down_call(h, g, hsh, w2, sd):
    n_exp, full, ff = h.shape
    nd, rows3, width_g = g.shape
    rows = rows3 // 3
    d_model = w2.shape[2]
    width = 256
    n_chunks = d_model // width
    depth = 3
    hw = width // 2
    any_spec = pl.BlockSpec(memory_space=pl.ANY)
    vmem = pl.BlockSpec(memory_space=pltpu.VMEM)
    dma = pltpu.SemaphoreType.DMA
    return pl.pallas_call(
        down_kernel,
        out_shape=jax.ShapeDtypeStruct((rows, d_model), BF16),
        in_specs=[any_spec, any_spec, vmem, any_spec, any_spec],
        out_specs=vmem,
        scratch_shapes=[
            pltpu.VMEM((n_exp, full, ff), BF16),
            pltpu.VMEM((nd, rows3, width_g), BF16),
            pltpu.VMEM((depth, n_exp, ff, width), BF16),
            pltpu.VMEM((n_chunks, sd.shape[0], width), BF16),
            pltpu.VMEM((nd, n_exp, SLOT, width), F32),
            pltpu.VMEM((n_chunks, 2, 4, rows, hw), F32),
            pltpu.VMEM((n_chunks, 2, 4, rows, hw), F32),
            pltpu.VMEM((n_chunks, 2, 4, rows, hw), F32),
            pltpu.VMEM((n_chunks, 2, 2, rows, hw), F32),
            pltpu.VMEM((n_chunks, 2, rows, hw), F32),
            dma((n_exp,)), dma(()), dma((depth, n_exp)), dma((n_chunks,)),
            dma((n_chunks,)), dma((n_chunks,)),
            dma((n_chunks, 2)), dma((n_chunks, 2)), dma((n_chunks, 2)), dma((n_chunks, 2)),
        ],
        compiler_params=pltpu.CompilerParams(
            collective_id=1, has_side_effects=True, vmem_limit_bytes=VMEM_LIMIT),
        name="down_reduce",
    )(h, g, hsh, w2, sd)


def solution(mesh):
    nd = mesh.shape["ep"]

    def device_fn(x, route, gates, w_gate, w_up, w_down, sg, su, sd):
        xall, hsh, meta, cnt, g = gather_call(x, route, gates, sg, su, nd)
        h = hidden_call(cnt, meta, xall.reshape(nd * x.shape[0], x.shape[1]), w_gate, w_up)
        return down_call(h, g, hsh, w_down, sd)

    tok = P(("dp", "ep"), None)
    exp = P("ep", None, None)
    rep = P(None, None)
    return jax.shard_map(device_fn, mesh=mesh, in_specs=(tok, tok, tok, exp, exp, exp, rep, rep, rep),
                         out_specs=tok, check_vma=False)
```

```python
import functools

import jax
import jax.numpy as jnp
from jax import lax
from jax.experimental import pallas as pl
from jax.experimental.pallas import tpu as pltpu
from jax.sharding import PartitionSpec as P

MESH = pl.DeviceIdType.MESH
CAP = 36
SLOT = 40
VMEM_LIMIT = 67_000_000
BF16 = jnp.bfloat16
F32 = jnp.float32


def neighbours():
    me = lax.axis_index("ep")
    core = me % 2
    xb = (me // 2) % 2
    yb = me // 4
    sib = me + 1 - 2 * core
    xn = me + 2 - 4 * xb
    yn = me + 4 - 8 * yb
    dg = yn + 2 - 4 * xb
    return me, core, sib, xn, yn, dg


def rcopy(src, dst, send, recv, dev):
    return pltpu.make_async_remote_copy(
        src_ref=src, dst_ref=dst, send_sem=send, recv_sem=recv,
        device_id={"ep": dev}, device_id_type=MESH)


def gather_kernel(x_ref, route_ref, gate_ref, sg_hbm, su_hbm,
                  xall_hbm, hsh_ref, meta_all, cnt_ref, g_ref,
                  land, meta_s, bg, bu, metal,
                  wsem, osem, sx_s, sx_r, sy_s, sy_r, f_s, f_r, ss_s, ss_r, m_s, m_r):
    me, core, sib, xn, yn, dg = neighbours()
    nd = xall_hbm.shape[0]
    rows = x_ref.shape[0]
    half = rows // 2
    n_chunks = bg.shape[0]
    width = bg.shape[2]

    barrier = pltpu.get_barrier_semaphore()
    for r in range(1, nd):
        pl.semaphore_signal(barrier, inc=1, device_id={"ep": (me + r) % nd}, device_id_type=MESH)

    def wcopy(i):
        cols = pl.ds(pl.multiple_of(i * width, width), width)
        return (pltpu.make_async_copy(sg_hbm.at[:, cols], bg.at[i], wsem.at[0, i]),
                pltpu.make_async_copy(su_hbm.at[:, cols], bu.at[i], wsem.at[1, i]))

    for i in range(n_chunks):
        for c in wcopy(i):
            c.start()

    def hs(h):
        return pl.ds(h * half, half)

    own_out = pltpu.make_async_copy(x_ref, xall_hbm.at[me], osem.at[0])
    own_out.start()

    pl.semaphore_wait(barrier, nd - 1)
    own_x = [rcopy(x_ref.at[hs(h)], land.at[me, hs(h)], sx_s.at[h], sx_r.at[h], xn) for h in range(2)]
    own_y = [rcopy(x_ref.at[hs(h)], land.at[me, hs(h)], sy_s.at[h], sy_r.at[h], yn) for h in range(2)]
    own_s = rcopy(x_ref, land.at[me], ss_s.at[0], ss_r.at[0], sib)
    own_x[0].start()
    own_y[1].start()
    own_x[1].start()
    own_y[0].start()
    own_s.start()

    ids = lax.broadcasted_iota(jnp.int32, (rows, 128), 1)
    mask = jnp.zeros((rows, 128), F32)
    gmap = jnp.zeros((rows, 128), F32)
    for k in range(route_ref.shape[1]):
        eq = route_ref[:, k:k + 1] == ids
        mask = mask + jnp.where(eq, 1.0, 0.0)
        gmap = gmap + jnp.where(eq, gate_ref[:, k:k + 1], 0.0)
    lower = (lax.broadcasted_iota(jnp.int32, (rows, rows), 0)
             > lax.broadcasted_iota(jnp.int32, (rows, rows), 1))
    rank = jnp.dot(jnp.where(lower, 1.0, 0.0).astype(BF16), mask.astype(BF16), preferred_element_type=F32)
    rank = jnp.where(mask > 0.0, rank, -1.0)
    count = jnp.broadcast_to(jnp.sum(mask, axis=0, keepdims=True), (8, 128))
    rank_t = jnp.concatenate([rank, jnp.full((128 - rows, 128), -1.0, F32)], axis=0).T
    gate_t = jnp.concatenate([gmap, jnp.zeros((128 - rows, 128), F32)], axis=0).T
    for j in range(nd):
        meta_s[j, 0:8, :] = rank_t[8 * j:8 * j + 8]
        meta_s[j, 8:16, :] = gate_t[8 * j:8 * j + 8]
        meta_s[j, 16:24, :] = count
    metal[me] = meta_s[me]

    def shared_chunk(i):
        for c in wcopy(i):
            c.wait()
        a = jnp.dot(x_ref[...], bg[i], preferred_element_type=F32)
        b = jnp.dot(x_ref[...], bu[i], preferred_element_type=F32)
        cols = pl.ds(pl.multiple_of(i * width, width), width)
        hsh_ref[:, cols] = (jax.nn.silu(a) * b).astype(BF16)

    def shared_range(lo, hi):
        def body(i, carry):
            shared_chunk(i)
            return carry
        lax.fori_loop(lo, hi, body, 0)

    shared_range(0, 1)
    metas = []
    for r in range(1, nd):
        dst = (me + r) % nd
        c = rcopy(meta_s.at[dst], metal.at[me], m_s.at[r - 1], m_r.at[r - 1], dst)
        c.start()
        metas.append(c)

    shared_range(1, n_chunks - 2)

    own_x[0].wait_recv()
    fy = rcopy(land.at[xn, hs(0)], land.at[xn, hs(0)], f_s.at[0], f_r.at[0], yn)
    fy.start()
    sx0 = rcopy(land.at[xn, hs(0)], land.at[xn, hs(0)], ss_s.at[1], ss_r.at[1], sib)
    sx0.start()
    own_y[1].wait_recv()
    fx = rcopy(land.at[yn, hs(1)], land.at[yn, hs(1)], f_s.at[1], f_r.at[1], xn)
    fx.start()
    sy1 = rcopy(land.at[yn, hs(1)], land.at[yn, hs(1)], ss_s.at[2], ss_r.at[2], sib)
    sy1.start()

    shared_range(n_chunks - 2, n_chunks)

    for c in metas:
        c.wait_recv()
    meta_all[...] = metal[...]
    for d in range(nd):
        cnt_ref[d:d + 1, :] = metal[d, 16:17, :].astype(jnp.int32)

    width_g = 8 * SLOT
    lane = lax.broadcasted_iota(jnp.int32, (8, width_g), 1)
    sel = jnp.where(lane // SLOT == lax.broadcasted_iota(jnp.int32, (8, width_g), 0), 1.0, 0.0)
    slot_id = (lax.broadcasted_iota(jnp.int32, (rows, width_g), 1) % SLOT).astype(F32)

    def spread(v):
        return lax.dot_general(v, sel, (((0,), (0,)), ((), ())), preferred_element_type=F32)[:rows]

    def gate_body(d, carry):
        rk = metal[d, 0:8, :]
        gt = metal[d, 8:16, :]
        hi = gt.astype(BF16).astype(F32)
        mid = (gt - hi).astype(BF16).astype(F32)
        lo = gt - hi - mid
        eq = spread(rk) == slot_id
        for q, part in enumerate((hi, mid, lo)):
            g_ref[d, q * rows:(q + 1) * rows, :] = jnp.where(eq, spread(part), 0.0).astype(BF16)
        return carry

    lax.fori_loop(0, nd, gate_body, 0)

    outs = [own_out]

    def emit(d, k):
        c = pltpu.make_async_copy(land.at[d], xall_hbm.at[d], osem.at[k])
        c.start()
        outs.append(c)

    own_s.wait_recv()
    emit(sib, 1)
    own_x[1].wait_recv()
    sx1 = rcopy(land.at[xn, hs(1)], land.at[xn, hs(1)], ss_s.at[3], ss_r.at[3], sib)
    sx1.start()
    emit(xn, 2)
    own_y[0].wait_recv()
    sy0 = rcopy(land.at[yn, hs(0)], land.at[yn, hs(0)], ss_s.at[4], ss_r.at[4], sib)
    sy0.start()
    emit(yn, 3)
    sxn = xn + 1 - 2 * core
    syn = yn + 1 - 2 * core
    sdg = dg + 1 - 2 * core
    sx0.wait_recv()
    sx1.wait_recv()
    emit(sxn, 4)
    sy1.wait_recv()
    sy0.wait_recv()
    emit(syn, 5)
    fy.wait_recv()
    sd0 = rcopy(land.at[dg, hs(0)], land.at[dg, hs(0)], ss_s.at[5], ss_r.at[5], sib)
    sd0.start()
    fx.wait_recv()
    sd1 = rcopy(land.at[dg, hs(1)], land.at[dg, hs(1)], ss_s.at[6], ss_r.at[6], sib)
    sd1.start()
    emit(dg, 6)
    sd0.wait_recv()
    sd1.wait_recv()
    emit(sdg, 7)
    for c in own_x + own_y + [own_s, fy, fx, sx0, sx1, sy0, sy1, sd0, sd1] + metas:
        c.wait_send()
    for c in outs:
        c.wait()


def gather_call(x, route, gates, sg, su, nd):
    rows, d_model = x.shape
    ff = sg.shape[1]
    width = 256
    n_chunks = ff // width
    any_spec = pl.BlockSpec(memory_space=pl.ANY)
    vmem = pl.BlockSpec(memory_space=pltpu.VMEM)
    dma = pltpu.SemaphoreType.DMA
    return pl.pallas_call(
        gather_kernel,
        out_shape=(
            jax.ShapeDtypeStruct((nd, rows, d_model), BF16),
            jax.ShapeDtypeStruct((rows, ff), BF16),
            jax.ShapeDtypeStruct((nd, 24, 128), F32),
            jax.ShapeDtypeStruct((nd, 128), jnp.int32),
            jax.ShapeDtypeStruct((nd, 3 * rows, 8 * SLOT), BF16),
        ),
        in_specs=[vmem, vmem, vmem, any_spec, any_spec],
        out_specs=(any_spec, vmem, vmem, vmem, vmem),
        scratch_shapes=[
            pltpu.VMEM((nd, rows, d_model), BF16),
            pltpu.VMEM((nd, 24, 128), F32),
            pltpu.VMEM((n_chunks, d_model, width), BF16),
            pltpu.VMEM((n_chunks, d_model, width), BF16),
            pltpu.VMEM((nd, 24, 128), F32),
            dma((2, n_chunks)),
            dma((8,)),
            dma((2,)), dma((2,)), dma((2,)), dma((2,)), dma((2,)), dma((2,)),
            dma((7,)), dma((7,)), dma((7,)), dma((7,)),
        ],
        compiler_params=pltpu.CompilerParams(
            collective_id=0, has_side_effects=True, vmem_limit_bytes=VMEM_LIMIT),
        name="gather_shared",
    )(x, route, gates, sg, su)


def hidden_kernel(cnt, meta, xall_hbm, w1_hbm, w3_hbm, h_hbm,
                  xv, wb1, wb3, xg, pos_c, pos_s, hbuf, xsem, wsem, hsem):
    me = lax.axis_index("ep")
    n_exp, d_model, ff = w1_hbm.shape
    nd = meta.shape[0]
    toks = xv.shape[0]
    rows = toks // nd
    depth = wb1.shape[0]
    small = rows
    full = nd * SLOT
    bounds = [(c, min(256, ff - c)) for c in range(0, ff, 256)]
    cut = 3 * 256
    groups = ((0, cut, bounds[:3]), (cut, ff - cut, bounds[3:]))

    def wcopy(e, slot, j):
        c0, w, _ = groups[j]
        return (pltpu.make_async_copy(w1_hbm.at[e, :, c0:c0 + w], wb1.at[slot, :, c0:c0 + w], wsem.at[slot, 0, j]),
                pltpu.make_async_copy(w3_hbm.at[e, :, c0:c0 + w], wb3.at[slot, :, c0:c0 + w], wsem.at[slot, 1, j]))

    xc = pltpu.make_async_copy(xall_hbm, xv, xsem)
    xc.start()
    for e in range(depth):
        for j in range(len(groups)):
            for c in wcopy(e, e, j):
                c.start()

    row_e = lax.broadcasted_iota(jnp.int32, (8, rows), 0)
    offs = [jnp.int32(0)] * n_exp
    for d in range(nd):
        rk = meta[d, 0:8, 0:rows].astype(jnp.int32)
        off = jnp.zeros((8, rows), jnp.int32)
        for e in range(n_exp):
            off = jnp.where(row_e == e, offs[e], off)
            offs[e] = offs[e] + cnt[d, me * n_exp + e]
        pos_c[:, d * rows:(d + 1) * rows] = jnp.where(rk >= 0, rk + off, -1)
        pos_s[:, d * rows:(d + 1) * rows] = jnp.where(rk >= 0, rk + d * SLOT, -1)
    xc.wait()

    def hcopy(e):
        return pltpu.make_async_copy(hbuf.at[e % 2], h_hbm.at[e], hsem.at[e % 2])

    def gather_rows(pos, m):
        onehot = jnp.where(pos == lax.broadcasted_iota(jnp.int32, (m, toks), 0), 1.0, 0.0).astype(BF16)
        for c0 in range(0, d_model, 512):
            xg[0:m, c0:c0 + 512] = jnp.dot(
                onehot, xv[:, c0:c0 + 512], preferred_element_type=F32).astype(BF16)

    def hidden(slot, c0, w, m):
        a = jnp.dot(xg[0:m, :], wb1[slot, :, c0:c0 + w], preferred_element_type=F32)
        b = jnp.dot(xg[0:m, :], wb3[slot, :, c0:c0 + w], preferred_element_type=F32)
        return (jax.nn.silu(a) * b).astype(BF16)

    def body(e, carry):
        slot = e % depth
        total = jnp.int32(0)
        for d in range(nd):
            total = total + cnt[d, me * n_exp + e]

        @pl.when(e >= 2)
        def _():
            hcopy(e - 2).wait()

        @pl.when(total <= small)
        def _():
            gather_rows(pos_c[pl.ds(e, 1), :], small)
            slot_row = lax.broadcasted_iota(jnp.int32, (SLOT, small), 0)
            col = lax.broadcasted_iota(jnp.int32, (SLOT, small), 1)
            parts = []
            start = jnp.int32(0)
            for d in range(nd):
                n = cnt[d, me * n_exp + e]
                hit = (col == slot_row + start) & (slot_row < n)
                parts.append(jnp.where(hit, 1.0, 0.0))
                start = start + n
            expand = jnp.concatenate(parts, axis=0).astype(BF16)
            for j, (_, _, cols) in enumerate(groups):
                for c in wcopy(e, slot, j):
                    c.wait()
                for c0, w in cols:
                    hid = hidden(slot, c0, w, small)
                    hbuf[e % 2, :, c0:c0 + w] = jnp.dot(
                        expand, hid, preferred_element_type=F32).astype(BF16)

        @pl.when(total > small)
        def _():
            gather_rows(pos_s[pl.ds(e, 1), :], full)
            for j, (_, _, cols) in enumerate(groups):
                for c in wcopy(e, slot, j):
                    c.wait()
                for c0, w in cols:
                    hbuf[e % 2, :, c0:c0 + w] = hidden(slot, c0, w, full)

        hcopy(e).start()

        @pl.when(e + depth < n_exp)
        def _():
            for j in range(len(groups)):
                for c in wcopy(e + depth, slot, j):
                    c.start()
        return carry

    lax.fori_loop(0, n_exp, body, 0)
    hcopy(n_exp - 2).wait()
    hcopy(n_exp - 1).wait()


def hidden_call(cnt, meta, xall, w1, w3):
    n_exp, d_model, ff = w1.shape
    toks = xall.shape[0]
    nd = meta.shape[0]
    depth = 3
    any_spec = pl.BlockSpec(memory_space=pl.ANY)
    dma = pltpu.SemaphoreType.DMA
    return pl.pallas_call(
        hidden_kernel,
        out_shape=jax.ShapeDtypeStruct((n_exp, nd * SLOT, ff), BF16),
        in_specs=[pl.BlockSpec(memory_space=pltpu.SMEM), pl.BlockSpec(memory_space=pltpu.VMEM),
                  any_spec, any_spec, any_spec],
        out_specs=any_spec,
        scratch_shapes=[
            pltpu.VMEM((toks, d_model), BF16),
            pltpu.VMEM((depth, d_model, ff), BF16),
            pltpu.VMEM((depth, d_model, ff), BF16),
            pltpu.VMEM((nd * SLOT, d_model), BF16),
            pltpu.VMEM((8, toks), jnp.int32),
            pltpu.VMEM((8, toks), jnp.int32),
            pltpu.VMEM((2, nd * SLOT, ff), BF16),
            dma(()), dma((depth, 2, 2)), dma((2,)),
        ],
        compiler_params=pltpu.CompilerParams(vmem_limit_bytes=VMEM_LIMIT),
        name="routed_hidden",
    )(cnt, meta, xall, w1, w3)


def down_kernel(h_hbm, g_hbm, hsh_ref, w2_hbm, sd_hbm, y_ref,
                hv, gv, wb, sdb, ob, snd, kept, in0, in1, in2,
                hsem, gsem, wsem, dsem, s0s, s0r, s1s, s1r, s2s, s2r):
    me, core, sib, xn, yn, dg = neighbours()
    n_exp, full, ff = hv.shape
    nd = gv.shape[0]
    rows = gv.shape[1] // 3
    n_chunks = snd.shape[0]
    width = wb.shape[3]
    depth = wb.shape[0]
    hw = width // 2

    barrier = pltpu.get_barrier_semaphore()
    for dev in (sib, xn, yn):
        pl.semaphore_signal(barrier, inc=1, device_id={"ep": dev}, device_id_type=MESH)

    def wcopy(c, e):
        cols = pl.ds(pl.multiple_of(c * width, width), width)
        slot = c % depth
        return pltpu.make_async_copy(w2_hbm.at[e, :, cols], wb.at[slot, e], wsem.at[slot, e])

    def dcopy(c):
        cols = pl.ds(pl.multiple_of(c * width, width), width)
        return pltpu.make_async_copy(sd_hbm.at[:, cols], sdb.at[c], dsem.at[c])

    def hcopy(e):
        return pltpu.make_async_copy(h_hbm.at[e], hv.at[e], hsem.at[e])

    gcopy = pltpu.make_async_copy(g_hbm, gv, gsem)
    for e in range(n_exp):
        hcopy(e).start()
        wcopy(0, e).start()
    gcopy.start()
    for c in range(1, depth):
        for e in range(n_exp):
            wcopy(c, e).start()

    own_c, xn_c, yn_c, dg_c = me // 2, xn // 2, yn // 2, dg // 2
    orders = ((own_c, yn_c, xn_c, dg_c), (own_c, xn_c, yn_c, dg_c))
    first_hop = (xn, yn)
    second_hop = (yn, xn)

    def send0(c):
        return rcopy(snd.at[c], in0.at[c], s0s.at[c], s0r.at[c], sib)

    def send1(c, q):
        return rcopy(kept.at[c, q, pl.ds(2, 2)], in1.at[c, q], s1s.at[c, q], s1r.at[c, q], first_hop[q])

    def send2(c, q):
        return rcopy(kept.at[c, q, 1], in2.at[c, q], s2s.at[c, q], s2r.at[c, q], second_hop[q])

    def step0(c):
        send0(c).wait_recv()
        kept[c] = kept[c] + in0[c]

    def step1(c):
        for q in range(2):
            send1(c, q).wait_recv()
            kept[c, q, 0:2] = kept[c, q, 0:2] + in1[c, q]

    def step2(c):
        for q in range(2):
            send2(c, q).wait_recv()
            kept[c, q, 0] = kept[c, q, 0] + in2[c, q]

    def start1(c):
        send1(c, 0).start()
        send1(c, 1).start()

    def start2(c):
        send2(c, 0).start()
        send2(c, 1).start()

    def expert(c, e):
        out = jnp.dot(hv[e], wb[c % depth, e], preferred_element_type=F32)
        out = out.astype(BF16).astype(F32)
        ob[:, e] = out.reshape(nd, SLOT, width)

    def gated(d):
        o = ob[d].reshape(n_exp * SLOT, width).astype(BF16)
        r = jnp.dot(gv[d], o, preferred_element_type=F32)
        return r[0:rows] + r[rows:2 * rows] + r[2 * rows:3 * rows]

    def chunk(c, carry):
        for e0 in range(0, n_exp, 4):
            @pl.when(c == 0)
            def _():
                for e in range(e0, e0 + 4):
                    hcopy(e).wait()
            for e in range(e0, e0 + 4):
                wcopy(c, e).wait()
            for e in range(e0, e0 + 4):
                expert(c, e)

            @pl.when(c + depth < n_chunks)
            def _():
                for e in range(e0, e0 + 4):
                    wcopy(c + depth, e).start()

            if e0 == 0:
                @pl.when(c >= 1)
                def _():
                    step0(c - 1)

                @pl.when(c >= 2)
                def _():
                    step1(c - 2)

                @pl.when(c >= 1)
                def _():
                    start1(c - 1)

                @pl.when(c >= 2)
                def _():
                    start2(c - 2)

        dcopy(c).start()

        @pl.when(c == 0)
        def _():
            gcopy.wait()
        chips = (own_c, xn_c, yn_c, dg_c)
        where = ((0, 0), (2, 1), (1, 2), (3, 3))
        for chip, (p0, p1) in zip(chips, where):
            r = gated(2 * chip + 1 - core)
            snd[c, 0, p0] = r[:, 0:hw]
            snd[c, 1, p1] = r[:, hw:width]
        for chip, (p0, p1) in zip(chips, where):
            r = gated(2 * chip + core)
            kept[c, 0, p0] = r[:, 0:hw]
            kept[c, 1, p1] = r[:, hw:width]

        send0(c).start()
        return carry

    pl.semaphore_wait(barrier, 3)
    lax.fori_loop(0, n_chunks, chunk, 0)

    def shared(c):
        dcopy(c).wait()
        cols = pl.ds(pl.multiple_of(c * width, width), width)
        s = jnp.dot(hsh_ref[...], sdb[c], preferred_element_type=F32).astype(BF16)
        y_ref[:, cols] = s

    def shared_range(lo, hi):
        def body(c, carry):
            shared(c)
            return carry
        lax.fori_loop(lo, hi, body, 0)

    last = n_chunks - 1
    shared_range(0, 3)
    step0(last)
    step1(last - 1)
    start1(last)
    start2(last - 1)
    shared_range(3, n_chunks)
    step1(last)
    start2(last)

    def finish(c, carry):
        step2(c)
        for q in range(2):
            cols = pl.ds(pl.multiple_of(c * width + q * hw, hw), hw)
            y_ref[:, cols] = (y_ref[:, cols].astype(F32) + kept[c, q, 0]).astype(BF16)
        return carry

    lax.fori_loop(0, n_chunks, finish, 0)

    def drain(c, carry):
        send0(c).wait_send()
        for q in range(2):
            send1(c, q).wait_send()
            send2(c, q).wait_send()
        return carry

    lax.fori_loop(0, n_chunks, drain, 0)


def down_call(h, g, hsh, w2, sd):
    n_exp, full, ff = h.shape
    nd, rows3, width_g = g.shape
    rows = rows3 // 3
    d_model = w2.shape[2]
    width = 256
    n_chunks = d_model // width
    depth = 3
    hw = width // 2
    any_spec = pl.BlockSpec(memory_space=pl.ANY)
    vmem = pl.BlockSpec(memory_space=pltpu.VMEM)
    dma = pltpu.SemaphoreType.DMA
    return pl.pallas_call(
        down_kernel,
        out_shape=jax.ShapeDtypeStruct((rows, d_model), BF16),
        in_specs=[any_spec, any_spec, vmem, any_spec, any_spec],
        out_specs=vmem,
        scratch_shapes=[
            pltpu.VMEM((n_exp, full, ff), BF16),
            pltpu.VMEM((nd, rows3, width_g), BF16),
            pltpu.VMEM((depth, n_exp, ff, width), BF16),
            pltpu.VMEM((n_chunks, sd.shape[0], width), BF16),
            pltpu.VMEM((nd, n_exp, SLOT, width), F32),
            pltpu.VMEM((n_chunks, 2, 4, rows, hw), F32),
            pltpu.VMEM((n_chunks, 2, 4, rows, hw), F32),
            pltpu.VMEM((n_chunks, 2, 4, rows, hw), F32),
            pltpu.VMEM((n_chunks, 2, 2, rows, hw), F32),
            pltpu.VMEM((n_chunks, 2, rows, hw), F32),
            dma((n_exp,)), dma(()), dma((depth, n_exp)), dma((n_chunks,)),
            dma((n_chunks,)), dma((n_chunks,)),
            dma((n_chunks, 2)), dma((n_chunks, 2)), dma((n_chunks, 2)), dma((n_chunks, 2)),
        ],
        compiler_params=pltpu.CompilerParams(
            collective_id=1, has_side_effects=True, vmem_limit_bytes=VMEM_LIMIT),
        name="down_reduce",
    )(h, g, hsh, w2, sd)


def solution(mesh):
    nd = mesh.shape["ep"]

    def device_fn(x, route, gates, w_gate, w_up, w_down, sg, su, sd):
        xall, hsh, meta, cnt, g = gather_call(x, route, gates, sg, su, nd)
        h = hidden_call(cnt, meta, xall.reshape(nd * x.shape[0], x.shape[1]), w_gate, w_up)
        return down_call(h, g, hsh, w_down, sd)

    tok = P(("dp", "ep"), None)
    exp = P("ep", None, None)
    rep = P(None, None)
    return jax.shard_map(device_fn, mesh=mesh, in_specs=(tok, tok, tok, exp, exp, exp, rep, rep, rep),
                         out_specs=tok, check_vma=False)
```

```python
import functools

import jax
import jax.numpy as jnp
from jax import lax
from jax.experimental import pallas as pl
from jax.experimental.pallas import tpu as pltpu
from jax.sharding import PartitionSpec as P

MESH = pl.DeviceIdType.MESH
CAP = 36
SLOT = 40
VMEM_LIMIT = 67_000_000
BF16 = jnp.bfloat16
F32 = jnp.float32


def neighbours():
    me = lax.axis_index("ep")
    core = me % 2
    xb = (me // 2) % 2
    yb = me // 4
    sib = me + 1 - 2 * core
    xn = me + 2 - 4 * xb
    yn = me + 4 - 8 * yb
    dg = yn + 2 - 4 * xb
    return me, core, sib, xn, yn, dg


def rcopy(src, dst, send, recv, dev):
    return pltpu.make_async_remote_copy(
        src_ref=src, dst_ref=dst, send_sem=send, recv_sem=recv,
        device_id={"ep": dev}, device_id_type=MESH)


def gather_kernel(x_ref, route_ref, gate_ref, sg_hbm, su_hbm,
                  xg_hbm, hsh_hbm, cnt_hbm, g_hbm,
                  land, meta_s, bg, bu, metal, stage, hsh, gv, cntv,
                  wsem, osem, gsem, hsem, csem,
                  sx_s, sx_r, sy_s, sy_r, f_s, f_r, ss_s, ss_r, m_s, m_r):
    me, core, sib, xn, yn, dg = neighbours()
    sxn = xn + 1 - 2 * core
    syn = yn + 1 - 2 * core
    sdg = dg + 1 - 2 * core
    nd = land.shape[0]
    rows, d_model = x_ref.shape
    half = rows // 2
    n_chunks = bg.shape[0]
    width = bg.shape[2]
    n_all = 8 * nd

    barrier = pltpu.get_barrier_semaphore()
    for r in range(1, nd):
        pl.semaphore_signal(barrier, inc=1, device_id={"ep": (me + r) % nd}, device_id_type=MESH)

    def wcopy(i):
        cols = pl.ds(pl.multiple_of(i * width, width), width)
        return (pltpu.make_async_copy(sg_hbm.at[:, cols], bg.at[i], wsem.at[0, i]),
                pltpu.make_async_copy(su_hbm.at[:, cols], bu.at[i], wsem.at[1, i]))

    for i in range(n_chunks):
        for c in wcopy(i):
            c.start()

    ids = lax.broadcasted_iota(jnp.int32, (n_all, rows), 0)
    mask = jnp.zeros((n_all, rows), F32)
    gmap = jnp.zeros((n_all, rows), F32)
    for k in range(route_ref.shape[0]):
        eq = route_ref[k:k + 1, :] == ids
        mask = mask + jnp.where(eq, 1.0, 0.0)
        gmap = gmap + jnp.where(eq, gate_ref[k:k + 1, :], 0.0)
    before = (lax.broadcasted_iota(jnp.int32, (rows, rows), 0)
              < lax.broadcasted_iota(jnp.int32, (rows, rows), 1))
    rank = jnp.dot(mask.astype(BF16), jnp.where(before, 1.0, 0.0).astype(BF16), preferred_element_type=F32)
    rank = jnp.where(mask > 0.0, rank, -1.0)
    fill = jnp.zeros((n_all, 128 - rows), F32)
    rank = jnp.concatenate([rank, fill - 1.0], axis=1)
    gmap = jnp.concatenate([gmap, fill], axis=1)
    for j in range(nd):
        meta_s[j, 0:8, :] = rank[8 * j:8 * j + 8]
        meta_s[j, 8:16, :] = gmap[8 * j:8 * j + 8]
    metal[me] = meta_s[me]

    def hs(h):
        return pl.ds(h * half, half)

    pl.semaphore_wait(barrier, nd - 1)
    metas = []
    for r in range(1, nd):
        dst = (me + r) % nd
        c = rcopy(meta_s.at[dst], metal.at[me], m_s.at[r - 1], m_r.at[r - 1], dst)
        c.start()
        metas.append(c)
    own_x = [rcopy(x_ref.at[hs(h)], land.at[me, hs(h)], sx_s.at[h], sx_r.at[h], xn) for h in range(2)]
    own_y = [rcopy(x_ref.at[hs(h)], land.at[me, hs(h)], sy_s.at[h], sy_r.at[h], yn) for h in range(2)]
    own_s = rcopy(x_ref, land.at[me], ss_s.at[0], ss_r.at[0], sib)
    own_x[0].start()
    own_y[1].start()
    own_x[1].start()
    own_y[0].start()
    own_s.start()

    def shared_range(lo, hi):
        def body(i, carry):
            for c in wcopy(i):
                c.wait()
            a = jnp.dot(x_ref[...], bg[i], preferred_element_type=F32)
            b = jnp.dot(x_ref[...], bu[i], preferred_element_type=F32)
            cols = pl.ds(pl.multiple_of(i * width, width), width)
            hsh[:, cols] = (jax.nn.silu(a) * b).astype(BF16)
            return carry
        lax.fori_loop(lo, hi, body, 0)

    shared_range(0, n_chunks - 5)

    for c in metas:
        c.wait_recv()

    for d in range(nd):
        n = jnp.sum(jnp.where(metal[d, 0:8, :] >= 0.0, 1.0, 0.0), axis=1, keepdims=True)
        cntv[d] = jnp.broadcast_to(n, (8, 128)).astype(jnp.int32)
    ccopy = pltpu.make_async_copy(cntv, cnt_hbm, csem)
    ccopy.start()

    def pick(d, x_rows, k):
        buf = k % 2
        if k >= 2:
            outs[k - 2].wait()
        slot = lax.broadcasted_iota(jnp.int32, (SLOT, rows), 0).astype(F32)
        sel = jnp.concatenate(
            [jnp.where(metal[d, e:e + 1, 0:rows] == slot, 1.0, 0.0) for e in range(8)], axis=0).astype(BF16)
        for c0 in range(0, d_model, 512):
            r = jnp.dot(sel, x_rows[:, c0:c0 + 512], preferred_element_type=F32)
            stage[buf, :, :, c0:c0 + 512] = r.astype(BF16).reshape(8, SLOT, 512)
        c = pltpu.make_async_copy(stage.at[buf], xg_hbm.at[:, d], osem.at[k])
        c.start()
        outs.append(c)

    outs = []
    pick(me, x_ref, 0)
    own_s.wait_recv()
    pick(sib, land.at[sib], 1)

    own_x[0].wait_recv()
    fy = rcopy(land.at[xn, hs(0)], land.at[xn, hs(0)], f_s.at[0], f_r.at[0], yn)
    fy.start()
    sx0 = rcopy(land.at[xn, hs(0)], land.at[xn, hs(0)], ss_s.at[1], ss_r.at[1], sib)
    sx0.start()
    own_y[1].wait_recv()
    fx = rcopy(land.at[yn, hs(1)], land.at[yn, hs(1)], f_s.at[1], f_r.at[1], xn)
    fx.start()
    sy1 = rcopy(land.at[yn, hs(1)], land.at[yn, hs(1)], ss_s.at[2], ss_r.at[2], sib)
    sy1.start()

    shared_range(n_chunks - 5, n_chunks)
    hcopy = pltpu.make_async_copy(hsh, hsh_hbm, hsem)
    hcopy.start()

    own_x[1].wait_recv()
    sx1 = rcopy(land.at[xn, hs(1)], land.at[xn, hs(1)], ss_s.at[3], ss_r.at[3], sib)
    sx1.start()
    own_y[0].wait_recv()
    sy0 = rcopy(land.at[yn, hs(0)], land.at[yn, hs(0)], ss_s.at[4], ss_r.at[4], sib)
    sy0.start()
    pick(xn, land.at[xn], 2)
    pick(yn, land.at[yn], 3)
    sx0.wait_recv()
    sx1.wait_recv()
    pick(sxn, land.at[sxn], 4)
    sy1.wait_recv()
    sy0.wait_recv()
    pick(syn, land.at[syn], 5)

    width_g = 8 * SLOT
    lane = lax.broadcasted_iota(jnp.int32, (8, width_g), 1)
    sel = jnp.where(lane // SLOT == lax.broadcasted_iota(jnp.int32, (8, width_g), 0), 1.0, 0.0)
    slot_id = (lax.broadcasted_iota(jnp.int32, (rows, width_g), 1) % SLOT).astype(F32)

    def spread(v):
        return lax.dot_general(v, sel, (((0,), (0,)), ((), ())), preferred_element_type=F32)[:rows]

    def gate_body(d, carry):
        rk = metal[d, 0:8, :]
        gt = metal[d, 8:16, :]
        hi = gt.astype(BF16).astype(F32)
        mid = (gt - hi).astype(BF16).astype(F32)
        lo = gt - hi - mid
        eq = spread(rk) == slot_id
        for q, part in enumerate((hi, mid, lo)):
            gv[d, q * rows:(q + 1) * rows, :] = jnp.where(eq, spread(part), 0.0).astype(BF16)
        return carry

    lax.fori_loop(0, nd, gate_body, 0)
    gcopy = pltpu.make_async_copy(gv, g_hbm, gsem)
    gcopy.start()

    fy.wait_recv()
    sd0 = rcopy(land.at[dg, hs(0)], land.at[dg, hs(0)], ss_s.at[5], ss_r.at[5], sib)
    sd0.start()
    fx.wait_recv()
    sd1 = rcopy(land.at[dg, hs(1)], land.at[dg, hs(1)], ss_s.at[6], ss_r.at[6], sib)
    sd1.start()
    pick(dg, land.at[dg], 6)
    sd0.wait_recv()
    sd1.wait_recv()
    pick(sdg, land.at[sdg], 7)
    for c in own_x + own_y + [own_s, fy, fx, sx0, sx1, sy0, sy1, sd0, sd1] + metas:
        c.wait_send()
    for c in outs[6:] + [ccopy, hcopy, gcopy]:
        c.wait()


def gather_call(x, route, gates, sg, su, nd):
    rows, d_model = x.shape
    ff = sg.shape[1]
    width = 256
    n_chunks = ff // width
    any_spec = pl.BlockSpec(memory_space=pl.ANY)
    vmem = pl.BlockSpec(memory_space=pltpu.VMEM)
    dma = pltpu.SemaphoreType.DMA
    return pl.pallas_call(
        gather_kernel,
        out_shape=(
            jax.ShapeDtypeStruct((8, nd, SLOT, d_model), BF16),
            jax.ShapeDtypeStruct((rows, ff), BF16),
            jax.ShapeDtypeStruct((nd, 8, 128), jnp.int32),
            jax.ShapeDtypeStruct((nd, 3 * rows, 8 * SLOT), BF16),
        ),
        in_specs=[vmem, vmem, vmem, any_spec, any_spec],
        out_specs=(any_spec,) * 4,
        scratch_shapes=[
            pltpu.VMEM((nd, rows, d_model), BF16),
            pltpu.VMEM((nd, 16, 128), F32),
            pltpu.VMEM((n_chunks, d_model, width), BF16),
            pltpu.VMEM((n_chunks, d_model, width), BF16),
            pltpu.VMEM((nd, 16, 128), F32),
            pltpu.VMEM((2, 8, SLOT, d_model), BF16),
            pltpu.VMEM((rows, ff), BF16),
            pltpu.VMEM((nd, 3 * rows, 8 * SLOT), BF16),
            pltpu.VMEM((nd, 8, 128), jnp.int32),
            dma((2, n_chunks)),
            dma((8,)), dma(()), dma(()), dma(()),
            dma((2,)), dma((2,)), dma((2,)), dma((2,)), dma((2,)), dma((2,)),
            dma((7,)), dma((7,)), dma((7,)), dma((7,)),
        ],
        compiler_params=pltpu.CompilerParams(
            collective_id=0, has_side_effects=True, vmem_limit_bytes=VMEM_LIMIT),
        name="gather_shared",
    )(x, route, gates, sg, su)


FEW = 16


def hidden_kernel(cnt, xg_hbm, w1_hbm, w3_hbm, h_hbm,
                  wb1, wb3, xfew, xall, hbuf, wsem, xsem, hsem):
    n_exp, d_model, ff = w1_hbm.shape
    nd = cnt.shape[0]
    depth = wb1.shape[0]
    bounds = [(c, min(256, ff - c)) for c in range(0, ff, 256)]
    cut = 3 * 256
    groups = ((0, cut, bounds[:3]), (cut, ff - cut, bounds[3:]))

    def wcopy(e, slot, j):
        c0, w, _ = groups[j]
        return (pltpu.make_async_copy(w1_hbm.at[e, :, c0:c0 + w], wb1.at[slot, :, c0:c0 + w], wsem.at[slot, 0, j]),
                pltpu.make_async_copy(w3_hbm.at[e, :, c0:c0 + w], wb3.at[slot, :, c0:c0 + w], wsem.at[slot, 1, j]))

    def few(e):
        top = cnt[0, e, 0]
        for d in range(1, nd):
            top = jnp.maximum(top, cnt[d, e, 0])
        return top <= FEW

    def few_copy(e):
        return pltpu.make_async_copy(xg_hbm.at[e, :, pl.ds(0, FEW)], xfew.at[e % 2], xsem.at[e % 2])

    def all_copy(e):
        return pltpu.make_async_copy(xg_hbm.at[e], xall.at[e % 2], xsem.at[e % 2])

    def rows_start(e):
        @pl.when(few(e))
        def _():
            few_copy(e).start()

        @pl.when(jnp.logical_not(few(e)))
        def _():
            all_copy(e).start()

    rows_start(0)
    for e in range(depth):
        for j in range(len(groups)):
            for c in wcopy(e, e, j):
                c.start()
        if e == 0:
            rows_start(1)
    hbuf[...] = jnp.zeros_like(hbuf)

    def hcopy(e):
        return pltpu.make_async_copy(hbuf.at[e % 2], h_hbm.at[e], hsem.at[e % 2])

    def hidden(rows_ref, slot, c0, w):
        m = rows_ref.shape[0] * rows_ref.shape[1]
        a = jnp.dot(rows_ref[...].reshape(m, d_model), wb1[slot, :, c0:c0 + w], preferred_element_type=F32)
        b = jnp.dot(rows_ref[...].reshape(m, d_model), wb3[slot, :, c0:c0 + w], preferred_element_type=F32)
        return (jax.nn.silu(a) * b).astype(BF16).reshape(rows_ref.shape[0], rows_ref.shape[1], w)

    def body(e, carry):
        slot = e % depth
        small = few(e)

        @pl.when(e >= 2)
        def _():
            hcopy(e - 2).wait()

        @pl.when(small)
        def _():
            few_copy(e).wait()
            for j, (_, _, cols) in enumerate(groups):
                for c in wcopy(e, slot, j):
                    c.wait()
                for c0, w in cols:
                    hbuf[e % 2, :, 0:FEW, c0:c0 + w] = hidden(xfew.at[e % 2], slot, c0, w)

        @pl.when(jnp.logical_not(small))
        def _():
            all_copy(e).wait()
            for j, (_, _, cols) in enumerate(groups):
                for c in wcopy(e, slot, j):
                    c.wait()
                for c0, w in cols:
                    hbuf[e % 2, :, :, c0:c0 + w] = hidden(xall.at[e % 2], slot, c0, w)

        hcopy(e).start()

        @pl.when(e + 2 < n_exp)
        def _():
            rows_start(e + 2)

        @pl.when(e + depth < n_exp)
        def _():
            for j in range(len(groups)):
                for c in wcopy(e + depth, slot, j):
                    c.start()
        return carry

    lax.fori_loop(0, n_exp, body, 0)
    hcopy(n_exp - 2).wait()
    hcopy(n_exp - 1).wait()


def hidden_call(cnt, xg, w1, w3):
    n_exp, d_model, ff = w1.shape
    nd = cnt.shape[0]
    depth = 3
    any_spec = pl.BlockSpec(memory_space=pl.ANY)
    dma = pltpu.SemaphoreType.DMA
    return pl.pallas_call(
        hidden_kernel,
        out_shape=jax.ShapeDtypeStruct((n_exp, nd, SLOT, ff), BF16),
        in_specs=[pl.BlockSpec(memory_space=pltpu.SMEM), any_spec, any_spec, any_spec],
        out_specs=any_spec,
        scratch_shapes=[
            pltpu.VMEM((depth, d_model, ff), BF16),
            pltpu.VMEM((depth, d_model, ff), BF16),
            pltpu.VMEM((2, nd, FEW, d_model), BF16),
            pltpu.VMEM((2, nd, SLOT, d_model), BF16),
            pltpu.VMEM((2, nd, SLOT, ff), BF16),
            dma((depth, 2, 2)), dma((2,)), dma((2,)),
        ],
        compiler_params=pltpu.CompilerParams(vmem_limit_bytes=VMEM_LIMIT),
        name="routed_hidden",
    )(cnt, xg, w1, w3)


def down_kernel(h_hbm, g_hbm, hsh_ref, w2_hbm, sd_hbm, y_ref,
                hv, gv, wb, sdb, ob, snd, kept, in0, in1, in2,
                hsem, gsem, wsem, dsem, s0s, s0r, s1s, s1r, s2s, s2r):
    me, core, sib, xn, yn, dg = neighbours()
    n_exp, full, ff = hv.shape
    nd = gv.shape[0]
    rows = gv.shape[1] // 3
    n_chunks = snd.shape[0]
    width = wb.shape[3]
    depth = wb.shape[0]
    hw = width // 2

    barrier = pltpu.get_barrier_semaphore()
    for dev in (sib, xn, yn):
        pl.semaphore_signal(barrier, inc=1, device_id={"ep": dev}, device_id_type=MESH)

    def wcopy(c, e):
        cols = pl.ds(pl.multiple_of(c * width, width), width)
        slot = c % depth
        return pltpu.make_async_copy(w2_hbm.at[e, :, cols], wb.at[slot, e], wsem.at[slot, e])

    def dcopy(c):
        cols = pl.ds(pl.multiple_of(c * width, width), width)
        return pltpu.make_async_copy(sd_hbm.at[:, cols], sdb.at[c], dsem.at[c])

    def hcopy(e):
        return pltpu.make_async_copy(h_hbm.at[e], hv.at[e], hsem.at[e])

    gcopy = pltpu.make_async_copy(g_hbm, gv, gsem)
    for e in range(n_exp):
        hcopy(e).start()
        wcopy(0, e).start()
    gcopy.start()
    for c in range(1, depth):
        for e in range(n_exp):
            wcopy(c, e).start()

    own_c, xn_c, yn_c, dg_c = me // 2, xn // 2, yn // 2, dg // 2
    orders = ((own_c, yn_c, xn_c, dg_c), (own_c, xn_c, yn_c, dg_c))
    first_hop = (xn, yn)
    second_hop = (yn, xn)

    def send0(c):
        return rcopy(snd.at[c], in0.at[c], s0s.at[c], s0r.at[c], sib)

    def send1(c, q):
        return rcopy(kept.at[c, q, pl.ds(2, 2)], in1.at[c, q], s1s.at[c, q], s1r.at[c, q], first_hop[q])

    def send2(c, q):
        return rcopy(kept.at[c, q, 1], in2.at[c, q], s2s.at[c, q], s2r.at[c, q], second_hop[q])

    def step0(c):
        send0(c).wait_recv()
        kept[c] = kept[c] + in0[c]

    def step1(c):
        for q in range(2):
            send1(c, q).wait_recv()
            kept[c, q, 0:2] = kept[c, q, 0:2] + in1[c, q]

    def step2(c):
        for q in range(2):
            send2(c, q).wait_recv()
            kept[c, q, 0] = kept[c, q, 0] + in2[c, q]

    def start1(c):
        send1(c, 0).start()
        send1(c, 1).start()

    def start2(c):
        send2(c, 0).start()
        send2(c, 1).start()

    def expert(c, e):
        out = jnp.dot(hv[e], wb[c % depth, e], preferred_element_type=F32)
        out = out.astype(BF16).astype(F32)
        ob[:, e] = out.reshape(nd, SLOT, width)

    def gated(d):
        o = ob[d].reshape(n_exp * SLOT, width).astype(BF16)
        r = jnp.dot(gv[d], o, preferred_element_type=F32)
        return r[0:rows] + r[rows:2 * rows] + r[2 * rows:3 * rows]

    def chunk(c, carry):
        for e0 in range(0, n_exp, 4):
            @pl.when(c == 0)
            def _():
                for e in range(e0, e0 + 4):
                    hcopy(e).wait()
            for e in range(e0, e0 + 4):
                wcopy(c, e).wait()
            for e in range(e0, e0 + 4):
                expert(c, e)

            @pl.when(c + depth < n_chunks)
            def _():
                for e in range(e0, e0 + 4):
                    wcopy(c + depth, e).start()

            if e0 == 0:
                @pl.when(c >= 1)
                def _():
                    step0(c - 1)

                @pl.when(c >= 3)
                def _():
                    step1(c - 3)

                @pl.when(c >= 1)
                def _():
                    start1(c - 1)

                @pl.when(c >= 3)
                def _():
                    start2(c - 3)

        dcopy(c).start()

        @pl.when(c == 0)
        def _():
            gcopy.wait()
        chips = (own_c, xn_c, yn_c, dg_c)
        where = ((0, 0), (2, 1), (1, 2), (3, 3))
        for chip, (p0, p1) in zip(chips, where):
            r = gated(2 * chip + 1 - core)
            snd[c, 0, p0] = r[:, 0:hw]
            snd[c, 1, p1] = r[:, hw:width]
        for chip, (p0, p1) in zip(chips, where):
            r = gated(2 * chip + core)
            kept[c, 0, p0] = r[:, 0:hw]
            kept[c, 1, p1] = r[:, hw:width]

        send0(c).start()
        return carry

    pl.semaphore_wait(barrier, 3)
    lax.fori_loop(0, n_chunks, chunk, 0)

    def shared(c):
        dcopy(c).wait()
        cols = pl.ds(pl.multiple_of(c * width, width), width)
        s = jnp.dot(hsh_ref[...], sdb[c], preferred_element_type=F32).astype(BF16)
        y_ref[:, cols] = s

    def shared_range(lo, hi):
        def body(c, carry):
            shared(c)
            return carry
        lax.fori_loop(lo, hi, body, 0)

    last = n_chunks - 1
    shared_range(0, 3)
    step0(last)
    step1(last - 2)
    start1(last)
    start2(last - 2)
    shared_range(3, 6)
    step1(last - 1)
    start2(last - 1)
    shared_range(6, n_chunks)
    step1(last)
    start2(last)

    def finish(c, carry):
        step2(c)
        for q in range(2):
            cols = pl.ds(pl.multiple_of(c * width + q * hw, hw), hw)
            y_ref[:, cols] = (y_ref[:, cols].astype(F32) + kept[c, q, 0]).astype(BF16)
        return carry

    lax.fori_loop(0, n_chunks, finish, 0)

    def drain(c, carry):
        send0(c).wait_send()
        for q in range(2):
            send1(c, q).wait_send()
            send2(c, q).wait_send()
        return carry

    lax.fori_loop(0, n_chunks, drain, 0)


def down_call(h, g, hsh, w2, sd):
    n_exp, full, ff = h.shape
    nd, rows3, width_g = g.shape
    rows = rows3 // 3
    d_model = w2.shape[2]
    width = 256
    n_chunks = d_model // width
    depth = 3
    hw = width // 2
    any_spec = pl.BlockSpec(memory_space=pl.ANY)
    vmem = pl.BlockSpec(memory_space=pltpu.VMEM)
    dma = pltpu.SemaphoreType.DMA
    return pl.pallas_call(
        down_kernel,
        out_shape=jax.ShapeDtypeStruct((rows, d_model), BF16),
        in_specs=[any_spec, any_spec, vmem, any_spec, any_spec],
        out_specs=vmem,
        scratch_shapes=[
            pltpu.VMEM((n_exp, full, ff), BF16),
            pltpu.VMEM((nd, rows3, width_g), BF16),
            pltpu.VMEM((depth, n_exp, ff, width), BF16),
            pltpu.VMEM((n_chunks, sd.shape[0], width), BF16),
            pltpu.VMEM((nd, n_exp, SLOT, width), F32),
            pltpu.VMEM((n_chunks, 2, 4, rows, hw), F32),
            pltpu.VMEM((n_chunks, 2, 4, rows, hw), F32),
            pltpu.VMEM((n_chunks, 2, 4, rows, hw), F32),
            pltpu.VMEM((n_chunks, 2, 2, rows, hw), F32),
            pltpu.VMEM((n_chunks, 2, rows, hw), F32),
            dma((n_exp,)), dma(()), dma((depth, n_exp)), dma((n_chunks,)),
            dma((n_chunks,)), dma((n_chunks,)),
            dma((n_chunks, 2)), dma((n_chunks, 2)), dma((n_chunks, 2)), dma((n_chunks, 2)),
        ],
        compiler_params=pltpu.CompilerParams(
            collective_id=1, has_side_effects=True, vmem_limit_bytes=VMEM_LIMIT),
        name="down_reduce",
    )(h, g, hsh, w2, sd)


def solution(mesh):
    nd = mesh.shape["ep"]

    def device_fn(x, route, gates, w_gate, w_up, w_down, sg, su, sd):
        xg, hsh, cnt, g = gather_call(x, route.T, gates.T, sg, su, nd)
        h = hidden_call(cnt, xg, w_gate, w_up)
        return down_call(h.reshape(h.shape[0], -1, h.shape[3]), g, hsh, w_down, sd)

    tok = P(("dp", "ep"), None)
    exp = P("ep", None, None)
    rep = P(None, None)
    return jax.shard_map(device_fn, mesh=mesh, in_specs=(tok, tok, tok, exp, exp, exp, rep, rep, rep),
                         out_specs=tok, check_vma=False)
```

```python
import functools

import jax
import jax.numpy as jnp
from jax import lax
from jax.experimental import pallas as pl
from jax.experimental.pallas import tpu as pltpu
from jax.sharding import PartitionSpec as P

MESH = pl.DeviceIdType.MESH
CAP = 36
SLOT = 40
VMEM_LIMIT = 67_000_000
H_BYTES = 8_000_000
PRE = 2
PRE_BYTES = 23_500_000
BF16 = jnp.bfloat16
F32 = jnp.float32


def neighbours():
    me = lax.axis_index("ep")
    core = me % 2
    xb = (me // 2) % 2
    yb = me // 4
    sib = me + 1 - 2 * core
    xn = me + 2 - 4 * xb
    yn = me + 4 - 8 * yb
    dg = yn + 2 - 4 * xb
    return me, core, sib, xn, yn, dg


def rcopy(src, dst, send, recv, dev):
    return pltpu.make_async_remote_copy(
        src_ref=src, dst_ref=dst, send_sem=send, recv_sem=recv,
        device_id={"ep": dev}, device_id_type=MESH)


def gather_kernel(x_ref, route_ref, gate_ref, sg_hbm, su_hbm, w1_hbm, w3_hbm,
                  xg_hbm, hsh_hbm, cnt_hbm, g_hbm, pre1, pre3,
                  land, meta_s, bg, bu, metal, stage, hsh, gv, cntv,
                  wsem, osem, psem, gsem, hsem, csem,
                  sx_s, sx_r, sy_s, sy_r, f_s, f_r, ss_s, ss_r, m_s, m_r):
    me, core, sib, xn, yn, dg = neighbours()
    sxn = xn + 1 - 2 * core
    syn = yn + 1 - 2 * core
    sdg = dg + 1 - 2 * core
    nd = land.shape[0]
    rows, d_model = x_ref.shape
    half = rows // 2
    ring = bg.shape[0]
    width = bg.shape[2]
    n_chunks = sg_hbm.shape[1] // width
    n_all = 8 * nd

    barrier = pltpu.get_barrier_semaphore()
    for r in range(1, nd):
        pl.semaphore_signal(barrier, inc=1, device_id={"ep": (me + r) % nd}, device_id_type=MESH)

    def wcopy(i):
        cols = pl.ds(pl.multiple_of(i * width, width), width)
        slot = i % ring
        return (pltpu.make_async_copy(sg_hbm.at[:, cols], bg.at[slot], wsem.at[0, slot]),
                pltpu.make_async_copy(su_hbm.at[:, cols], bu.at[slot], wsem.at[1, slot]))

    for i in range(ring):
        for c in wcopy(i):
            c.start()

    def pcopy(e):
        return (pltpu.make_async_copy(w1_hbm.at[e], pre1.at[e], psem.at[0, e]),
                pltpu.make_async_copy(w3_hbm.at[e], pre3.at[e], psem.at[1, e]))

    def prefetch(e):
        for c in pcopy(e):
            c.start()

    ids = lax.broadcasted_iota(jnp.int32, (n_all, rows), 0)
    mask = jnp.zeros((n_all, rows), F32)
    gmap = jnp.zeros((n_all, rows), F32)
    for k in range(route_ref.shape[0]):
        eq = route_ref[k:k + 1, :] == ids
        mask = mask + jnp.where(eq, 1.0, 0.0)
        gmap = gmap + jnp.where(eq, gate_ref[k:k + 1, :], 0.0)
    before = (lax.broadcasted_iota(jnp.int32, (rows, rows), 0)
              < lax.broadcasted_iota(jnp.int32, (rows, rows), 1))
    rank = jnp.dot(mask.astype(BF16), jnp.where(before, 1.0, 0.0).astype(BF16), preferred_element_type=F32)
    rank = jnp.where(mask > 0.0, rank, -1.0)
    fill = jnp.zeros((n_all, 128 - rows), F32)
    rank = jnp.concatenate([rank, fill - 1.0], axis=1)
    gmap = jnp.concatenate([gmap, fill], axis=1)
    for j in range(nd):
        meta_s[j, 0:8, :] = rank[8 * j:8 * j + 8]
        meta_s[j, 8:16, :] = gmap[8 * j:8 * j + 8]
    metal[me] = meta_s[me]

    def hs(h):
        return pl.ds(h * half, half)

    pl.semaphore_wait(barrier, nd - 1)
    metas = []
    for r in range(1, nd):
        dst = (me + r) % nd
        c = rcopy(meta_s.at[dst], metal.at[me], m_s.at[r - 1], m_r.at[r - 1], dst)
        c.start()
        metas.append(c)
    own_x = [rcopy(x_ref.at[hs(h)], land.at[me, hs(h)], sx_s.at[h], sx_r.at[h], xn) for h in range(2)]
    own_y = [rcopy(x_ref.at[hs(h)], land.at[me, hs(h)], sy_s.at[h], sy_r.at[h], yn) for h in range(2)]
    own_s = rcopy(x_ref, land.at[me], ss_s.at[0], ss_r.at[0], sib)
    own_x[0].start()
    own_y[1].start()
    own_x[1].start()
    own_y[0].start()
    own_s.start()

    def shared_range(lo, hi):
        def body(i, carry):
            for c in wcopy(i):
                c.wait()
            a = jnp.dot(x_ref[...], bg[i % ring], preferred_element_type=F32)
            b = jnp.dot(x_ref[...], bu[i % ring], preferred_element_type=F32)
            cols = pl.ds(pl.multiple_of(i * width, width), width)
            hsh[:, cols] = (jax.nn.silu(a) * b).astype(BF16)

            @pl.when(i + ring < n_chunks)
            def _():
                for c in wcopy(i + ring):
                    c.start()
            return carry
        lax.fori_loop(lo, hi, body, 0)

    shared_range(0, 2)
    prefetch(0)
    shared_range(2, n_chunks - 5)
    prefetch(1)

    for c in metas:
        c.wait_recv()

    for d in range(nd):
        n = jnp.sum(jnp.where(metal[d, 0:8, :] >= 0.0, 1.0, 0.0), axis=1, keepdims=True)
        cntv[d] = jnp.broadcast_to(n, (8, 128)).astype(jnp.int32)
    ccopy = pltpu.make_async_copy(cntv, cnt_hbm, csem)
    ccopy.start()

    def pick(d, x_rows, k):
        buf = k % 2
        if k >= 2:
            outs[k - 2].wait()
        slot = lax.broadcasted_iota(jnp.int32, (SLOT, rows), 0).astype(F32)
        sel = jnp.concatenate(
            [jnp.where(metal[d, e:e + 1, 0:rows] == slot, 1.0, 0.0) for e in range(8)], axis=0).astype(BF16)
        for c0 in range(0, d_model, 512):
            r = jnp.dot(sel, x_rows[:, c0:c0 + 512], preferred_element_type=F32)
            stage[buf, :, :, c0:c0 + 512] = r.astype(BF16).reshape(8, SLOT, 512)
        c = pltpu.make_async_copy(stage.at[buf], xg_hbm.at[:, d], osem.at[k])
        c.start()
        outs.append(c)

    outs = []
    pick(me, x_ref, 0)
    own_s.wait_recv()
    pick(sib, land.at[sib], 1)

    own_x[0].wait_recv()
    fy = rcopy(land.at[xn, hs(0)], land.at[xn, hs(0)], f_s.at[0], f_r.at[0], yn)
    fy.start()
    sx0 = rcopy(land.at[xn, hs(0)], land.at[xn, hs(0)], ss_s.at[1], ss_r.at[1], sib)
    sx0.start()
    own_y[1].wait_recv()
    fx = rcopy(land.at[yn, hs(1)], land.at[yn, hs(1)], f_s.at[1], f_r.at[1], xn)
    fx.start()
    sy1 = rcopy(land.at[yn, hs(1)], land.at[yn, hs(1)], ss_s.at[2], ss_r.at[2], sib)
    sy1.start()

    shared_range(n_chunks - 5, n_chunks)
    for e in range(2, pre1.shape[0]):
        prefetch(e)
    hcopy = pltpu.make_async_copy(hsh, hsh_hbm, hsem)
    hcopy.start()

    own_x[1].wait_recv()
    sx1 = rcopy(land.at[xn, hs(1)], land.at[xn, hs(1)], ss_s.at[3], ss_r.at[3], sib)
    sx1.start()
    own_y[0].wait_recv()
    sy0 = rcopy(land.at[yn, hs(0)], land.at[yn, hs(0)], ss_s.at[4], ss_r.at[4], sib)
    sy0.start()
    pick(xn, land.at[xn], 2)
    pick(yn, land.at[yn], 3)
    sx0.wait_recv()
    sx1.wait_recv()
    pick(sxn, land.at[sxn], 4)
    sy1.wait_recv()
    sy0.wait_recv()
    pick(syn, land.at[syn], 5)

    width_g = 8 * SLOT
    lane = lax.broadcasted_iota(jnp.int32, (8, width_g), 1)
    sel = jnp.where(lane // SLOT == lax.broadcasted_iota(jnp.int32, (8, width_g), 0), 1.0, 0.0)
    slot_id = (lax.broadcasted_iota(jnp.int32, (rows, width_g), 1) % SLOT).astype(F32)

    def spread(v):
        return lax.dot_general(v, sel, (((0,), (0,)), ((), ())), preferred_element_type=F32)[:rows]

    def gate_body(d, carry):
        rk = metal[d, 0:8, :]
        gt = metal[d, 8:16, :]
        hi = gt.astype(BF16).astype(F32)
        mid = (gt - hi).astype(BF16).astype(F32)
        lo = gt - hi - mid
        eq = spread(rk) == slot_id
        for q, part in enumerate((hi, mid, lo)):
            gv[d, q * rows:(q + 1) * rows, :] = jnp.where(eq, spread(part), 0.0).astype(BF16)
        return carry

    lax.fori_loop(0, nd, gate_body, 0)
    gcopy = pltpu.make_async_copy(gv, g_hbm, gsem)
    gcopy.start()

    fy.wait_recv()
    sd0 = rcopy(land.at[dg, hs(0)], land.at[dg, hs(0)], ss_s.at[5], ss_r.at[5], sib)
    sd0.start()
    fx.wait_recv()
    sd1 = rcopy(land.at[dg, hs(1)], land.at[dg, hs(1)], ss_s.at[6], ss_r.at[6], sib)
    sd1.start()
    pick(dg, land.at[dg], 6)
    sd0.wait_recv()
    sd1.wait_recv()
    pick(sdg, land.at[sdg], 7)
    for c in own_x + own_y + [own_s, fy, fx, sx0, sx1, sy0, sy1, sd0, sd1] + metas:
        c.wait_send()
    for c in outs[6:] + [ccopy, hcopy, gcopy]:
        c.wait()
    for e in range(pre1.shape[0]):
        for c in pcopy(e):
            c.wait()


def gather_call(x, route, gates, sg, su, w1, w3, nd):
    rows, d_model = x.shape
    ff = sg.shape[1]
    width = 256
    ring = 4
    any_spec = pl.BlockSpec(memory_space=pl.ANY)
    vmem = pl.BlockSpec(memory_space=pltpu.VMEM)
    dma = pltpu.SemaphoreType.DMA
    return pl.pallas_call(
        gather_kernel,
        out_shape=(
            jax.ShapeDtypeStruct((8, nd, SLOT, d_model), BF16),
            jax.ShapeDtypeStruct((rows, ff), BF16),
            jax.ShapeDtypeStruct((nd, 8, 128), jnp.int32),
            jax.ShapeDtypeStruct((nd, 3 * rows, 8 * SLOT), BF16),
            pltpu.VMEM((PRE,) + w1.shape[1:], BF16),
            pltpu.VMEM((PRE,) + w3.shape[1:], BF16),
        ),
        in_specs=[vmem, vmem, vmem] + [any_spec] * 4,
        out_specs=(pl.BlockSpec(memory_space=pltpu.HBM),) * 4 + (vmem, vmem),
        scratch_shapes=[
            pltpu.VMEM((nd, rows, d_model), BF16),
            pltpu.VMEM((nd, 16, 128), F32),
            pltpu.VMEM((ring, d_model, width), BF16),
            pltpu.VMEM((ring, d_model, width), BF16),
            pltpu.VMEM((nd, 16, 128), F32),
            pltpu.VMEM((2, 8, SLOT, d_model), BF16),
            pltpu.VMEM((rows, ff), BF16),
            pltpu.VMEM((nd, 3 * rows, 8 * SLOT), BF16),
            pltpu.VMEM((nd, 8, 128), jnp.int32),
            dma((2, ring)),
            dma((8,)), dma((2, PRE)), dma(()), dma(()), dma(()),
            dma((2,)), dma((2,)), dma((2,)), dma((2,)), dma((2,)), dma((2,)),
            dma((7,)), dma((7,)), dma((7,)), dma((7,)),
        ],
        compiler_params=pltpu.CompilerParams(
            collective_id=0, has_side_effects=True, vmem_limit_bytes=36_000_000),
        name="gather_shared",
    )(x, route, gates, sg, su, w1, w3)


FEW = 16


def hidden_kernel(cnt, xg_hbm, w1_hbm, w3_hbm, pre1, pre3, h_ref,
                  wb1, wb3, xfew, xall, wsem, xsem):
    n_exp, d_model, ff = w1_hbm.shape
    nd = cnt.shape[0]
    depth = wb1.shape[0]
    first = pre1.shape[0]
    bounds = [(c, min(256, ff - c)) for c in range(0, ff, 256)]
    cut = 3 * 256
    groups = ((0, cut, bounds[:3]), (cut, ff - cut, bounds[3:]))

    def wcopy(e, slot, j):
        c0, w, _ = groups[j]
        return (pltpu.make_async_copy(w1_hbm.at[e, :, c0:c0 + w], wb1.at[slot, :, c0:c0 + w], wsem.at[slot, 0, j]),
                pltpu.make_async_copy(w3_hbm.at[e, :, c0:c0 + w], wb3.at[slot, :, c0:c0 + w], wsem.at[slot, 1, j]))

    def few(e):
        top = cnt[0, e, 0]
        for d in range(1, nd):
            top = jnp.maximum(top, cnt[d, e, 0])
        return top <= FEW

    def few_copy(e):
        return pltpu.make_async_copy(xg_hbm.at[e, :, pl.ds(0, FEW)], xfew.at[e % 2], xsem.at[e % 2])

    def all_copy(e):
        return pltpu.make_async_copy(xg_hbm.at[e], xall.at[e % 2], xsem.at[e % 2])

    def rows_start(e):
        @pl.when(few(e))
        def _():
            few_copy(e).start()

        @pl.when(jnp.logical_not(few(e)))
        def _():
            all_copy(e).start()

    rows_start(0)
    rows_start(1)
    for e in range(first, first + depth):
        for j in range(len(groups)):
            for c in wcopy(e, e % depth, j):
                c.start()
    h_ref[...] = jnp.zeros_like(h_ref)

    def hidden(rows_ref, up, gate, c0, w):
        m = rows_ref.shape[0] * rows_ref.shape[1]
        a = jnp.dot(rows_ref[...].reshape(m, d_model), gate[:, c0:c0 + w], preferred_element_type=F32)
        b = jnp.dot(rows_ref[...].reshape(m, d_model), up[:, c0:c0 + w], preferred_element_type=F32)
        return (jax.nn.silu(a) * b).astype(BF16).reshape(rows_ref.shape[0], rows_ref.shape[1], w)

    def expert(e, gate, up, wait):
        small = few(e)

        @pl.when(small)
        def _():
            few_copy(e).wait()
            for j, (_, _, cols) in enumerate(groups):
                wait(j)
                for c0, w in cols:
                    h_ref[e, :, 0:FEW, c0:c0 + w] = hidden(xfew.at[e % 2], up, gate, c0, w)

        @pl.when(jnp.logical_not(small))
        def _():
            all_copy(e).wait()
            for j, (_, _, cols) in enumerate(groups):
                wait(j)
                for c0, w in cols:
                    h_ref[e, :, :, c0:c0 + w] = hidden(xall.at[e % 2], up, gate, c0, w)

        @pl.when(e + 2 < n_exp)
        def _():
            rows_start(e + 2)

    def early(e, carry):
        expert(e, pre1.at[e], pre3.at[e], lambda j: None)
        return carry

    def late(e, carry):
        slot = e % depth

        def wait(j):
            for c in wcopy(e, slot, j):
                c.wait()

        expert(e, wb1.at[slot], wb3.at[slot], wait)

        @pl.when(e + depth < n_exp)
        def _():
            for j in range(len(groups)):
                for c in wcopy(e + depth, slot, j):
                    c.start()
        return carry

    lax.fori_loop(0, first, early, 0)
    lax.fori_loop(first, n_exp, late, 0)


def hidden_call(cnt, xg, w1, w3, pre1, pre3):
    n_exp, d_model, ff = w1.shape
    nd = cnt.shape[0]
    depth = 2
    any_spec = pl.BlockSpec(memory_space=pl.ANY)
    vmem = pl.BlockSpec(memory_space=pltpu.VMEM)
    dma = pltpu.SemaphoreType.DMA
    return pl.pallas_call(
        hidden_kernel,
        out_shape=pltpu.VMEM((n_exp, nd, SLOT, ff), BF16),
        in_specs=[pl.BlockSpec(memory_space=pltpu.SMEM), any_spec, any_spec, any_spec, vmem, vmem],
        out_specs=vmem,
        scratch_shapes=[
            pltpu.VMEM((depth, d_model, ff), BF16),
            pltpu.VMEM((depth, d_model, ff), BF16),
            pltpu.VMEM((2, nd, FEW, d_model), BF16),
            pltpu.VMEM((2, nd, SLOT, d_model), BF16),
            dma((depth, 2, 2)), dma((2,)),
        ],
        compiler_params=pltpu.CompilerParams(vmem_limit_bytes=36_000_000),
        name="routed_hidden",
    )(cnt, xg, w1, w3, pltpu.with_memory_space_constraint(pre1, pltpu.VMEM),
      pltpu.with_memory_space_constraint(pre3, pltpu.VMEM))


def down_kernel(hv, g_hbm, hsh_ref, w2_hbm, sd_hbm, y_ref,
                gv, wb, sdb, ob, snd, kept, in0, in1, in2,
                gsem, wsem, dsem, s0s, s0r, s1s, s1r, s2s, s2r):
    me, core, sib, xn, yn, dg = neighbours()
    n_exp, full, ff = hv.shape
    nd = gv.shape[0]
    rows = gv.shape[1] // 3
    n_chunks = snd.shape[0]
    width = wb.shape[3]
    depth = wb.shape[0]
    hw = width // 2

    barrier = pltpu.get_barrier_semaphore()
    for dev in (sib, xn, yn):
        pl.semaphore_signal(barrier, inc=1, device_id={"ep": dev}, device_id_type=MESH)

    def wcopy(c, e):
        cols = pl.ds(pl.multiple_of(c * width, width), width)
        slot = c % depth
        return pltpu.make_async_copy(w2_hbm.at[e, :, cols], wb.at[slot, e], wsem.at[slot, e])

    def dcopy(c):
        cols = pl.ds(pl.multiple_of(c * width, width), width)
        return pltpu.make_async_copy(sd_hbm.at[:, cols], sdb.at[c], dsem.at[c])

    gcopy = pltpu.make_async_copy(g_hbm, gv, gsem)
    for e in range(n_exp):
        wcopy(0, e).start()
    gcopy.start()
    for c in range(1, depth):
        for e in range(n_exp):
            wcopy(c, e).start()

    own_c, xn_c, yn_c, dg_c = me // 2, xn // 2, yn // 2, dg // 2
    orders = ((own_c, yn_c, xn_c, dg_c), (own_c, xn_c, yn_c, dg_c))
    first_hop = (xn, yn)
    second_hop = (yn, xn)

    def send0(c):
        return rcopy(snd.at[c], in0.at[c], s0s.at[c], s0r.at[c], sib)

    def send1(c, q):
        return rcopy(kept.at[c, q, pl.ds(2, 2)], in1.at[c, q], s1s.at[c, q], s1r.at[c, q], first_hop[q])

    def send2(c, q):
        return rcopy(kept.at[c, q, 1], in2.at[c, q], s2s.at[c, q], s2r.at[c, q], second_hop[q])

    def step0(c):
        send0(c).wait_recv()
        kept[c] = kept[c] + in0[c]

    def step1(c):
        for q in range(2):
            send1(c, q).wait_recv()
            kept[c, q, 0:2] = kept[c, q, 0:2] + in1[c, q]

    def step2(c):
        for q in range(2):
            send2(c, q).wait_recv()
            kept[c, q, 0] = kept[c, q, 0] + in2[c, q]

    def start1(c):
        send1(c, 0).start()
        send1(c, 1).start()

    def start2(c):
        send2(c, 0).start()
        send2(c, 1).start()

    def expert(c, e):
        out = jnp.dot(hv[e], wb[c % depth, e], preferred_element_type=F32)
        out = out.astype(BF16).astype(F32)
        ob[:, e] = out.reshape(nd, SLOT, width)

    def gated(d):
        o = ob[d].reshape(n_exp * SLOT, width).astype(BF16)
        r = jnp.dot(gv[d], o, preferred_element_type=F32)
        return r[0:rows] + r[rows:2 * rows] + r[2 * rows:3 * rows]

    def chunk(c, carry):
        for e0 in range(0, n_exp, 4):
            for e in range(e0, e0 + 4):
                wcopy(c, e).wait()
            for e in range(e0, e0 + 4):
                expert(c, e)

            @pl.when(c + depth < n_chunks)
            def _():
                for e in range(e0, e0 + 4):
                    wcopy(c + depth, e).start()

            if e0 == 0:
                @pl.when(c >= 1)
                def _():
                    step0(c - 1)

                @pl.when(c >= 3)
                def _():
                    step1(c - 3)

                @pl.when(c >= 1)
                def _():
                    start1(c - 1)

                @pl.when(c >= 3)
                def _():
                    start2(c - 3)

        dcopy(c).start()

        @pl.when(c == 0)
        def _():
            gcopy.wait()
        chips = (own_c, xn_c, yn_c, dg_c)
        where = ((0, 0), (2, 1), (1, 2), (3, 3))
        for chip, (p0, p1) in zip(chips, where):
            r = gated(2 * chip + 1 - core)
            snd[c, 0, p0] = r[:, 0:hw]
            snd[c, 1, p1] = r[:, hw:width]
        for chip, (p0, p1) in zip(chips, where):
            r = gated(2 * chip + core)
            kept[c, 0, p0] = r[:, 0:hw]
            kept[c, 1, p1] = r[:, hw:width]

        send0(c).start()
        return carry

    pl.semaphore_wait(barrier, 3)
    lax.fori_loop(0, n_chunks, chunk, 0)

    def shared(c):
        dcopy(c).wait()
        cols = pl.ds(pl.multiple_of(c * width, width), width)
        s = jnp.dot(hsh_ref[...], sdb[c], preferred_element_type=F32).astype(BF16)
        y_ref[:, cols] = s

    def shared_range(lo, hi):
        def body(c, carry):
            shared(c)
            return carry
        lax.fori_loop(lo, hi, body, 0)

    last = n_chunks - 1
    shared_range(0, 3)
    step0(last)
    step1(last - 2)
    start1(last)
    start2(last - 2)
    shared_range(3, 6)
    step1(last - 1)
    start2(last - 1)
    shared_range(6, n_chunks)
    step1(last)
    start2(last)

    def finish(c, carry):
        step2(c)
        for q in range(2):
            cols = pl.ds(pl.multiple_of(c * width + q * hw, hw), hw)
            y_ref[:, cols] = (y_ref[:, cols].astype(F32) + kept[c, q, 0]).astype(BF16)
        return carry

    lax.fori_loop(0, n_chunks, finish, 0)

    def drain(c, carry):
        send0(c).wait_send()
        for q in range(2):
            send1(c, q).wait_send()
            send2(c, q).wait_send()
        return carry

    lax.fori_loop(0, n_chunks, drain, 0)


def down_call(h, g, hsh, w2, sd):
    n_exp, full, ff = h.shape
    nd, rows3, width_g = g.shape
    rows = rows3 // 3
    d_model = w2.shape[2]
    width = 256
    n_chunks = d_model // width
    depth = 3
    hw = width // 2
    any_spec = pl.BlockSpec(memory_space=pl.ANY)
    vmem = pl.BlockSpec(memory_space=pltpu.VMEM)
    dma = pltpu.SemaphoreType.DMA
    return pl.pallas_call(
        down_kernel,
        out_shape=jax.ShapeDtypeStruct((rows, d_model), BF16),
        in_specs=[vmem, any_spec, vmem, any_spec, any_spec],
        out_specs=vmem,
        scratch_shapes=[
            pltpu.VMEM((nd, rows3, width_g), BF16),
            pltpu.VMEM((depth, n_exp, ff, width), BF16),
            pltpu.VMEM((n_chunks, sd.shape[0], width), BF16),
            pltpu.VMEM((nd, n_exp, SLOT, width), F32),
            pltpu.VMEM((n_chunks, 2, 4, rows, hw), F32),
            pltpu.VMEM((n_chunks, 2, 4, rows, hw), F32),
            pltpu.VMEM((n_chunks, 2, 4, rows, hw), F32),
            pltpu.VMEM((n_chunks, 2, 2, rows, hw), F32),
            pltpu.VMEM((n_chunks, 2, rows, hw), F32),
            dma(()), dma((depth, n_exp)), dma((n_chunks,)),
            dma((n_chunks,)), dma((n_chunks,)),
            dma((n_chunks, 2)), dma((n_chunks, 2)), dma((n_chunks, 2)), dma((n_chunks, 2)),
        ],
        compiler_params=pltpu.CompilerParams(
            collective_id=1, has_side_effects=True, vmem_limit_bytes=VMEM_LIMIT - H_BYTES),
        name="down_reduce",
    )(pltpu.with_memory_space_constraint(h, pltpu.VMEM), g, hsh, w2, sd)


def solution(mesh):
    nd = mesh.shape["ep"]

    def device_fn(x, route, gates, w_gate, w_up, w_down, sg, su, sd):
        xg, hsh, cnt, g, pre1, pre3 = gather_call(x, route.T, gates.T, sg, su, w_gate, w_up, nd)
        h = hidden_call(cnt, xg, w_gate, w_up, pre1, pre3)
        return down_call(h.reshape(h.shape[0], -1, h.shape[3]), g, hsh, w_down, sd)

    tok = P(("dp", "ep"), None)
    exp = P("ep", None, None)
    rep = P(None, None)
    return jax.shard_map(device_fn, mesh=mesh, in_specs=(tok, tok, tok, exp, exp, exp, rep, rep, rep),
                         out_specs=tok, check_vma=False)
```

```python
import functools

import jax
import jax.numpy as jnp
from jax import lax
from jax.experimental import pallas as pl
from jax.experimental.pallas import tpu as pltpu
from jax.sharding import PartitionSpec as P

MESH = pl.DeviceIdType.MESH
CAP = 36
SLOT = 40
VMEM_LIMIT = 67_000_000
H_BYTES = 10_500_000
CHUNK = 256
EARLY = 2
PRE = 2
PRE_BYTES = 23_500_000
BF16 = jnp.bfloat16
F32 = jnp.float32


def neighbours():
    me = lax.axis_index("ep")
    core = me % 2
    xb = (me // 2) % 2
    yb = me // 4
    sib = me + 1 - 2 * core
    xn = me + 2 - 4 * xb
    yn = me + 4 - 8 * yb
    dg = yn + 2 - 4 * xb
    return me, core, sib, xn, yn, dg


def rcopy(src, dst, send, recv, dev):
    return pltpu.make_async_remote_copy(
        src_ref=src, dst_ref=dst, send_sem=send, recv_sem=recv,
        device_id={"ep": dev}, device_id_type=MESH)


def gather_kernel(x_ref, route_ref, gate_ref, sg_hbm, su_hbm, w1_hbm, w3_hbm,
                  xg_hbm, hsh_hbm, cnt_hbm, g_hbm, pre1, pre3,
                  land, meta_s, bg, bu, metal, stage, hsh, gv, cntv,
                  wsem, osem, psem, gsem, hsem, csem,
                  sx_s, sx_r, sy_s, sy_r, f_s, f_r, ss_s, ss_r, m_s, m_r):
    me, core, sib, xn, yn, dg = neighbours()
    sxn = xn + 1 - 2 * core
    syn = yn + 1 - 2 * core
    sdg = dg + 1 - 2 * core
    nd = land.shape[0]
    rows, d_model = x_ref.shape
    half = rows // 2
    ring = bg.shape[0]
    width = bg.shape[2]
    n_chunks = sg_hbm.shape[1] // width
    n_all = 8 * nd

    barrier = pltpu.get_barrier_semaphore()
    for r in range(1, nd):
        pl.semaphore_signal(barrier, inc=1, device_id={"ep": (me + r) % nd}, device_id_type=MESH)

    def wcopy(i):
        cols = pl.ds(pl.multiple_of(i * width, width), width)
        slot = i % ring
        return (pltpu.make_async_copy(sg_hbm.at[:, cols], bg.at[slot], wsem.at[0, slot]),
                pltpu.make_async_copy(su_hbm.at[:, cols], bu.at[slot], wsem.at[1, slot]))

    for i in range(ring):
        for c in wcopy(i):
            c.start()

    def pcopy(e):
        return (pltpu.make_async_copy(w1_hbm.at[e], pre1.at[e], psem.at[0, e]),
                pltpu.make_async_copy(w3_hbm.at[e], pre3.at[e], psem.at[1, e]))

    def prefetch(e):
        for c in pcopy(e):
            c.start()

    ids = lax.broadcasted_iota(jnp.int32, (n_all, rows), 0)
    mask = jnp.zeros((n_all, rows), F32)
    gmap = jnp.zeros((n_all, rows), F32)
    for k in range(route_ref.shape[0]):
        eq = route_ref[k:k + 1, :] == ids
        mask = mask + jnp.where(eq, 1.0, 0.0)
        gmap = gmap + jnp.where(eq, gate_ref[k:k + 1, :], 0.0)
    before = (lax.broadcasted_iota(jnp.int32, (rows, rows), 0)
              < lax.broadcasted_iota(jnp.int32, (rows, rows), 1))
    rank = jnp.dot(mask.astype(BF16), jnp.where(before, 1.0, 0.0).astype(BF16), preferred_element_type=F32)
    rank = jnp.where(mask > 0.0, rank, -1.0)
    fill = jnp.zeros((n_all, 128 - rows), F32)
    rank = jnp.concatenate([rank, fill - 1.0], axis=1)
    gmap = jnp.concatenate([gmap, fill], axis=1)
    for j in range(nd):
        meta_s[j, 0:8, :] = rank[8 * j:8 * j + 8]
        meta_s[j, 8:16, :] = gmap[8 * j:8 * j + 8]
    metal[me] = meta_s[me]

    def hs(h):
        return pl.ds(h * half, half)

    pl.semaphore_wait(barrier, nd - 1)
    metas = []
    for r in range(1, nd):
        dst = (me + r) % nd
        c = rcopy(meta_s.at[dst], metal.at[me], m_s.at[r - 1], m_r.at[r - 1], dst)
        c.start()
        metas.append(c)
    own_x = [rcopy(x_ref.at[hs(h)], land.at[me, hs(h)], sx_s.at[h], sx_r.at[h], xn) for h in range(2)]
    own_y = [rcopy(x_ref.at[hs(h)], land.at[me, hs(h)], sy_s.at[h], sy_r.at[h], yn) for h in range(2)]
    own_s = rcopy(x_ref, land.at[me], ss_s.at[0], ss_r.at[0], sib)
    own_x[0].start()
    own_y[1].start()
    own_x[1].start()
    own_y[0].start()
    own_s.start()

    def shared_range(lo, hi):
        def body(i, carry):
            for c in wcopy(i):
                c.wait()
            a = jnp.dot(x_ref[...], bg[i % ring], preferred_element_type=F32)
            b = jnp.dot(x_ref[...], bu[i % ring], preferred_element_type=F32)
            cols = pl.ds(pl.multiple_of(i * width, width), width)
            hsh[:, cols] = (jax.nn.silu(a) * b).astype(BF16)

            @pl.when(i + ring < n_chunks)
            def _():
                for c in wcopy(i + ring):
                    c.start()
            return carry
        lax.fori_loop(lo, hi, body, 0)

    shared_range(0, 2)
    prefetch(0)
    shared_range(2, n_chunks - 5)
    prefetch(1)

    for c in metas:
        c.wait_recv()

    for d in range(nd):
        n = jnp.sum(jnp.where(metal[d, 0:8, :] >= 0.0, 1.0, 0.0), axis=1, keepdims=True)
        cntv[d] = jnp.broadcast_to(n, (8, 128)).astype(jnp.int32)
    ccopy = pltpu.make_async_copy(cntv, cnt_hbm, csem)
    ccopy.start()

    def pick(d, x_rows, k):
        buf = k % 2
        if k >= 2:
            outs[k - 2].wait()
        slot = lax.broadcasted_iota(jnp.int32, (SLOT, rows), 0).astype(F32)
        sel = jnp.concatenate(
            [jnp.where(metal[d, e:e + 1, 0:rows] == slot, 1.0, 0.0) for e in range(8)], axis=0).astype(BF16)
        for c0 in range(0, d_model, 512):
            r = jnp.dot(sel, x_rows[:, c0:c0 + 512], preferred_element_type=F32)
            stage[buf, :, :, c0:c0 + 512] = r.astype(BF16).reshape(8, SLOT, 512)
        c = pltpu.make_async_copy(stage.at[buf], xg_hbm.at[:, d], osem.at[k])
        c.start()
        outs.append(c)

    outs = []
    pick(me, x_ref, 0)
    own_s.wait_recv()
    pick(sib, land.at[sib], 1)

    own_x[0].wait_recv()
    fy = rcopy(land.at[xn, hs(0)], land.at[xn, hs(0)], f_s.at[0], f_r.at[0], yn)
    fy.start()
    sx0 = rcopy(land.at[xn, hs(0)], land.at[xn, hs(0)], ss_s.at[1], ss_r.at[1], sib)
    sx0.start()
    own_y[1].wait_recv()
    fx = rcopy(land.at[yn, hs(1)], land.at[yn, hs(1)], f_s.at[1], f_r.at[1], xn)
    fx.start()
    sy1 = rcopy(land.at[yn, hs(1)], land.at[yn, hs(1)], ss_s.at[2], ss_r.at[2], sib)
    sy1.start()

    shared_range(n_chunks - 5, n_chunks)
    for e in range(2, pre1.shape[0]):
        prefetch(e)
    hcopy = pltpu.make_async_copy(hsh, hsh_hbm, hsem)
    hcopy.start()

    own_x[1].wait_recv()
    sx1 = rcopy(land.at[xn, hs(1)], land.at[xn, hs(1)], ss_s.at[3], ss_r.at[3], sib)
    sx1.start()
    own_y[0].wait_recv()
    sy0 = rcopy(land.at[yn, hs(0)], land.at[yn, hs(0)], ss_s.at[4], ss_r.at[4], sib)
    sy0.start()
    pick(xn, land.at[xn], 2)
    pick(yn, land.at[yn], 3)
    sx0.wait_recv()
    sx1.wait_recv()
    pick(sxn, land.at[sxn], 4)
    sy1.wait_recv()
    sy0.wait_recv()
    pick(syn, land.at[syn], 5)

    width_g = 8 * SLOT
    lane = lax.broadcasted_iota(jnp.int32, (8, width_g), 1)
    sel = jnp.where(lane // SLOT == lax.broadcasted_iota(jnp.int32, (8, width_g), 0), 1.0, 0.0)
    slot_id = (lax.broadcasted_iota(jnp.int32, (rows, width_g), 1) % SLOT).astype(F32)

    def spread(v):
        return lax.dot_general(v, sel, (((0,), (0,)), ((), ())), preferred_element_type=F32)[:rows]

    def gate_body(d, carry):
        rk = metal[d, 0:8, :]
        gt = metal[d, 8:16, :]
        hi = gt.astype(BF16).astype(F32)
        mid = (gt - hi).astype(BF16).astype(F32)
        lo = gt - hi - mid
        eq = spread(rk) == slot_id
        for q, part in enumerate((hi, mid, lo)):
            gv[d, q * rows:(q + 1) * rows, :] = jnp.where(eq, spread(part), 0.0).astype(BF16)
        return carry

    lax.fori_loop(0, nd, gate_body, 0)
    gcopy = pltpu.make_async_copy(gv, g_hbm, gsem)
    gcopy.start()

    fy.wait_recv()
    sd0 = rcopy(land.at[dg, hs(0)], land.at[dg, hs(0)], ss_s.at[5], ss_r.at[5], sib)
    sd0.start()
    fx.wait_recv()
    sd1 = rcopy(land.at[dg, hs(1)], land.at[dg, hs(1)], ss_s.at[6], ss_r.at[6], sib)
    sd1.start()
    pick(dg, land.at[dg], 6)
    sd0.wait_recv()
    sd1.wait_recv()
    pick(sdg, land.at[sdg], 7)
    for c in own_x + own_y + [own_s, fy, fx, sx0, sx1, sy0, sy1, sd0, sd1] + metas:
        c.wait_send()
    for c in outs[6:] + [ccopy, hcopy, gcopy]:
        c.wait()
    for e in range(pre1.shape[0]):
        for c in pcopy(e):
            c.wait()


def gather_call(x, route, gates, sg, su, w1, w3, nd):
    rows, d_model = x.shape
    ff = sg.shape[1]
    width = 256
    ring = 4
    any_spec = pl.BlockSpec(memory_space=pl.ANY)
    vmem = pl.BlockSpec(memory_space=pltpu.VMEM)
    dma = pltpu.SemaphoreType.DMA
    return pl.pallas_call(
        gather_kernel,
        out_shape=(
            jax.ShapeDtypeStruct((8, nd, SLOT, d_model), BF16),
            jax.ShapeDtypeStruct((rows, ff), BF16),
            jax.ShapeDtypeStruct((nd, 8, 128), jnp.int32),
            jax.ShapeDtypeStruct((nd, 3 * rows, 8 * SLOT), BF16),
            pltpu.VMEM((PRE,) + w1.shape[1:], BF16),
            pltpu.VMEM((PRE,) + w3.shape[1:], BF16),
        ),
        in_specs=[vmem, vmem, vmem] + [any_spec] * 4,
        out_specs=(pl.BlockSpec(memory_space=pltpu.HBM),) * 4 + (vmem, vmem),
        scratch_shapes=[
            pltpu.VMEM((nd, rows, d_model), BF16),
            pltpu.VMEM((nd, 16, 128), F32),
            pltpu.VMEM((ring, d_model, width), BF16),
            pltpu.VMEM((ring, d_model, width), BF16),
            pltpu.VMEM((nd, 16, 128), F32),
            pltpu.VMEM((2, 8, SLOT, d_model), BF16),
            pltpu.VMEM((rows, ff), BF16),
            pltpu.VMEM((nd, 3 * rows, 8 * SLOT), BF16),
            pltpu.VMEM((nd, 8, 128), jnp.int32),
            dma((2, ring)),
            dma((8,)), dma((2, PRE)), dma(()), dma(()), dma(()),
            dma((2,)), dma((2,)), dma((2,)), dma((2,)), dma((2,)), dma((2,)),
            dma((7,)), dma((7,)), dma((7,)), dma((7,)),
        ],
        compiler_params=pltpu.CompilerParams(
            collective_id=0, has_side_effects=True, vmem_limit_bytes=33_800_000),
        name="gather_shared",
    )(x, route, gates, sg, su, w1, w3)


FEW = 16


def hidden_kernel(cnt, xg_hbm, w1_hbm, w3_hbm, w2_hbm, pre1, pre3, h_ref,
                  wb1, wb3, wb2, xfew, xall, wsem, dsem, xsem):
    n_exp, d_model, ff = w1_hbm.shape
    nd = cnt.shape[0]
    depth = wb1.shape[0]
    first = pre1.shape[0]
    bounds = [(c, min(256, ff - c)) for c in range(0, ff, 256)]
    cut = 3 * 256
    groups = ((0, cut, bounds[:3]), (cut, ff - cut, bounds[3:]))

    def wcopy(e, slot, j):
        c0, w, _ = groups[j]
        return (pltpu.make_async_copy(w1_hbm.at[e, :, c0:c0 + w], wb1.at[slot, :, c0:c0 + w], wsem.at[slot, 0, j]),
                pltpu.make_async_copy(w3_hbm.at[e, :, c0:c0 + w], wb3.at[slot, :, c0:c0 + w], wsem.at[slot, 1, j]))

    def few(e):
        top = cnt[0, e, 0]
        for d in range(1, nd):
            top = jnp.maximum(top, cnt[d, e, 0])
        return top <= FEW

    def few_copy(e):
        return pltpu.make_async_copy(xg_hbm.at[e, :, pl.ds(0, FEW)], xfew.at[e % 2], xsem.at[e % 2])

    def all_copy(e):
        return pltpu.make_async_copy(xg_hbm.at[e], xall.at[e % 2], xsem.at[e % 2])

    def rows_start(e):
        @pl.when(few(e))
        def _():
            few_copy(e).start()

        @pl.when(jnp.logical_not(few(e)))
        def _():
            all_copy(e).start()

    early_w = wb2.shape[2]

    def dcopy(e):
        return pltpu.make_async_copy(w2_hbm.at[e, :, pl.ds(0, early_w)], wb2.at[e % 2], dsem.at[e % 2])

    rows_start(0)
    dcopy(0).start()
    rows_start(1)
    dcopy(1).start()
    for e in range(first, first + depth):
        for j in range(len(groups)):
            for c in wcopy(e, e % depth, j):
                c.start()
    h_ref[...] = jnp.zeros_like(h_ref)

    def hidden(rows_ref, up, gate, c0, w):
        m = rows_ref.shape[0] * rows_ref.shape[1]
        a = jnp.dot(rows_ref[...].reshape(m, d_model), gate[:, c0:c0 + w], preferred_element_type=F32)
        b = jnp.dot(rows_ref[...].reshape(m, d_model), up[:, c0:c0 + w], preferred_element_type=F32)
        return (jax.nn.silu(a) * b).astype(BF16).reshape(rows_ref.shape[0], rows_ref.shape[1], w)

    def down(e, slots):
        rows = h_ref[e, :, 0:slots, 0:ff].reshape(nd * slots, ff)
        for c0 in range(0, early_w, 256):
            out = jnp.dot(rows, wb2[e % 2, :, c0:c0 + 256], preferred_element_type=F32)
            h_ref[e, :, 0:slots, ff + c0:ff + c0 + 256] = out.astype(BF16).reshape(nd, slots, 256)

    def expert(e, gate, up, wait):
        small = few(e)

        @pl.when(small)
        def _():
            few_copy(e).wait()
            for j, (_, _, cols) in enumerate(groups):
                wait(j)
                for c0, w in cols:
                    h_ref[e, :, 0:FEW, c0:c0 + w] = hidden(xfew.at[e % 2], up, gate, c0, w)
            dcopy(e).wait()
            down(e, FEW)

        @pl.when(jnp.logical_not(small))
        def _():
            all_copy(e).wait()
            for j, (_, _, cols) in enumerate(groups):
                wait(j)
                for c0, w in cols:
                    h_ref[e, :, :, c0:c0 + w] = hidden(xall.at[e % 2], up, gate, c0, w)
            dcopy(e).wait()
            down(e, SLOT)

        @pl.when(e + 2 < n_exp)
        def _():
            rows_start(e + 2)
            dcopy(e + 2).start()

    def early(e, carry):
        expert(e, pre1.at[e], pre3.at[e], lambda j: None)
        return carry

    def late(e, carry):
        slot = e % depth

        def wait(j):
            for c in wcopy(e, slot, j):
                c.wait()

        expert(e, wb1.at[slot], wb3.at[slot], wait)

        @pl.when(e + depth < n_exp)
        def _():
            for j in range(len(groups)):
                for c in wcopy(e + depth, slot, j):
                    c.start()
        return carry

    lax.fori_loop(0, first, early, 0)
    lax.fori_loop(first, n_exp, late, 0)


def hidden_call(cnt, xg, w1, w3, w2, pre1, pre3):
    n_exp, d_model, ff = w1.shape
    nd = cnt.shape[0]
    depth = 2
    any_spec = pl.BlockSpec(memory_space=pl.ANY)
    vmem = pl.BlockSpec(memory_space=pltpu.VMEM)
    dma = pltpu.SemaphoreType.DMA
    return pl.pallas_call(
        hidden_kernel,
        out_shape=pltpu.VMEM((n_exp, nd, SLOT, ff + EARLY * CHUNK), BF16),
        in_specs=[pl.BlockSpec(memory_space=pltpu.SMEM)] + [any_spec] * 4 + [vmem, vmem],
        out_specs=vmem,
        scratch_shapes=[
            pltpu.VMEM((depth, d_model, ff), BF16),
            pltpu.VMEM((depth, d_model, ff), BF16),
            pltpu.VMEM((2, ff, EARLY * CHUNK), BF16),
            pltpu.VMEM((2, nd, FEW, d_model), BF16),
            pltpu.VMEM((2, nd, SLOT, d_model), BF16),
            dma((depth, 2, 2)), dma((2,)), dma((2,)),
        ],
        compiler_params=pltpu.CompilerParams(vmem_limit_bytes=33_800_000),
        name="routed_hidden",
    )(cnt, xg, w1, w3, w2, pltpu.with_memory_space_constraint(pre1, pltpu.VMEM),
      pltpu.with_memory_space_constraint(pre3, pltpu.VMEM))


def down_kernel(hv, g_hbm, hsh_ref, w2_hbm, sd_hbm, y_ref,
                gv, wb, sdb, ob, snd, kept, in0, in1, in2,
                gsem, wsem, dsem, s0s, s0r, s1s, s1r, s2s, s2r):
    me, core, sib, xn, yn, dg = neighbours()
    n_exp, full, _ = hv.shape
    ff = w2_hbm.shape[1]
    nd = gv.shape[0]
    rows = gv.shape[1] // 3
    n_chunks = snd.shape[0]
    width = wb.shape[3]
    depth = wb.shape[0]
    hw = width // 2

    barrier = pltpu.get_barrier_semaphore()
    for dev in (sib, xn, yn):
        pl.semaphore_signal(barrier, inc=1, device_id={"ep": dev}, device_id_type=MESH)

    def wcopy(c, e):
        cols = pl.ds(pl.multiple_of(c * width, width), width)
        slot = c % depth
        return pltpu.make_async_copy(w2_hbm.at[e, :, cols], wb.at[slot, e], wsem.at[slot, e])

    def dcopy(c):
        cols = pl.ds(pl.multiple_of(c * width, width), width)
        return pltpu.make_async_copy(sd_hbm.at[:, cols], sdb.at[c], dsem.at[c])

    gcopy = pltpu.make_async_copy(g_hbm, gv, gsem)
    early = (hv.shape[2] - ff) // width
    gcopy.start()
    for c in range(early, early + depth):
        for e in range(n_exp):
            wcopy(c, e).start()

    own_c, xn_c, yn_c, dg_c = me // 2, xn // 2, yn // 2, dg // 2
    orders = ((own_c, yn_c, xn_c, dg_c), (own_c, xn_c, yn_c, dg_c))
    first_hop = (xn, yn)
    second_hop = (yn, xn)

    def send0(c):
        return rcopy(snd.at[c], in0.at[c], s0s.at[c], s0r.at[c], sib)

    def send1(c, q):
        return rcopy(kept.at[c, q, pl.ds(2, 2)], in1.at[c, q], s1s.at[c, q], s1r.at[c, q], first_hop[q])

    def send2(c, q):
        return rcopy(kept.at[c, q, 1], in2.at[c, q], s2s.at[c, q], s2r.at[c, q], second_hop[q])

    def step0(c):
        send0(c).wait_recv()
        kept[c] = kept[c] + in0[c]

    def step1(c):
        for q in range(2):
            send1(c, q).wait_recv()
            kept[c, q, 0:2] = kept[c, q, 0:2] + in1[c, q]

    def step2(c):
        for q in range(2):
            send2(c, q).wait_recv()
            kept[c, q, 0] = kept[c, q, 0] + in2[c, q]

    def start1(c):
        send1(c, 0).start()
        send1(c, 1).start()

    def start2(c):
        send2(c, 0).start()
        send2(c, 1).start()

    def expert(c, e):
        out = jnp.dot(hv[e, :, 0:ff], wb[c % depth, e], preferred_element_type=F32)
        out = out.astype(BF16).astype(F32)
        ob[:, e] = out.reshape(nd, SLOT, width)

    def gated(d, o):
        r = jnp.dot(gv[d], o, preferred_element_type=F32)
        return r[0:rows] + r[rows:2 * rows] + r[2 * rows:3 * rows]

    def chunk(c, carry):
        for e0 in range(0, n_exp, 4):
            for e in range(e0, e0 + 4):
                wcopy(c, e).wait()
            for e in range(e0, e0 + 4):
                expert(c, e)

            @pl.when(c + depth < n_chunks)
            def _():
                for e in range(e0, e0 + 4):
                    wcopy(c + depth, e).start()

            if e0 == 0:
                @pl.when(c >= 1)
                def _():
                    step0(c - 1)

                @pl.when(c >= 3)
                def _():
                    step1(c - 3)

                @pl.when(c >= 1)
                def _():
                    start1(c - 1)

                @pl.when(c >= 3)
                def _():
                    start2(c - 3)

        dcopy(c).start()
        reduce_start(c, lambda d: ob[d].reshape(n_exp * SLOT, width).astype(BF16))
        return carry

    def reduce_start(c, rows_of):
        chips = (own_c, xn_c, yn_c, dg_c)
        where = ((0, 0), (2, 1), (1, 2), (3, 3))
        for chip, (p0, p1) in zip(chips, where):
            d = 2 * chip + 1 - core
            r = gated(d, rows_of(d))
            snd[c, 0, p0] = r[:, 0:hw]
            snd[c, 1, p1] = r[:, hw:width]
        for chip, (p0, p1) in zip(chips, where):
            d = 2 * chip + core
            r = gated(d, rows_of(d))
            kept[c, 0, p0] = r[:, 0:hw]
            kept[c, 1, p1] = r[:, hw:width]

        send0(c).start()

    pl.semaphore_wait(barrier, 3)
    gcopy.wait()
    for c in range(early):
        dcopy(c).start()
        cols = slice(ff + c * width, ff + (c + 1) * width)
        reduce_start(c, lambda d: hv[:, pl.ds(pl.multiple_of(d * SLOT, SLOT), SLOT), cols].reshape(n_exp * SLOT, width))
    for c in range(early - 1):
        step0(c)
        start1(c)
    lax.fori_loop(early, n_chunks, chunk, 0)

    def shared(c):
        dcopy(c).wait()
        cols = pl.ds(pl.multiple_of(c * width, width), width)
        s = jnp.dot(hsh_ref[...], sdb[c], preferred_element_type=F32).astype(BF16)
        y_ref[:, cols] = s

    def shared_range(lo, hi):
        def body(c, carry):
            shared(c)
            return carry
        lax.fori_loop(lo, hi, body, 0)

    last = n_chunks - 1
    shared_range(0, 3)
    step0(last)
    step1(last - 2)
    start1(last)
    start2(last - 2)
    shared_range(3, 6)
    step1(last - 1)
    start2(last - 1)
    shared_range(6, n_chunks)
    step1(last)
    start2(last)

    def finish(c, carry):
        step2(c)
        for q in range(2):
            cols = pl.ds(pl.multiple_of(c * width + q * hw, hw), hw)
            y_ref[:, cols] = (y_ref[:, cols].astype(F32) + kept[c, q, 0]).astype(BF16)
        return carry

    lax.fori_loop(0, n_chunks, finish, 0)

    def drain(c, carry):
        send0(c).wait_send()
        for q in range(2):
            send1(c, q).wait_send()
            send2(c, q).wait_send()
        return carry

    lax.fori_loop(0, n_chunks, drain, 0)


def down_call(h, g, hsh, w2, sd):
    n_exp, full, _ = h.shape
    ff = w2.shape[1]
    nd, rows3, width_g = g.shape
    rows = rows3 // 3
    d_model = w2.shape[2]
    width = CHUNK
    n_chunks = d_model // width
    depth = 3
    hw = width // 2
    any_spec = pl.BlockSpec(memory_space=pl.ANY)
    vmem = pl.BlockSpec(memory_space=pltpu.VMEM)
    dma = pltpu.SemaphoreType.DMA
    return pl.pallas_call(
        down_kernel,
        out_shape=jax.ShapeDtypeStruct((rows, d_model), BF16),
        in_specs=[vmem, any_spec, vmem, any_spec, any_spec],
        out_specs=vmem,
        scratch_shapes=[
            pltpu.VMEM((nd, rows3, width_g), BF16),
            pltpu.VMEM((depth, n_exp, ff, width), BF16),
            pltpu.VMEM((n_chunks, sd.shape[0], width), BF16),
            pltpu.VMEM((nd, n_exp, SLOT, width), F32),
            pltpu.VMEM((n_chunks, 2, 4, rows, hw), F32),
            pltpu.VMEM((n_chunks, 2, 4, rows, hw), F32),
            pltpu.VMEM((n_chunks, 2, 4, rows, hw), F32),
            pltpu.VMEM((n_chunks, 2, 2, rows, hw), F32),
            pltpu.VMEM((n_chunks, 2, rows, hw), F32),
            dma(()), dma((depth, n_exp)), dma((n_chunks,)),
            dma((n_chunks,)), dma((n_chunks,)),
            dma((n_chunks, 2)), dma((n_chunks, 2)), dma((n_chunks, 2)), dma((n_chunks, 2)),
        ],
        compiler_params=pltpu.CompilerParams(
            collective_id=1, has_side_effects=True, vmem_limit_bytes=55_000_000),
        name="down_reduce",
    )(pltpu.with_memory_space_constraint(h, pltpu.VMEM), g, hsh, w2, sd)


def solution(mesh):
    nd = mesh.shape["ep"]

    def device_fn(x, route, gates, w_gate, w_up, w_down, sg, su, sd):
        xg, hsh, cnt, g, pre1, pre3 = gather_call(x, route.T, gates.T, sg, su, w_gate, w_up, nd)
        h = hidden_call(cnt, xg, w_gate, w_up, w_down, pre1, pre3)
        return down_call(h.reshape(h.shape[0], -1, h.shape[3]), g, hsh, w_down, sd)

    tok = P(("dp", "ep"), None)
    exp = P("ep", None, None)
    rep = P(None, None)
    return jax.shard_map(device_fn, mesh=mesh, in_specs=(tok, tok, tok, exp, exp, exp, rep, rep, rep),
                         out_specs=tok, check_vma=False)
```

```python
import functools

import jax
import jax.numpy as jnp
from jax import lax
from jax.experimental import pallas as pl
from jax.experimental.pallas import tpu as pltpu
from jax.sharding import PartitionSpec as P

MESH = pl.DeviceIdType.MESH
CAP = 36
SLOT = 40
VMEM_LIMIT = 67_000_000
H_BYTES = 10_500_000
CHUNK = 256
EARLY = 2
PRE = 2
PRE_BYTES = 23_500_000
BF16 = jnp.bfloat16
F32 = jnp.float32


def neighbours():
    me = lax.axis_index("ep")
    core = me % 2
    xb = (me // 2) % 2
    yb = me // 4
    sib = me + 1 - 2 * core
    xn = me + 2 - 4 * xb
    yn = me + 4 - 8 * yb
    dg = yn + 2 - 4 * xb
    return me, core, sib, xn, yn, dg


def rcopy(src, dst, send, recv, dev):
    return pltpu.make_async_remote_copy(
        src_ref=src, dst_ref=dst, send_sem=send, recv_sem=recv,
        device_id={"ep": dev}, device_id_type=MESH)


def gather_kernel(x_ref, route_ref, gate_ref, sg_hbm, su_hbm, w1_hbm, w3_hbm,
                  xg_hbm, hsh_hbm, cnt_hbm, g_hbm, pre1, pre3,
                  land, meta_s, bg, bu, metal, stage, hsh, gv, cntv,
                  wsem, osem, psem, gsem, hsem, csem,
                  sx_s, sx_r, sy_s, sy_r, f_s, f_r, ss_s, ss_r, m_s, m_r):
    me, core, sib, xn, yn, dg = neighbours()
    sxn = xn + 1 - 2 * core
    syn = yn + 1 - 2 * core
    sdg = dg + 1 - 2 * core
    nd = land.shape[0]
    rows, d_model = x_ref.shape
    half = rows // 2
    ring = bg.shape[0]
    width = bg.shape[2]
    n_chunks = sg_hbm.shape[1] // width
    n_all = 8 * nd

    barrier = pltpu.get_barrier_semaphore()
    for r in range(1, nd):
        pl.semaphore_signal(barrier, inc=1, device_id={"ep": (me + r) % nd}, device_id_type=MESH)

    def wcopy(i):
        cols = pl.ds(pl.multiple_of(i * width, width), width)
        slot = i % ring
        return (pltpu.make_async_copy(sg_hbm.at[:, cols], bg.at[slot], wsem.at[0, slot]),
                pltpu.make_async_copy(su_hbm.at[:, cols], bu.at[slot], wsem.at[1, slot]))

    for i in range(ring):
        for c in wcopy(i):
            c.start()

    def pcopy(e):
        return (pltpu.make_async_copy(w1_hbm.at[e], pre1.at[e], psem.at[0, e]),
                pltpu.make_async_copy(w3_hbm.at[e], pre3.at[e], psem.at[1, e]))

    def prefetch(e):
        for c in pcopy(e):
            c.start()

    ids = lax.broadcasted_iota(jnp.int32, (n_all, rows), 0)
    mask = jnp.zeros((n_all, rows), F32)
    gmap = jnp.zeros((n_all, rows), F32)
    for k in range(route_ref.shape[0]):
        eq = route_ref[k:k + 1, :] == ids
        mask = mask + jnp.where(eq, 1.0, 0.0)
        gmap = gmap + jnp.where(eq, gate_ref[k:k + 1, :], 0.0)
    before = (lax.broadcasted_iota(jnp.int32, (rows, rows), 0)
              < lax.broadcasted_iota(jnp.int32, (rows, rows), 1))
    rank = jnp.dot(mask.astype(BF16), jnp.where(before, 1.0, 0.0).astype(BF16), preferred_element_type=F32)
    rank = jnp.where(mask > 0.0, rank, -1.0)
    fill = jnp.zeros((n_all, 128 - rows), F32)
    rank = jnp.concatenate([rank, fill - 1.0], axis=1)
    gmap = jnp.concatenate([gmap, fill], axis=1)
    for j in range(nd):
        meta_s[j, 0:8, :] = rank[8 * j:8 * j + 8]
        meta_s[j, 8:16, :] = gmap[8 * j:8 * j + 8]
    metal[me] = meta_s[me]

    def hs(h):
        return pl.ds(h * half, half)

    pl.semaphore_wait(barrier, nd - 1)
    metas = []
    for r in range(1, nd):
        dst = (me + r) % nd
        c = rcopy(meta_s.at[dst], metal.at[me], m_s.at[r - 1], m_r.at[r - 1], dst)
        c.start()
        metas.append(c)
    own_x = [rcopy(x_ref.at[hs(h)], land.at[me, hs(h)], sx_s.at[h], sx_r.at[h], xn) for h in range(2)]
    own_y = [rcopy(x_ref.at[hs(h)], land.at[me, hs(h)], sy_s.at[h], sy_r.at[h], yn) for h in range(2)]
    own_s = rcopy(x_ref, land.at[me], ss_s.at[0], ss_r.at[0], sib)
    own_x[0].start()
    own_y[1].start()
    own_x[1].start()
    own_y[0].start()
    own_s.start()

    def shared_range(lo, hi):
        def body(i, carry):
            for c in wcopy(i):
                c.wait()
            a = jnp.dot(x_ref[...], bg[i % ring], preferred_element_type=F32)
            b = jnp.dot(x_ref[...], bu[i % ring], preferred_element_type=F32)
            cols = pl.ds(pl.multiple_of(i * width, width), width)
            hsh[:, cols] = (jax.nn.silu(a) * b).astype(BF16)

            @pl.when(i + ring < n_chunks)
            def _():
                for c in wcopy(i + ring):
                    c.start()
            return carry
        lax.fori_loop(lo, hi, body, 0)

    shared_range(0, n_chunks - 6)
    prefetch(0)

    for c in metas:
        c.wait_recv()

    for d in range(nd):
        n = jnp.sum(jnp.where(metal[d, 0:8, :] >= 0.0, 1.0, 0.0), axis=1, keepdims=True)
        cntv[d] = jnp.broadcast_to(n, (8, 128)).astype(jnp.int32)
    ccopy = pltpu.make_async_copy(cntv, cnt_hbm, csem)
    ccopy.start()

    def pick(d, x_rows, k):
        buf = k % 2
        if k >= 2:
            outs[k - 2].wait()
        slot = lax.broadcasted_iota(jnp.int32, (SLOT, rows), 0).astype(F32)
        sel = jnp.concatenate(
            [jnp.where(metal[d, e:e + 1, 0:rows] == slot, 1.0, 0.0) for e in range(8)], axis=0).astype(BF16)
        for c0 in range(0, d_model, 512):
            r = jnp.dot(sel, x_rows[:, c0:c0 + 512], preferred_element_type=F32)
            stage[buf, :, :, c0:c0 + 512] = r.astype(BF16).reshape(8, SLOT, 512)
        c = pltpu.make_async_copy(stage.at[buf], xg_hbm.at[:, d], osem.at[k])
        c.start()
        outs.append(c)

    outs = []
    pick(me, x_ref, 0)
    own_s.wait_recv()
    pick(sib, land.at[sib], 1)

    own_x[0].wait_recv()
    fy = rcopy(land.at[xn, hs(0)], land.at[xn, hs(0)], f_s.at[0], f_r.at[0], yn)
    fy.start()
    sx0 = rcopy(land.at[xn, hs(0)], land.at[xn, hs(0)], ss_s.at[1], ss_r.at[1], sib)
    sx0.start()
    own_y[1].wait_recv()
    fx = rcopy(land.at[yn, hs(1)], land.at[yn, hs(1)], f_s.at[1], f_r.at[1], xn)
    fx.start()
    sy1 = rcopy(land.at[yn, hs(1)], land.at[yn, hs(1)], ss_s.at[2], ss_r.at[2], sib)
    sy1.start()

    shared_range(n_chunks - 6, n_chunks)
    for e in range(1, pre1.shape[0]):
        prefetch(e)
    hcopy = pltpu.make_async_copy(hsh, hsh_hbm, hsem)
    hcopy.start()

    width_g = 8 * SLOT
    lane = lax.broadcasted_iota(jnp.int32, (8, width_g), 1)
    sel = jnp.where(lane // SLOT == lax.broadcasted_iota(jnp.int32, (8, width_g), 0), 1.0, 0.0)
    slot_id = (lax.broadcasted_iota(jnp.int32, (rows, width_g), 1) % SLOT).astype(F32)

    def spread(v):
        return lax.dot_general(v, sel, (((0,), (0,)), ((), ())), preferred_element_type=F32)[:rows]

    def gate_body(d, carry):
        rk = metal[d, 0:8, :]
        gt = metal[d, 8:16, :]
        hi = gt.astype(BF16).astype(F32)
        mid = (gt - hi).astype(BF16).astype(F32)
        lo = gt - hi - mid
        eq = spread(rk) == slot_id
        for q, part in enumerate((hi, mid, lo)):
            gv[d, q * rows:(q + 1) * rows, :] = jnp.where(eq, spread(part), 0.0).astype(BF16)
        return carry

    lax.fori_loop(0, nd, gate_body, 0)
    gcopy = pltpu.make_async_copy(gv, g_hbm, gsem)
    gcopy.start()

    own_x[1].wait_recv()
    sx1 = rcopy(land.at[xn, hs(1)], land.at[xn, hs(1)], ss_s.at[3], ss_r.at[3], sib)
    sx1.start()
    own_y[0].wait_recv()
    sy0 = rcopy(land.at[yn, hs(0)], land.at[yn, hs(0)], ss_s.at[4], ss_r.at[4], sib)
    sy0.start()
    pick(xn, land.at[xn], 2)
    pick(yn, land.at[yn], 3)
    sx0.wait_recv()
    sx1.wait_recv()
    pick(sxn, land.at[sxn], 4)
    sy1.wait_recv()
    sy0.wait_recv()
    pick(syn, land.at[syn], 5)

    fy.wait_recv()
    sd0 = rcopy(land.at[dg, hs(0)], land.at[dg, hs(0)], ss_s.at[5], ss_r.at[5], sib)
    sd0.start()
    fx.wait_recv()
    sd1 = rcopy(land.at[dg, hs(1)], land.at[dg, hs(1)], ss_s.at[6], ss_r.at[6], sib)
    sd1.start()
    pick(dg, land.at[dg], 6)
    sd0.wait_recv()
    sd1.wait_recv()
    pick(sdg, land.at[sdg], 7)
    for c in own_x + own_y + [own_s, fy, fx, sx0, sx1, sy0, sy1, sd0, sd1] + metas:
        c.wait_send()
    for c in outs[6:] + [ccopy, hcopy, gcopy]:
        c.wait()
    for e in range(pre1.shape[0]):
        for c in pcopy(e):
            c.wait()


def gather_call(x, route, gates, sg, su, w1, w3, nd):
    rows, d_model = x.shape
    ff = sg.shape[1]
    width = 256
    ring = 8
    any_spec = pl.BlockSpec(memory_space=pl.ANY)
    vmem = pl.BlockSpec(memory_space=pltpu.VMEM)
    dma = pltpu.SemaphoreType.DMA
    return pl.pallas_call(
        gather_kernel,
        out_shape=(
            jax.ShapeDtypeStruct((8, nd, SLOT, d_model), BF16),
            jax.ShapeDtypeStruct((rows, ff), BF16),
            jax.ShapeDtypeStruct((nd, 8, 128), jnp.int32),
            jax.ShapeDtypeStruct((nd, 3 * rows, 8 * SLOT), BF16),
            pltpu.VMEM((PRE,) + w1.shape[1:], BF16),
            pltpu.VMEM((PRE,) + w3.shape[1:], BF16),
        ),
        in_specs=[vmem, vmem, vmem] + [any_spec] * 4,
        out_specs=(pl.BlockSpec(memory_space=pltpu.HBM),) * 4 + (vmem, vmem),
        scratch_shapes=[
            pltpu.VMEM((nd, rows, d_model), BF16),
            pltpu.VMEM((nd, 16, 128), F32),
            pltpu.VMEM((ring, d_model, width), BF16),
            pltpu.VMEM((ring, d_model, width), BF16),
            pltpu.VMEM((nd, 16, 128), F32),
            pltpu.VMEM((2, 8, SLOT, d_model), BF16),
            pltpu.VMEM((rows, ff), BF16),
            pltpu.VMEM((nd, 3 * rows, 8 * SLOT), BF16),
            pltpu.VMEM((nd, 8, 128), jnp.int32),
            dma((2, ring)),
            dma((8,)), dma((2, PRE)), dma(()), dma(()), dma(()),
            dma((2,)), dma((2,)), dma((2,)), dma((2,)), dma((2,)), dma((2,)),
            dma((7,)), dma((7,)), dma((7,)), dma((7,)),
        ],
        compiler_params=pltpu.CompilerParams(
            collective_id=0, has_side_effects=True, vmem_limit_bytes=33_800_000),
        name="gather_shared",
    )(x, route, gates, sg, su, w1, w3)


FEW = 16


def hidden_kernel(cnt, xg_hbm, w1_hbm, w3_hbm, w2_hbm, pre1, pre3, h_ref,
                  wb1, wb3, wb2, xfew, xall, wsem, dsem, xsem):
    n_exp, d_model, ff = w1_hbm.shape
    nd = cnt.shape[0]
    depth = wb1.shape[0]
    first = pre1.shape[0]
    bounds = [(c, min(256, ff - c)) for c in range(0, ff, 256)]
    cut = 3 * 256
    groups = ((0, cut, bounds[:3]), (cut, ff - cut, bounds[3:]))

    def wcopy(e, slot, j):
        c0, w, _ = groups[j]
        return (pltpu.make_async_copy(w1_hbm.at[e, :, c0:c0 + w], wb1.at[slot, :, c0:c0 + w], wsem.at[slot, 0, j]),
                pltpu.make_async_copy(w3_hbm.at[e, :, c0:c0 + w], wb3.at[slot, :, c0:c0 + w], wsem.at[slot, 1, j]))

    def few(e):
        top = cnt[0, e, 0]
        for d in range(1, nd):
            top = jnp.maximum(top, cnt[d, e, 0])
        return top <= FEW

    def few_copy(e):
        return pltpu.make_async_copy(xg_hbm.at[e, :, pl.ds(0, FEW)], xfew.at[e % 2], xsem.at[e % 2])

    def all_copy(e):
        return pltpu.make_async_copy(xg_hbm.at[e], xall.at[e % 2], xsem.at[e % 2])

    def rows_start(e):
        @pl.when(few(e))
        def _():
            few_copy(e).start()

        @pl.when(jnp.logical_not(few(e)))
        def _():
            all_copy(e).start()

    early_w = wb2.shape[2]

    def dcopy(e):
        return pltpu.make_async_copy(w2_hbm.at[e, :, pl.ds(0, early_w)], wb2.at[e % 2], dsem.at[e % 2])

    rows_start(0)
    dcopy(0).start()
    rows_start(1)
    dcopy(1).start()
    for e in range(first, first + depth):
        for j in range(len(groups)):
            for c in wcopy(e, e % depth, j):
                c.start()
    h_ref[...] = jnp.zeros_like(h_ref)

    def hidden(rows_ref, up, gate, c0, w):
        m = rows_ref.shape[0] * rows_ref.shape[1]
        a = jnp.dot(rows_ref[...].reshape(m, d_model), gate[:, c0:c0 + w], preferred_element_type=F32)
        b = jnp.dot(rows_ref[...].reshape(m, d_model), up[:, c0:c0 + w], preferred_element_type=F32)
        return (jax.nn.silu(a) * b).astype(BF16).reshape(rows_ref.shape[0], rows_ref.shape[1], w)

    def down(e, slots):
        rows = h_ref[e, :, 0:slots, 0:ff].reshape(nd * slots, ff)
        for c0 in range(0, early_w, 256):
            out = jnp.dot(rows, wb2[e % 2, :, c0:c0 + 256], preferred_element_type=F32)
            h_ref[e, :, 0:slots, ff + c0:ff + c0 + 256] = out.astype(BF16).reshape(nd, slots, 256)

    def expert(e, gate, up, wait, refill):
        small = few(e)

        @pl.when(small)
        def _():
            few_copy(e).wait()
            for j, (_, _, cols) in enumerate(groups):
                wait(j)
                for c0, w in cols:
                    h_ref[e, :, 0:FEW, c0:c0 + w] = hidden(xfew.at[e % 2], up, gate, c0, w)
                refill(j)
            dcopy(e).wait()
            down(e, FEW)

        @pl.when(jnp.logical_not(small))
        def _():
            all_copy(e).wait()
            for j, (_, _, cols) in enumerate(groups):
                wait(j)
                for c0, w in cols:
                    h_ref[e, :, :, c0:c0 + w] = hidden(xall.at[e % 2], up, gate, c0, w)
                refill(j)
            dcopy(e).wait()
            down(e, SLOT)

        @pl.when(e + 2 < n_exp)
        def _():
            rows_start(e + 2)
            dcopy(e + 2).start()

    def early(e, carry):
        expert(e, pre1.at[e], pre3.at[e], lambda j: None, lambda j: None)
        return carry

    def late(e, carry):
        slot = e % depth

        def wait(j):
            for c in wcopy(e, slot, j):
                c.wait()

        def refill(j):
            @pl.when(e + depth < n_exp)
            def _():
                for c in wcopy(e + depth, slot, j):
                    c.start()

        expert(e, wb1.at[slot], wb3.at[slot], wait, refill)
        return carry

    lax.fori_loop(0, first, early, 0)
    lax.fori_loop(first, n_exp, late, 0)


def hidden_call(cnt, xg, w1, w3, w2, pre1, pre3):
    n_exp, d_model, ff = w1.shape
    nd = cnt.shape[0]
    depth = 2
    any_spec = pl.BlockSpec(memory_space=pl.ANY)
    vmem = pl.BlockSpec(memory_space=pltpu.VMEM)
    dma = pltpu.SemaphoreType.DMA
    return pl.pallas_call(
        hidden_kernel,
        out_shape=pltpu.VMEM((n_exp, nd, SLOT, ff + EARLY * CHUNK), BF16),
        in_specs=[pl.BlockSpec(memory_space=pltpu.SMEM)] + [any_spec] * 4 + [vmem, vmem],
        out_specs=vmem,
        scratch_shapes=[
            pltpu.VMEM((depth, d_model, ff), BF16),
            pltpu.VMEM((depth, d_model, ff), BF16),
            pltpu.VMEM((2, ff, EARLY * CHUNK), BF16),
            pltpu.VMEM((2, nd, FEW, d_model), BF16),
            pltpu.VMEM((2, nd, SLOT, d_model), BF16),
            dma((depth, 2, 2)), dma((2,)), dma((2,)),
        ],
        compiler_params=pltpu.CompilerParams(vmem_limit_bytes=33_800_000),
        name="routed_hidden",
    )(cnt, xg, w1, w3, w2, pltpu.with_memory_space_constraint(pre1, pltpu.VMEM),
      pltpu.with_memory_space_constraint(pre3, pltpu.VMEM))


def down_kernel(hv, g_hbm, hsh_ref, w2_hbm, sd_hbm, y_ref,
                gv, wb, sdb, ob, snd, kept, in0, in1, in2,
                gsem, wsem, dsem, s0s, s0r, s1s, s1r, s2s, s2r):
    me, core, sib, xn, yn, dg = neighbours()
    n_exp, full, _ = hv.shape
    ff = w2_hbm.shape[1]
    nd = gv.shape[0]
    rows = gv.shape[1] // 3
    n_chunks = snd.shape[0]
    width = wb.shape[3]
    depth = wb.shape[0]
    hw = width // 2

    barrier = pltpu.get_barrier_semaphore()
    for dev in (sib, xn, yn):
        pl.semaphore_signal(barrier, inc=1, device_id={"ep": dev}, device_id_type=MESH)

    def wcopy(c, e):
        cols = pl.ds(pl.multiple_of(c * width, width), width)
        slot = c % depth
        return pltpu.make_async_copy(w2_hbm.at[e, :, cols], wb.at[slot, e], wsem.at[slot, e])

    def dcopy(c):
        cols = pl.ds(pl.multiple_of(c * width, width), width)
        return pltpu.make_async_copy(sd_hbm.at[:, cols], sdb.at[c], dsem.at[c])

    gcopy = pltpu.make_async_copy(g_hbm, gv, gsem)
    early = (hv.shape[2] - ff) // width
    gcopy.start()
    for c in range(early, early + depth):
        for e in range(n_exp):
            wcopy(c, e).start()

    own_c, xn_c, yn_c, dg_c = me // 2, xn // 2, yn // 2, dg // 2
    orders = ((own_c, yn_c, xn_c, dg_c), (own_c, xn_c, yn_c, dg_c))
    first_hop = (xn, yn)
    second_hop = (yn, xn)

    def send0(c):
        return rcopy(snd.at[c], in0.at[c], s0s.at[c], s0r.at[c], sib)

    def send1(c, q):
        return rcopy(kept.at[c, q, pl.ds(2, 2)], in1.at[c, q], s1s.at[c, q], s1r.at[c, q], first_hop[q])

    def send2(c, q):
        return rcopy(kept.at[c, q, 1], in2.at[c, q], s2s.at[c, q], s2r.at[c, q], second_hop[q])

    def step0(c):
        send0(c).wait_recv()
        kept[c] = kept[c] + in0[c]

    def step1(c):
        for q in range(2):
            send1(c, q).wait_recv()
            kept[c, q, 0:2] = kept[c, q, 0:2] + in1[c, q]

    def step2(c):
        for q in range(2):
            send2(c, q).wait_recv()
            kept[c, q, 0] = kept[c, q, 0] + in2[c, q]

    def start1(c):
        send1(c, 0).start()
        send1(c, 1).start()

    def start2(c):
        send2(c, 0).start()
        send2(c, 1).start()

    def expert(c, e):
        out = jnp.dot(hv[e, :, 0:ff], wb[c % depth, e], preferred_element_type=F32)
        out = out.astype(BF16).astype(F32)
        ob[:, e] = out.reshape(nd, SLOT, width)

    def gated(d, o):
        r = jnp.dot(gv[d], o, preferred_element_type=F32)
        return r[0:rows] + r[rows:2 * rows] + r[2 * rows:3 * rows]

    def chunk(c, carry):
        for e0 in range(0, n_exp, 4):
            for e in range(e0, e0 + 4):
                wcopy(c, e).wait()
            for e in range(e0, e0 + 4):
                expert(c, e)

            @pl.when(c + depth < n_chunks)
            def _():
                for e in range(e0, e0 + 4):
                    wcopy(c + depth, e).start()

            if e0 == 0:
                step0(c - 1)
                start1(c - 1)

                @pl.when(c == early)
                def _():
                    for i in range(early - 2):
                        step1(i)
                        start2(i)

        dcopy(c).start()
        reduce_start(c, lambda d: ob[d].reshape(n_exp * SLOT, width).astype(BF16))
        step1(c - 2)
        start2(c - 2)
        return carry

    def reduce_start(c, rows_of):
        chips = (own_c, xn_c, yn_c, dg_c)
        where = ((0, 0), (2, 1), (1, 2), (3, 3))
        for chip, (p0, p1) in zip(chips, where):
            d = 2 * chip + 1 - core
            r = gated(d, rows_of(d))
            snd[c, 0, p0] = r[:, 0:hw]
            snd[c, 1, p1] = r[:, hw:width]
        for chip, (p0, p1) in zip(chips, where):
            d = 2 * chip + core
            r = gated(d, rows_of(d))
            kept[c, 0, p0] = r[:, 0:hw]
            kept[c, 1, p1] = r[:, hw:width]

        send0(c).start()

    pl.semaphore_wait(barrier, 3)
    gcopy.wait()
    for c in range(early):
        dcopy(c).start()
        cols = slice(ff + c * width, ff + (c + 1) * width)
        reduce_start(c, lambda d: hv[:, pl.ds(pl.multiple_of(d * SLOT, SLOT), SLOT), cols].reshape(n_exp * SLOT, width))
    for c in range(early - 1):
        step0(c)
        start1(c)
    lax.fori_loop(early, n_chunks, chunk, 0)

    def shared(c):
        dcopy(c).wait()
        cols = pl.ds(pl.multiple_of(c * width, width), width)
        s = jnp.dot(hsh_ref[...], sdb[c], preferred_element_type=F32).astype(BF16)
        y_ref[:, cols] = s

    def shared_range(lo, hi):
        def body(c, carry):
            shared(c)
            return carry
        lax.fori_loop(lo, hi, body, 0)

    def finish_range(lo, hi):
        def body(c, carry):
            step2(c)
            for q in range(2):
                cols = pl.ds(pl.multiple_of(c * width + q * hw, hw), hw)
                y_ref[:, cols] = (y_ref[:, cols].astype(F32) + kept[c, q, 0]).astype(BF16)
            return carry
        lax.fori_loop(lo, hi, body, 0)

    last = n_chunks - 1
    shared_range(0, 3)
    step0(last)
    start1(last)
    shared_range(3, n_chunks)
    step1(last - 1)
    start2(last - 1)
    finish_range(0, last - 1)
    step1(last)
    start2(last)
    finish_range(last - 1, n_chunks)

    def drain(c, carry):
        send0(c).wait_send()
        for q in range(2):
            send1(c, q).wait_send()
            send2(c, q).wait_send()
        return carry

    lax.fori_loop(0, n_chunks, drain, 0)


def down_call(h, g, hsh, w2, sd):
    n_exp, full, _ = h.shape
    ff = w2.shape[1]
    nd, rows3, width_g = g.shape
    rows = rows3 // 3
    d_model = w2.shape[2]
    width = CHUNK
    n_chunks = d_model // width
    depth = 3
    hw = width // 2
    any_spec = pl.BlockSpec(memory_space=pl.ANY)
    vmem = pl.BlockSpec(memory_space=pltpu.VMEM)
    dma = pltpu.SemaphoreType.DMA
    return pl.pallas_call(
        down_kernel,
        out_shape=jax.ShapeDtypeStruct((rows, d_model), BF16),
        in_specs=[vmem, any_spec, vmem, any_spec, any_spec],
        out_specs=vmem,
        scratch_shapes=[
            pltpu.VMEM((nd, rows3, width_g), BF16),
            pltpu.VMEM((depth, n_exp, ff, width), BF16),
            pltpu.VMEM((n_chunks, sd.shape[0], width), BF16),
            pltpu.VMEM((nd, n_exp, SLOT, width), F32),
            pltpu.VMEM((n_chunks, 2, 4, rows, hw), F32),
            pltpu.VMEM((n_chunks, 2, 4, rows, hw), F32),
            pltpu.VMEM((n_chunks, 2, 4, rows, hw), F32),
            pltpu.VMEM((n_chunks, 2, 2, rows, hw), F32),
            pltpu.VMEM((n_chunks, 2, rows, hw), F32),
            dma(()), dma((depth, n_exp)), dma((n_chunks,)),
            dma((n_chunks,)), dma((n_chunks,)),
            dma((n_chunks, 2)), dma((n_chunks, 2)), dma((n_chunks, 2)), dma((n_chunks, 2)),
        ],
        compiler_params=pltpu.CompilerParams(
            collective_id=1, has_side_effects=True, vmem_limit_bytes=55_000_000),
        name="down_reduce",
    )(pltpu.with_memory_space_constraint(h, pltpu.VMEM), g, hsh, w2, sd)


def solution(mesh):
    nd = mesh.shape["ep"]

    def device_fn(x, route, gates, w_gate, w_up, w_down, sg, su, sd):
        xg, hsh, cnt, g, pre1, pre3 = gather_call(x, route.T, gates.T, sg, su, w_gate, w_up, nd)
        h = hidden_call(cnt, xg, w_gate, w_up, w_down, pre1, pre3)
        return down_call(h.reshape(h.shape[0], -1, h.shape[3]), g, hsh, w_down, sd)

    tok = P(("dp", "ep"), None)
    exp = P("ep", None, None)
    rep = P(None, None)
    return jax.shard_map(device_fn, mesh=mesh, in_specs=(tok, tok, tok, exp, exp, exp, rep, rep, rep),
                         out_specs=tok, check_vma=False)
```

```python
import functools

import jax
import jax.numpy as jnp
from jax import lax
from jax.experimental import pallas as pl
from jax.experimental.pallas import tpu as pltpu
from jax.sharding import PartitionSpec as P

MESH = pl.DeviceIdType.MESH
CAP = 36
SLOT = 40
VMEM_LIMIT = 67_000_000
H_BYTES = 10_500_000
CHUNK = 256
GROUP = 8
EARLY = 2
PRE = 2
PRE_BYTES = 23_500_000
BF16 = jnp.bfloat16
F32 = jnp.float32


def neighbours():
    me = lax.axis_index("ep")
    core = me % 2
    xb = (me // 2) % 2
    yb = me // 4
    sib = me + 1 - 2 * core
    xn = me + 2 - 4 * xb
    yn = me + 4 - 8 * yb
    dg = yn + 2 - 4 * xb
    return me, core, sib, xn, yn, dg


def rcopy(src, dst, send, recv, dev):
    return pltpu.make_async_remote_copy(
        src_ref=src, dst_ref=dst, send_sem=send, recv_sem=recv,
        device_id={"ep": dev}, device_id_type=MESH)


def gather_kernel(x_ref, route_ref, gate_ref, sg_hbm, su_hbm, w1_hbm, w3_hbm,
                  xg_hbm, hsh_hbm, cnt_hbm, g_hbm, pre1, pre3,
                  land, meta_s, bg, bu, metal, stage, hsh, gv, cntv,
                  wsem, osem, psem, gsem, hsem, csem,
                  sx_s, sx_r, sy_s, sy_r, f_s, f_r, ss_s, ss_r, m_s, m_r):
    me, core, sib, xn, yn, dg = neighbours()
    sxn = xn + 1 - 2 * core
    syn = yn + 1 - 2 * core
    sdg = dg + 1 - 2 * core
    nd = land.shape[0]
    rows, d_model = x_ref.shape
    half = rows // 2
    ring = bg.shape[0]
    width = bg.shape[2]
    n_chunks = sg_hbm.shape[1] // width
    n_all = 8 * nd

    barrier = pltpu.get_barrier_semaphore()
    for r in range(1, nd):
        pl.semaphore_signal(barrier, inc=1, device_id={"ep": (me + r) % nd}, device_id_type=MESH)

    def wcopy(i):
        cols = pl.ds(pl.multiple_of(i * width, width), width)
        slot = i % ring
        return (pltpu.make_async_copy(sg_hbm.at[:, cols], bg.at[slot], wsem.at[0, slot]),
                pltpu.make_async_copy(su_hbm.at[:, cols], bu.at[slot], wsem.at[1, slot]))

    for i in range(ring):
        for c in wcopy(i):
            c.start()

    def pcopy(e):
        return (pltpu.make_async_copy(w1_hbm.at[e], pre1.at[e], psem.at[0, e]),
                pltpu.make_async_copy(w3_hbm.at[e], pre3.at[e], psem.at[1, e]))

    def prefetch(e):
        for c in pcopy(e):
            c.start()

    ids = lax.broadcasted_iota(jnp.int32, (n_all, rows), 0)
    mask = jnp.zeros((n_all, rows), F32)
    gmap = jnp.zeros((n_all, rows), F32)
    for k in range(route_ref.shape[0]):
        eq = route_ref[k:k + 1, :] == ids
        mask = mask + jnp.where(eq, 1.0, 0.0)
        gmap = gmap + jnp.where(eq, gate_ref[k:k + 1, :], 0.0)
    before = (lax.broadcasted_iota(jnp.int32, (rows, rows), 0)
              < lax.broadcasted_iota(jnp.int32, (rows, rows), 1))
    rank = jnp.dot(mask.astype(BF16), jnp.where(before, 1.0, 0.0).astype(BF16), preferred_element_type=F32)
    rank = jnp.where(mask > 0.0, rank, -1.0)
    fill = jnp.zeros((n_all, 128 - rows), F32)
    rank = jnp.concatenate([rank, fill - 1.0], axis=1)
    gmap = jnp.concatenate([gmap, fill], axis=1)
    for j in range(nd):
        meta_s[j, 0:8, :] = rank[8 * j:8 * j + 8]
        meta_s[j, 8:16, :] = gmap[8 * j:8 * j + 8]
    metal[me] = meta_s[me]

    def hs(h):
        return pl.ds(h * half, half)

    pl.semaphore_wait(barrier, nd - 1)
    metas = []
    for r in range(1, nd):
        dst = (me + r) % nd
        c = rcopy(meta_s.at[dst], metal.at[me], m_s.at[r - 1], m_r.at[r - 1], dst)
        c.start()
        metas.append(c)
    own_x = [rcopy(x_ref.at[hs(h)], land.at[me, hs(h)], sx_s.at[h], sx_r.at[h], xn) for h in range(2)]
    own_y = [rcopy(x_ref.at[hs(h)], land.at[me, hs(h)], sy_s.at[h], sy_r.at[h], yn) for h in range(2)]
    own_s = rcopy(x_ref, land.at[me], ss_s.at[0], ss_r.at[0], sib)
    own_x[0].start()
    own_y[1].start()
    own_x[1].start()
    own_y[0].start()
    own_s.start()

    def shared_range(lo, hi):
        def body(i, carry):
            for c in wcopy(i):
                c.wait()
            a = jnp.dot(x_ref[...], bg[i % ring], preferred_element_type=F32)
            b = jnp.dot(x_ref[...], bu[i % ring], preferred_element_type=F32)
            cols = pl.ds(pl.multiple_of(i * width, width), width)
            hsh[:, cols] = (jax.nn.silu(a) * b).astype(BF16)

            @pl.when(i + ring < n_chunks)
            def _():
                for c in wcopy(i + ring):
                    c.start()
            return carry
        lax.fori_loop(lo, hi, body, 0)

    shared_range(0, n_chunks - 6)
    prefetch(0)

    for c in metas:
        c.wait_recv()

    for d in range(nd):
        n = jnp.sum(jnp.where(metal[d, 0:8, :] >= 0.0, 1.0, 0.0), axis=1, keepdims=True)
        cntv[d] = jnp.broadcast_to(n, (8, 128)).astype(jnp.int32)
    ccopy = pltpu.make_async_copy(cntv, cnt_hbm, csem)
    ccopy.start()

    def pick(d, x_rows, k):
        buf = k % 2
        if k >= 2:
            outs[k - 2].wait()
        slot = lax.broadcasted_iota(jnp.int32, (SLOT, rows), 0).astype(F32)
        sel = jnp.concatenate(
            [jnp.where(metal[d, e:e + 1, 0:rows] == slot, 1.0, 0.0) for e in range(8)], axis=0).astype(BF16)
        for c0 in range(0, d_model, 512):
            r = jnp.dot(sel, x_rows[:, c0:c0 + 512], preferred_element_type=F32)
            stage[buf, :, :, c0:c0 + 512] = r.astype(BF16).reshape(8, SLOT, 512)
        c = pltpu.make_async_copy(stage.at[buf], xg_hbm.at[:, d], osem.at[k])
        c.start()
        outs.append(c)

    outs = []
    pick(me, x_ref, 0)
    own_s.wait_recv()
    pick(sib, land.at[sib], 1)

    own_x[0].wait_recv()
    fy = rcopy(land.at[xn, hs(0)], land.at[xn, hs(0)], f_s.at[0], f_r.at[0], yn)
    fy.start()
    sx0 = rcopy(land.at[xn, hs(0)], land.at[xn, hs(0)], ss_s.at[1], ss_r.at[1], sib)
    sx0.start()
    own_y[1].wait_recv()
    fx = rcopy(land.at[yn, hs(1)], land.at[yn, hs(1)], f_s.at[1], f_r.at[1], xn)
    fx.start()
    sy1 = rcopy(land.at[yn, hs(1)], land.at[yn, hs(1)], ss_s.at[2], ss_r.at[2], sib)
    sy1.start()

    shared_range(n_chunks - 6, n_chunks)
    for e in range(1, pre1.shape[0]):
        prefetch(e)
    hcopy = pltpu.make_async_copy(hsh, hsh_hbm, hsem)
    hcopy.start()

    width_g = 8 * SLOT
    lane = lax.broadcasted_iota(jnp.int32, (8, width_g), 1)
    sel = jnp.where(lane // SLOT == lax.broadcasted_iota(jnp.int32, (8, width_g), 0), 1.0, 0.0)
    slot_id = (lax.broadcasted_iota(jnp.int32, (rows, width_g), 1) % SLOT).astype(F32)

    def spread(v):
        return lax.dot_general(v, sel, (((0,), (0,)), ((), ())), preferred_element_type=F32)[:rows]

    def gate_body(d, carry):
        rk = metal[d, 0:8, :]
        gt = metal[d, 8:16, :]
        hi = gt.astype(BF16).astype(F32)
        mid = (gt - hi).astype(BF16).astype(F32)
        lo = gt - hi - mid
        eq = spread(rk) == slot_id
        for q, part in enumerate((hi, mid, lo)):
            gv[d, q * rows:(q + 1) * rows, :] = jnp.where(eq, spread(part), 0.0).astype(BF16)
        return carry

    lax.fori_loop(0, nd, gate_body, 0)
    gcopy = pltpu.make_async_copy(gv, g_hbm, gsem)
    gcopy.start()

    own_x[1].wait_recv()
    sx1 = rcopy(land.at[xn, hs(1)], land.at[xn, hs(1)], ss_s.at[3], ss_r.at[3], sib)
    sx1.start()
    own_y[0].wait_recv()
    sy0 = rcopy(land.at[yn, hs(0)], land.at[yn, hs(0)], ss_s.at[4], ss_r.at[4], sib)
    sy0.start()
    pick(xn, land.at[xn], 2)
    pick(yn, land.at[yn], 3)
    sx0.wait_recv()
    sx1.wait_recv()
    pick(sxn, land.at[sxn], 4)
    sy1.wait_recv()
    sy0.wait_recv()
    pick(syn, land.at[syn], 5)

    fy.wait_recv()
    sd0 = rcopy(land.at[dg, hs(0)], land.at[dg, hs(0)], ss_s.at[5], ss_r.at[5], sib)
    sd0.start()
    fx.wait_recv()
    sd1 = rcopy(land.at[dg, hs(1)], land.at[dg, hs(1)], ss_s.at[6], ss_r.at[6], sib)
    sd1.start()
    pick(dg, land.at[dg], 6)
    sd0.wait_recv()
    sd1.wait_recv()
    pick(sdg, land.at[sdg], 7)
    for c in own_x + own_y + [own_s, fy, fx, sx0, sx1, sy0, sy1, sd0, sd1] + metas:
        c.wait_send()
    for c in outs[6:] + [ccopy, hcopy, gcopy]:
        c.wait()
    for e in range(pre1.shape[0]):
        for c in pcopy(e):
            c.wait()


def gather_call(x, route, gates, sg, su, w1, w3, nd):
    rows, d_model = x.shape
    ff = sg.shape[1]
    width = 256
    ring = 8
    any_spec = pl.BlockSpec(memory_space=pl.ANY)
    vmem = pl.BlockSpec(memory_space=pltpu.VMEM)
    dma = pltpu.SemaphoreType.DMA
    return pl.pallas_call(
        gather_kernel,
        out_shape=(
            jax.ShapeDtypeStruct((8, nd, SLOT, d_model), BF16),
            jax.ShapeDtypeStruct((rows, ff), BF16),
            jax.ShapeDtypeStruct((nd, 8, 128), jnp.int32),
            jax.ShapeDtypeStruct((nd, 3 * rows, 8 * SLOT), BF16),
            pltpu.VMEM((PRE,) + w1.shape[1:], BF16),
            pltpu.VMEM((PRE,) + w3.shape[1:], BF16),
        ),
        in_specs=[vmem, vmem, vmem] + [any_spec] * 4,
        out_specs=(pl.BlockSpec(memory_space=pltpu.HBM),) * 4 + (vmem, vmem),
        scratch_shapes=[
            pltpu.VMEM((nd, rows, d_model), BF16),
            pltpu.VMEM((nd, 16, 128), F32),
            pltpu.VMEM((ring, d_model, width), BF16),
            pltpu.VMEM((ring, d_model, width), BF16),
            pltpu.VMEM((nd, 16, 128), F32),
            pltpu.VMEM((2, 8, SLOT, d_model), BF16),
            pltpu.VMEM((rows, ff), BF16),
            pltpu.VMEM((nd, 3 * rows, 8 * SLOT), BF16),
            pltpu.VMEM((nd, 8, 128), jnp.int32),
            dma((2, ring)),
            dma((8,)), dma((2, PRE)), dma(()), dma(()), dma(()),
            dma((2,)), dma((2,)), dma((2,)), dma((2,)), dma((2,)), dma((2,)),
            dma((7,)), dma((7,)), dma((7,)), dma((7,)),
        ],
        compiler_params=pltpu.CompilerParams(
            collective_id=0, has_side_effects=True, vmem_limit_bytes=33_800_000),
        name="gather_shared",
    )(x, route, gates, sg, su, w1, w3)


FEW = 16


def hidden_kernel(cnt, xg_hbm, w1_hbm, w3_hbm, w2_hbm, pre1, pre3, h_ref,
                  wb1, wb3, wb2, xfew, xall, wsem, dsem, xsem):
    n_exp, d_model, ff = w1_hbm.shape
    nd = cnt.shape[0]
    depth = wb1.shape[0]
    first = pre1.shape[0]
    bounds = [(c, min(256, ff - c)) for c in range(0, ff, 256)]
    cut = 3 * 256
    groups = ((0, cut, bounds[:3]), (cut, ff - cut, bounds[3:]))

    def wcopy(e, slot, j):
        c0, w, _ = groups[j]
        return (pltpu.make_async_copy(w1_hbm.at[e, :, c0:c0 + w], wb1.at[slot, :, c0:c0 + w], wsem.at[slot, 0, j]),
                pltpu.make_async_copy(w3_hbm.at[e, :, c0:c0 + w], wb3.at[slot, :, c0:c0 + w], wsem.at[slot, 1, j]))

    def few(e):
        top = cnt[0, e, 0]
        for d in range(1, nd):
            top = jnp.maximum(top, cnt[d, e, 0])
        return top <= FEW

    def few_copy(e):
        return pltpu.make_async_copy(xg_hbm.at[e, :, pl.ds(0, FEW)], xfew.at[e % 2], xsem.at[e % 2])

    def all_copy(e):
        return pltpu.make_async_copy(xg_hbm.at[e], xall.at[e % 2], xsem.at[e % 2])

    def rows_start(e):
        @pl.when(few(e))
        def _():
            few_copy(e).start()

        @pl.when(jnp.logical_not(few(e)))
        def _():
            all_copy(e).start()

    early_w = wb2.shape[2]

    def dcopy(e):
        return pltpu.make_async_copy(w2_hbm.at[e, :, pl.ds(0, early_w)], wb2.at[e % 2], dsem.at[e % 2])

    rows_start(0)
    dcopy(0).start()
    rows_start(1)
    dcopy(1).start()
    for e in range(first, first + depth):
        for j in range(len(groups)):
            for c in wcopy(e, e % depth, j):
                c.start()
    h_ref[...] = jnp.zeros_like(h_ref)

    def hidden(rows_ref, up, gate, c0, w):
        m = rows_ref.shape[0] * rows_ref.shape[1]
        a = jnp.dot(rows_ref[...].reshape(m, d_model), gate[:, c0:c0 + w], preferred_element_type=F32)
        b = jnp.dot(rows_ref[...].reshape(m, d_model), up[:, c0:c0 + w], preferred_element_type=F32)
        return (jax.nn.silu(a) * b).astype(BF16).reshape(rows_ref.shape[0], rows_ref.shape[1], w)

    def down(e, slots):
        rows = h_ref[e, :, 0:slots, 0:ff].reshape(nd * slots, ff)
        for c0 in range(0, early_w, 256):
            out = jnp.dot(rows, wb2[e % 2, :, c0:c0 + 256], preferred_element_type=F32)
            h_ref[e, :, 0:slots, ff + c0:ff + c0 + 256] = out.astype(BF16).reshape(nd, slots, 256)

    def expert(e, gate, up, wait, refill):
        small = few(e)

        @pl.when(small)
        def _():
            few_copy(e).wait()
            for j, (_, _, cols) in enumerate(groups):
                wait(j)
                for c0, w in cols:
                    h_ref[e, :, 0:FEW, c0:c0 + w] = hidden(xfew.at[e % 2], up, gate, c0, w)
                refill(j)
            dcopy(e).wait()
            down(e, FEW)

        @pl.when(jnp.logical_not(small))
        def _():
            all_copy(e).wait()
            for j, (_, _, cols) in enumerate(groups):
                wait(j)
                for c0, w in cols:
                    h_ref[e, :, :, c0:c0 + w] = hidden(xall.at[e % 2], up, gate, c0, w)
                refill(j)
            dcopy(e).wait()
            down(e, SLOT)

        @pl.when(e + 2 < n_exp)
        def _():
            rows_start(e + 2)
            dcopy(e + 2).start()

    def early(e, carry):
        expert(e, pre1.at[e], pre3.at[e], lambda j: None, lambda j: None)
        return carry

    def late(e, carry):
        slot = e % depth

        def wait(j):
            for c in wcopy(e, slot, j):
                c.wait()

        def refill(j):
            @pl.when(e + depth < n_exp)
            def _():
                for c in wcopy(e + depth, slot, j):
                    c.start()

        expert(e, wb1.at[slot], wb3.at[slot], wait, refill)
        return carry

    lax.fori_loop(0, first, early, 0)
    lax.fori_loop(first, n_exp, late, 0)


def hidden_call(cnt, xg, w1, w3, w2, pre1, pre3):
    n_exp, d_model, ff = w1.shape
    nd = cnt.shape[0]
    depth = 2
    any_spec = pl.BlockSpec(memory_space=pl.ANY)
    vmem = pl.BlockSpec(memory_space=pltpu.VMEM)
    dma = pltpu.SemaphoreType.DMA
    return pl.pallas_call(
        hidden_kernel,
        out_shape=pltpu.VMEM((n_exp, nd, SLOT, ff + EARLY * CHUNK), BF16),
        in_specs=[pl.BlockSpec(memory_space=pltpu.SMEM)] + [any_spec] * 4 + [vmem, vmem],
        out_specs=vmem,
        scratch_shapes=[
            pltpu.VMEM((depth, d_model, ff), BF16),
            pltpu.VMEM((depth, d_model, ff), BF16),
            pltpu.VMEM((2, ff, EARLY * CHUNK), BF16),
            pltpu.VMEM((2, nd, FEW, d_model), BF16),
            pltpu.VMEM((2, nd, SLOT, d_model), BF16),
            dma((depth, 2, 2)), dma((2,)), dma((2,)),
        ],
        compiler_params=pltpu.CompilerParams(vmem_limit_bytes=33_800_000),
        name="routed_hidden",
    )(cnt, xg, w1, w3, w2, pltpu.with_memory_space_constraint(pre1, pltpu.VMEM),
      pltpu.with_memory_space_constraint(pre3, pltpu.VMEM))


def down_kernel(hv, g_hbm, hsh_ref, w2_hbm, sd_hbm, y_ref,
                gv, wb, sdb, ob, snd, kept, in0, in1, in2,
                gsem, wsem, dsem, s0s, s0r, s1s, s1r, s2s, s2r):
    me, core, sib, xn, yn, dg = neighbours()
    n_exp, full, _ = hv.shape
    ff = w2_hbm.shape[1]
    nd = gv.shape[0]
    rows = gv.shape[1] // 3
    n_chunks = snd.shape[0]
    width = wb.shape[3]
    depth = wb.shape[0]
    hw = width // 2

    barrier = pltpu.get_barrier_semaphore()
    for dev in (sib, xn, yn):
        pl.semaphore_signal(barrier, inc=1, device_id={"ep": dev}, device_id_type=MESH)

    def wcopy(c, e):
        cols = pl.ds(pl.multiple_of(c * width, width), width)
        slot = c % depth
        return pltpu.make_async_copy(w2_hbm.at[e, :, cols], wb.at[slot, e], wsem.at[slot, e])

    def dcopy(c):
        cols = pl.ds(pl.multiple_of(c * width, width), width)
        return pltpu.make_async_copy(sd_hbm.at[:, cols], sdb.at[c], dsem.at[c])

    gcopy = pltpu.make_async_copy(g_hbm, gv, gsem)
    early = (hv.shape[2] - ff) // width
    gcopy.start()
    for e in range(n_exp):
        wcopy(early, e).start()

    own_c, xn_c, yn_c, dg_c = me // 2, xn // 2, yn // 2, dg // 2
    orders = ((own_c, yn_c, xn_c, dg_c), (own_c, xn_c, yn_c, dg_c))
    first_hop = (xn, yn)
    second_hop = (yn, xn)

    def send0(c):
        return rcopy(snd.at[c], in0.at[c], s0s.at[c], s0r.at[c], sib)

    def send1(c, q):
        return rcopy(kept.at[c, q, pl.ds(2, 2)], in1.at[c, q], s1s.at[c, q], s1r.at[c, q], first_hop[q])

    def send2(c, q):
        return rcopy(kept.at[c, q, 1], in2.at[c, q], s2s.at[c, q], s2r.at[c, q], second_hop[q])

    def step0(c):
        send0(c).wait_recv()
        kept[c] = kept[c] + in0[c]

    def step1(c):
        for q in range(2):
            send1(c, q).wait_recv()
            kept[c, q, 0:2] = kept[c, q, 0:2] + in1[c, q]

    def step2(c):
        for q in range(2):
            send2(c, q).wait_recv()
            kept[c, q, 0] = kept[c, q, 0] + in2[c, q]

    def start1(c):
        send1(c, 0).start()
        send1(c, 1).start()

    def start2(c):
        send2(c, 0).start()
        send2(c, 1).start()

    def expert(c, e):
        out = jnp.dot(hv[e, :, 0:ff], wb[c % depth, e], preferred_element_type=F32)
        out = out.astype(BF16).astype(F32)
        ob[:, e] = out.reshape(nd, SLOT, width)

    def gated(d, o):
        r = jnp.dot(gv[d], o, preferred_element_type=F32)
        return r[0:rows] + r[rows:2 * rows] + r[2 * rows:3 * rows]

    def chunk(c, carry):
        for e0 in range(0, n_exp, GROUP):
            for e in range(e0, e0 + GROUP):
                wcopy(c, e).wait()
            for e in range(e0, e0 + GROUP):
                expert(c, e)

            @pl.when(c + depth < n_chunks)
            def _():
                for e in range(e0, e0 + GROUP):
                    wcopy(c + depth, e).start()

            if e0 == 0:
                step0(c - 1)
                start1(c - 1)

                @pl.when(c == early)
                def _():
                    for i in range(early - 2):
                        step1(i)
                        start2(i)

        dcopy(c).start()
        reduce_start(c, lambda d: ob[d].reshape(n_exp * SLOT, width).astype(BF16))
        step1(c - 2)
        start2(c - 2)
        return carry

    def reduce_start(c, rows_of):
        chips = (own_c, xn_c, yn_c, dg_c)
        where = ((0, 0), (2, 1), (1, 2), (3, 3))
        for chip, (p0, p1) in zip(chips, where):
            d = 2 * chip + 1 - core
            r = gated(d, rows_of(d))
            snd[c, 0, p0] = r[:, 0:hw]
            snd[c, 1, p1] = r[:, hw:width]
        for chip, (p0, p1) in zip(chips, where):
            d = 2 * chip + core
            r = gated(d, rows_of(d))
            kept[c, 0, p0] = r[:, 0:hw]
            kept[c, 1, p1] = r[:, hw:width]

        send0(c).start()

    pl.semaphore_wait(barrier, 3)
    gcopy.wait()
    for c in range(early):
        cols = slice(ff + c * width, ff + (c + 1) * width)
        reduce_start(c, lambda d: hv[:, pl.ds(pl.multiple_of(d * SLOT, SLOT), SLOT), cols].reshape(n_exp * SLOT, width))
    for c in range(early + 1, early + depth):
        for e in range(n_exp):
            wcopy(c, e).start()
    for c in range(early):
        dcopy(c).start()
    for c in range(early - 1):
        step0(c)
        start1(c)
    lax.fori_loop(early, n_chunks, chunk, 0)

    def shared(c):
        dcopy(c).wait()
        cols = pl.ds(pl.multiple_of(c * width, width), width)
        s = jnp.dot(hsh_ref[...], sdb[c], preferred_element_type=F32).astype(BF16)
        y_ref[:, cols] = s

    def shared_range(lo, hi):
        def body(c, carry):
            shared(c)
            return carry
        lax.fori_loop(lo, hi, body, 0)

    def finish_range(lo, hi):
        def body(c, carry):
            step2(c)
            for q in range(2):
                cols = pl.ds(pl.multiple_of(c * width + q * hw, hw), hw)
                y_ref[:, cols] = (y_ref[:, cols].astype(F32) + kept[c, q, 0]).astype(BF16)
            return carry
        lax.fori_loop(lo, hi, body, 0)

    last = n_chunks - 1
    shared_range(0, 3)
    step0(last)
    start1(last)
    shared_range(3, n_chunks)
    step1(last - 1)
    start2(last - 1)
    finish_range(0, last - 1)
    step1(last)
    start2(last)
    finish_range(last - 1, n_chunks)

    def drain(c, carry):
        send0(c).wait_send()
        for q in range(2):
            send1(c, q).wait_send()
            send2(c, q).wait_send()
        return carry

    lax.fori_loop(0, n_chunks, drain, 0)


def down_call(h, g, hsh, w2, sd):
    n_exp, full, _ = h.shape
    ff = w2.shape[1]
    nd, rows3, width_g = g.shape
    rows = rows3 // 3
    d_model = w2.shape[2]
    width = CHUNK
    n_chunks = d_model // width
    depth = 3
    hw = width // 2
    any_spec = pl.BlockSpec(memory_space=pl.ANY)
    vmem = pl.BlockSpec(memory_space=pltpu.VMEM)
    dma = pltpu.SemaphoreType.DMA
    return pl.pallas_call(
        down_kernel,
        out_shape=jax.ShapeDtypeStruct((rows, d_model), BF16),
        in_specs=[vmem, any_spec, vmem, any_spec, any_spec],
        out_specs=vmem,
        scratch_shapes=[
            pltpu.VMEM((nd, rows3, width_g), BF16),
            pltpu.VMEM((depth, n_exp, ff, width), BF16),
            pltpu.VMEM((n_chunks, sd.shape[0], width), BF16),
            pltpu.VMEM((nd, n_exp, SLOT, width), F32),
            pltpu.VMEM((n_chunks, 2, 4, rows, hw), F32),
            pltpu.VMEM((n_chunks, 2, 4, rows, hw), F32),
            pltpu.VMEM((n_chunks, 2, 4, rows, hw), F32),
            pltpu.VMEM((n_chunks, 2, 2, rows, hw), F32),
            pltpu.VMEM((n_chunks, 2, rows, hw), F32),
            dma(()), dma((depth, n_exp)), dma((n_chunks,)),
            dma((n_chunks,)), dma((n_chunks,)),
            dma((n_chunks, 2)), dma((n_chunks, 2)), dma((n_chunks, 2)), dma((n_chunks, 2)),
        ],
        compiler_params=pltpu.CompilerParams(
            collective_id=1, has_side_effects=True, vmem_limit_bytes=55_000_000),
        name="down_reduce",
    )(pltpu.with_memory_space_constraint(h, pltpu.VMEM), g, hsh, w2, sd)


def solution(mesh):
    nd = mesh.shape["ep"]

    def device_fn(x, route, gates, w_gate, w_up, w_down, sg, su, sd):
        xg, hsh, cnt, g, pre1, pre3 = gather_call(x, route.T, gates.T, sg, su, w_gate, w_up, nd)
        h = hidden_call(cnt, xg, w_gate, w_up, w_down, pre1, pre3)
        return down_call(h.reshape(h.shape[0], -1, h.shape[3]), g, hsh, w_down, sd)

    tok = P(("dp", "ep"), None)
    exp = P("ep", None, None)
    rep = P(None, None)
    return jax.shard_map(device_fn, mesh=mesh, in_specs=(tok, tok, tok, exp, exp, exp, rep, rep, rep),
                         out_specs=tok, check_vma=False)
```

```python
import functools

import jax
import jax.numpy as jnp
from jax import lax
from jax.experimental import pallas as pl
from jax.experimental.pallas import tpu as pltpu
from jax.sharding import PartitionSpec as P

MESH = pl.DeviceIdType.MESH
CAP = 36
SLOT = 40
VMEM_LIMIT = 67_000_000
H_BYTES = 10_500_000
CHUNK = 256
GROUP = 8
EARLY = 1
PRE = 2
PRE_BYTES = 23_500_000
BF16 = jnp.bfloat16
F32 = jnp.float32


def neighbours():
    me = lax.axis_index("ep")
    core = me % 2
    xb = (me // 2) % 2
    yb = me // 4
    sib = me + 1 - 2 * core
    xn = me + 2 - 4 * xb
    yn = me + 4 - 8 * yb
    dg = yn + 2 - 4 * xb
    return me, core, sib, xn, yn, dg


def rcopy(src, dst, send, recv, dev):
    return pltpu.make_async_remote_copy(
        src_ref=src, dst_ref=dst, send_sem=send, recv_sem=recv,
        device_id={"ep": dev}, device_id_type=MESH)


def gather_kernel(x_hbm, route_hbm, gate_hbm, sg_hbm, su_hbm, w1_hbm, w3_hbm,
                  xg_hbm, hsh_hbm, cnt_hbm, g_hbm, pre1, pre3,
                  x_ref, route_ref, gate_ref, land, meta_s, bg, bu, metal, stage, hsh, gv, cntv,
                  isem, wsem, osem, psem, gsem, hsem, csem,
                  sx_s, sx_r, sy_s, sy_r, f_s, f_r, ss_s, ss_r, m_s, m_r):
    me, core, sib, xn, yn, dg = neighbours()
    sxn = xn + 1 - 2 * core
    syn = yn + 1 - 2 * core
    sdg = dg + 1 - 2 * core
    nd = land.shape[0]
    rows, d_model = x_ref.shape
    half = rows // 2
    ring = bg.shape[0]
    width = bg.shape[2]
    n_chunks = sg_hbm.shape[1] // width
    n_all = 8 * nd

    ins = [pltpu.make_async_copy(src, dst, isem.at[i]) for i, (src, dst) in enumerate(
        ((route_hbm, route_ref), (gate_hbm, gate_ref), (x_hbm, x_ref)))]
    for c in ins:
        c.start()
    barrier = pltpu.get_barrier_semaphore()
    for r in range(1, nd):
        pl.semaphore_signal(barrier, inc=1, device_id={"ep": (me + r) % nd}, device_id_type=MESH)

    def wcopy(i):
        cols = pl.ds(pl.multiple_of(i * width, width), width)
        slot = i % ring
        return (pltpu.make_async_copy(sg_hbm.at[:, cols], bg.at[slot], wsem.at[0, slot]),
                pltpu.make_async_copy(su_hbm.at[:, cols], bu.at[slot], wsem.at[1, slot]))

    for i in range(ring):
        for c in wcopy(i):
            c.start()

    def pcopy(e):
        return (pltpu.make_async_copy(w1_hbm.at[e], pre1.at[e], psem.at[0, e]),
                pltpu.make_async_copy(w3_hbm.at[e], pre3.at[e], psem.at[1, e]))

    def prefetch(e):
        for c in pcopy(e):
            c.start()

    ins[0].wait()
    ins[1].wait()
    ids = lax.broadcasted_iota(jnp.int32, (n_all, rows), 0)
    mask = jnp.zeros((n_all, rows), F32)
    gmap = jnp.zeros((n_all, rows), F32)
    for k in range(route_ref.shape[0]):
        eq = route_ref[k:k + 1, :] == ids
        mask = mask + jnp.where(eq, 1.0, 0.0)
        gmap = gmap + jnp.where(eq, gate_ref[k:k + 1, :], 0.0)
    before = (lax.broadcasted_iota(jnp.int32, (rows, rows), 0)
              < lax.broadcasted_iota(jnp.int32, (rows, rows), 1))
    rank = jnp.dot(mask.astype(BF16), jnp.where(before, 1.0, 0.0).astype(BF16), preferred_element_type=F32)
    rank = jnp.where(mask > 0.0, rank, -1.0)
    fill = jnp.zeros((n_all, 128 - rows), F32)
    rank = jnp.concatenate([rank, fill - 1.0], axis=1)
    gmap = jnp.concatenate([gmap, fill], axis=1)
    for j in range(nd):
        meta_s[j, 0:8, :] = rank[8 * j:8 * j + 8]
        meta_s[j, 8:16, :] = gmap[8 * j:8 * j + 8]
    metal[me] = meta_s[me]

    def hs(h):
        return pl.ds(h * half, half)

    pl.semaphore_wait(barrier, nd - 1)
    metas = []
    for r in range(1, nd):
        dst = (me + r) % nd
        c = rcopy(meta_s.at[dst], metal.at[me], m_s.at[r - 1], m_r.at[r - 1], dst)
        c.start()
        metas.append(c)
    ins[2].wait()
    own_x = [rcopy(x_ref.at[hs(h)], land.at[me, hs(h)], sx_s.at[h], sx_r.at[h], xn) for h in range(2)]
    own_y = [rcopy(x_ref.at[hs(h)], land.at[me, hs(h)], sy_s.at[h], sy_r.at[h], yn) for h in range(2)]
    own_s = rcopy(x_ref, land.at[me], ss_s.at[0], ss_r.at[0], sib)
    own_x[0].start()
    own_y[1].start()
    own_x[1].start()
    own_y[0].start()
    own_s.start()

    def shared_range(lo, hi):
        def body(i, carry):
            for c in wcopy(i):
                c.wait()
            a = jnp.dot(x_ref[...], bg[i % ring], preferred_element_type=F32)
            b = jnp.dot(x_ref[...], bu[i % ring], preferred_element_type=F32)
            cols = pl.ds(pl.multiple_of(i * width, width), width)
            hsh[:, cols] = (jax.nn.silu(a) * b).astype(BF16)

            @pl.when(i + ring < n_chunks)
            def _():
                for c in wcopy(i + ring):
                    c.start()
            return carry
        lax.fori_loop(lo, hi, body, 0)

    shared_range(0, n_chunks - 6)
    prefetch(0)

    for c in metas:
        c.wait_recv()

    for d in range(nd):
        n = jnp.sum(jnp.where(metal[d, 0:8, :] >= 0.0, 1.0, 0.0), axis=1, keepdims=True)
        cntv[d] = jnp.broadcast_to(n, (8, 128)).astype(jnp.int32)
    ccopy = pltpu.make_async_copy(cntv, cnt_hbm, csem)
    ccopy.start()

    def pick(d, x_rows, k):
        buf = k % 2
        if k >= 2:
            outs[k - 2].wait()
        slot = lax.broadcasted_iota(jnp.int32, (SLOT, rows), 0).astype(F32)
        sel = jnp.concatenate(
            [jnp.where(metal[d, e:e + 1, 0:rows] == slot, 1.0, 0.0) for e in range(8)], axis=0).astype(BF16)
        for c0 in range(0, d_model, 512):
            r = jnp.dot(sel, x_rows[:, c0:c0 + 512], preferred_element_type=F32)
            stage[buf, :, :, c0:c0 + 512] = r.astype(BF16).reshape(8, SLOT, 512)
        c = pltpu.make_async_copy(stage.at[buf], xg_hbm.at[:, d], osem.at[k])
        c.start()
        outs.append(c)

    outs = []
    pick(me, x_ref, 0)
    own_s.wait_recv()
    pick(sib, land.at[sib], 1)

    own_x[0].wait_recv()
    fy = rcopy(land.at[xn, hs(0)], land.at[xn, hs(0)], f_s.at[0], f_r.at[0], yn)
    fy.start()
    sx0 = rcopy(land.at[xn, hs(0)], land.at[xn, hs(0)], ss_s.at[1], ss_r.at[1], sib)
    sx0.start()
    own_y[1].wait_recv()
    fx = rcopy(land.at[yn, hs(1)], land.at[yn, hs(1)], f_s.at[1], f_r.at[1], xn)
    fx.start()
    sy1 = rcopy(land.at[yn, hs(1)], land.at[yn, hs(1)], ss_s.at[2], ss_r.at[2], sib)
    sy1.start()

    shared_range(n_chunks - 6, n_chunks)
    for e in range(1, pre1.shape[0]):
        prefetch(e)
    hcopy = pltpu.make_async_copy(hsh, hsh_hbm, hsem)
    hcopy.start()

    width_g = 8 * SLOT
    lane = lax.broadcasted_iota(jnp.int32, (8, width_g), 1)
    sel = jnp.where(lane // SLOT == lax.broadcasted_iota(jnp.int32, (8, width_g), 0), 1.0, 0.0)
    slot_id = (lax.broadcasted_iota(jnp.int32, (rows, width_g), 1) % SLOT).astype(F32)

    def spread(v):
        return lax.dot_general(v, sel, (((0,), (0,)), ((), ())), preferred_element_type=F32)[:rows]

    def gate_body(d, carry):
        rk = metal[d, 0:8, :]
        gt = metal[d, 8:16, :]
        hi = gt.astype(BF16).astype(F32)
        mid = (gt - hi).astype(BF16).astype(F32)
        lo = gt - hi - mid
        eq = spread(rk) == slot_id
        for q, part in enumerate((hi, mid, lo)):
            gv[d, q * rows:(q + 1) * rows, :] = jnp.where(eq, spread(part), 0.0).astype(BF16)
        return carry

    lax.fori_loop(0, nd, gate_body, 0)
    gcopy = pltpu.make_async_copy(gv, g_hbm, gsem)
    gcopy.start()

    own_x[1].wait_recv()
    sx1 = rcopy(land.at[xn, hs(1)], land.at[xn, hs(1)], ss_s.at[3], ss_r.at[3], sib)
    sx1.start()
    own_y[0].wait_recv()
    sy0 = rcopy(land.at[yn, hs(0)], land.at[yn, hs(0)], ss_s.at[4], ss_r.at[4], sib)
    sy0.start()
    pick(xn, land.at[xn], 2)
    pick(yn, land.at[yn], 3)
    sx0.wait_recv()
    sx1.wait_recv()
    pick(sxn, land.at[sxn], 4)
    sy1.wait_recv()
    sy0.wait_recv()
    pick(syn, land.at[syn], 5)

    fy.wait_recv()
    sd0 = rcopy(land.at[dg, hs(0)], land.at[dg, hs(0)], ss_s.at[5], ss_r.at[5], sib)
    sd0.start()
    fx.wait_recv()
    sd1 = rcopy(land.at[dg, hs(1)], land.at[dg, hs(1)], ss_s.at[6], ss_r.at[6], sib)
    sd1.start()
    pick(dg, land.at[dg], 6)
    sd0.wait_recv()
    sd1.wait_recv()
    pick(sdg, land.at[sdg], 7)
    for c in own_x + own_y + [own_s, fy, fx, sx0, sx1, sy0, sy1, sd0, sd1] + metas:
        c.wait_send()
    for c in outs[6:] + [ccopy, hcopy, gcopy]:
        c.wait()
    for e in range(pre1.shape[0]):
        for c in pcopy(e):
            c.wait()


def gather_call(x, route, gates, sg, su, w1, w3, nd):
    rows, d_model = x.shape
    ff = sg.shape[1]
    width = 256
    ring = 8
    any_spec = pl.BlockSpec(memory_space=pl.ANY)
    vmem = pl.BlockSpec(memory_space=pltpu.VMEM)
    dma = pltpu.SemaphoreType.DMA
    return pl.pallas_call(
        gather_kernel,
        out_shape=(
            jax.ShapeDtypeStruct((8, nd, SLOT, d_model), BF16),
            jax.ShapeDtypeStruct((rows, ff), BF16),
            jax.ShapeDtypeStruct((nd, 8, 128), jnp.int32),
            jax.ShapeDtypeStruct((nd, 3 * rows, 8 * SLOT), BF16),
            pltpu.VMEM((PRE,) + w1.shape[1:], BF16),
            pltpu.VMEM((PRE,) + w3.shape[1:], BF16),
        ),
        in_specs=[any_spec] * 7,
        out_specs=(pl.BlockSpec(memory_space=pltpu.HBM),) * 4 + (vmem, vmem),
        scratch_shapes=[
            pltpu.VMEM(x.shape, BF16),
            pltpu.VMEM(route.shape, jnp.int32),
            pltpu.VMEM(gates.shape, F32),
            pltpu.VMEM((nd, rows, d_model), BF16),
            pltpu.VMEM((nd, 16, 128), F32),
            pltpu.VMEM((ring, d_model, width), BF16),
            pltpu.VMEM((ring, d_model, width), BF16),
            pltpu.VMEM((nd, 16, 128), F32),
            pltpu.VMEM((2, 8, SLOT, d_model), BF16),
            pltpu.VMEM((rows, ff), BF16),
            pltpu.VMEM((nd, 3 * rows, 8 * SLOT), BF16),
            pltpu.VMEM((nd, 8, 128), jnp.int32),
            dma((3,)), dma((2, ring)),
            dma((8,)), dma((2, PRE)), dma(()), dma(()), dma(()),
            dma((2,)), dma((2,)), dma((2,)), dma((2,)), dma((2,)), dma((2,)),
            dma((7,)), dma((7,)), dma((7,)), dma((7,)),
        ],
        compiler_params=pltpu.CompilerParams(
            collective_id=0, has_side_effects=True, vmem_limit_bytes=33_800_000),
        name="gather_shared",
    )(x, route, gates, sg, su, w1, w3)


FEW = 16


def hidden_kernel(cnt_hbm, xg_hbm, w1_hbm, w3_hbm, w2_hbm, pre1, pre3, h_ref,
                  cnt, wb1, wb3, wb2, xfew, xall, csem, wsem, dsem, xsem):
    n_exp, d_model, ff = w1_hbm.shape
    nd = cnt.shape[0]
    depth = wb1.shape[0]
    first = pre1.shape[0]
    bounds = [(c, min(256, ff - c)) for c in range(0, ff, 256)]
    cut = 3 * 256
    groups = ((0, cut, bounds[:3]), (cut, ff - cut, bounds[3:]))

    def wcopy(e, slot, j):
        c0, w, _ = groups[j]
        return (pltpu.make_async_copy(w1_hbm.at[e, :, c0:c0 + w], wb1.at[slot, :, c0:c0 + w], wsem.at[slot, 0, j]),
                pltpu.make_async_copy(w3_hbm.at[e, :, c0:c0 + w], wb3.at[slot, :, c0:c0 + w], wsem.at[slot, 1, j]))

    def few(e):
        top = cnt[0, e, 0]
        for d in range(1, nd):
            top = jnp.maximum(top, cnt[d, e, 0])
        return top <= FEW

    def few_copy(e):
        return pltpu.make_async_copy(xg_hbm.at[e, :, pl.ds(0, FEW)], xfew.at[e % 2], xsem.at[e % 2])

    def all_copy(e):
        return pltpu.make_async_copy(xg_hbm.at[e], xall.at[e % 2], xsem.at[e % 2])

    def rows_start(e):
        @pl.when(few(e))
        def _():
            few_copy(e).start()

        @pl.when(jnp.logical_not(few(e)))
        def _():
            all_copy(e).start()

    early_w = wb2.shape[2]

    def dcopy(e):
        return pltpu.make_async_copy(w2_hbm.at[e, :, pl.ds(0, early_w)], wb2.at[e % 2], dsem.at[e % 2])

    ccopy = pltpu.make_async_copy(cnt_hbm, cnt, csem)
    ccopy.start()
    dcopy(0).start()
    dcopy(1).start()
    for e in range(first, first + depth):
        for j in range(len(groups)):
            for c in wcopy(e, e % depth, j):
                c.start()
    ccopy.wait()
    rows_start(0)
    rows_start(1)
    for e in range(n_exp):
        h_ref[e, :, FEW:SLOT, :] = jnp.zeros((nd, SLOT - FEW, h_ref.shape[3]), BF16)

    def hidden(rows_ref, up, gate, c0, w):
        m = rows_ref.shape[0] * rows_ref.shape[1]
        a = jnp.dot(rows_ref[...].reshape(m, d_model), gate[:, c0:c0 + w], preferred_element_type=F32)
        b = jnp.dot(rows_ref[...].reshape(m, d_model), up[:, c0:c0 + w], preferred_element_type=F32)
        return (jax.nn.silu(a) * b).astype(BF16).reshape(rows_ref.shape[0], rows_ref.shape[1], w)

    def down(e, slots):
        rows = h_ref[e, :, 0:slots, 0:ff].reshape(nd * slots, ff)
        for c0 in range(0, early_w, 256):
            out = jnp.dot(rows, wb2[e % 2, :, c0:c0 + 256], preferred_element_type=F32)
            h_ref[e, :, 0:slots, ff + c0:ff + c0 + 256] = out.astype(BF16).reshape(nd, slots, 256)

    def expert(e, gate, up, wait, refill):
        small = few(e)

        @pl.when(small)
        def _():
            few_copy(e).wait()
            for j, (_, _, cols) in enumerate(groups):
                wait(j)
                for c0, w in cols:
                    h_ref[e, :, 0:FEW, c0:c0 + w] = hidden(xfew.at[e % 2], up, gate, c0, w)
                refill(j)
            dcopy(e).wait()
            down(e, FEW)

        @pl.when(jnp.logical_not(small))
        def _():
            all_copy(e).wait()
            for j, (_, _, cols) in enumerate(groups):
                wait(j)
                for c0, w in cols:
                    h_ref[e, :, :, c0:c0 + w] = hidden(xall.at[e % 2], up, gate, c0, w)
                refill(j)
            dcopy(e).wait()
            down(e, SLOT)

        @pl.when(e + 2 < n_exp)
        def _():
            rows_start(e + 2)
            dcopy(e + 2).start()

    def early(e, carry):
        expert(e, pre1.at[e], pre3.at[e], lambda j: None, lambda j: None)
        return carry

    def late(e, carry):
        slot = e % depth

        def wait(j):
            for c in wcopy(e, slot, j):
                c.wait()

        def refill(j):
            @pl.when(e + depth < n_exp)
            def _():
                for c in wcopy(e + depth, slot, j):
                    c.start()

        expert(e, wb1.at[slot], wb3.at[slot], wait, refill)
        return carry

    lax.fori_loop(0, first, early, 0)
    lax.fori_loop(first, n_exp, late, 0)


def hidden_call(cnt, xg, w1, w3, w2, pre1, pre3):
    n_exp, d_model, ff = w1.shape
    nd = cnt.shape[0]
    depth = 2
    any_spec = pl.BlockSpec(memory_space=pl.ANY)
    vmem = pl.BlockSpec(memory_space=pltpu.VMEM)
    dma = pltpu.SemaphoreType.DMA
    return pl.pallas_call(
        hidden_kernel,
        out_shape=pltpu.VMEM((n_exp, nd, SLOT, ff + EARLY * CHUNK), BF16),
        in_specs=[any_spec] * 5 + [vmem, vmem],
        out_specs=vmem,
        scratch_shapes=[
            pltpu.SMEM(cnt.shape, jnp.int32),
            pltpu.VMEM((depth, d_model, ff), BF16),
            pltpu.VMEM((depth, d_model, ff), BF16),
            pltpu.VMEM((2, ff, EARLY * CHUNK), BF16),
            pltpu.VMEM((2, nd, FEW, d_model), BF16),
            pltpu.VMEM((2, nd, SLOT, d_model), BF16),
            dma(()), dma((depth, 2, 2)), dma((2,)), dma((2,)),
        ],
        compiler_params=pltpu.CompilerParams(vmem_limit_bytes=33_800_000),
        name="routed_hidden",
    )(cnt, xg, w1, w3, w2, pltpu.with_memory_space_constraint(pre1, pltpu.VMEM),
      pltpu.with_memory_space_constraint(pre3, pltpu.VMEM))


def down_kernel(hv, g_hbm, hsh_hbm, w2_hbm, sd_hbm, y_hbm,
                hsh_ref, y_ref, gv, wb, sdb, ob, snd, kept, in0, in1, in2,
                isem, ysem, gsem, wsem, dsem, s0s, s0r, s1s, s1r, s2s, s2r):
    me, core, sib, xn, yn, dg = neighbours()
    n_exp, full, _ = hv.shape
    ff = w2_hbm.shape[1]
    nd = gv.shape[0]
    rows = gv.shape[1] // 3
    n_chunks = snd.shape[0]
    width = wb.shape[3]
    depth = wb.shape[0]
    hw = width // 2

    barrier = pltpu.get_barrier_semaphore()
    for dev in (sib, xn, yn):
        pl.semaphore_signal(barrier, inc=1, device_id={"ep": dev}, device_id_type=MESH)

    def wcopy(c, e):
        cols = pl.ds(pl.multiple_of(c * width, width), width)
        slot = c % depth
        return pltpu.make_async_copy(w2_hbm.at[e, :, cols], wb.at[slot, e], wsem.at[slot, e])

    def dcopy(c):
        cols = pl.ds(pl.multiple_of(c * width, width), width)
        return pltpu.make_async_copy(sd_hbm.at[:, cols], sdb.at[c], dsem.at[c])

    gcopy = pltpu.make_async_copy(g_hbm, gv, gsem)
    early = (hv.shape[2] - ff) // width
    gcopy.start()
    for e in range(n_exp):
        wcopy(early, e).start()
    scopy = pltpu.make_async_copy(hsh_hbm, hsh_ref, isem)
    scopy.start()

    own_c, xn_c, yn_c, dg_c = me // 2, xn // 2, yn // 2, dg // 2
    orders = ((own_c, yn_c, xn_c, dg_c), (own_c, xn_c, yn_c, dg_c))
    first_hop = (xn, yn)
    second_hop = (yn, xn)

    def send0(c):
        return rcopy(snd.at[c], in0.at[c], s0s.at[c], s0r.at[c], sib)

    def send1(c, q):
        return rcopy(kept.at[c, q, pl.ds(2, 2)], in1.at[c, q], s1s.at[c, q], s1r.at[c, q], first_hop[q])

    def send2(c, q):
        return rcopy(kept.at[c, q, 1], in2.at[c, q], s2s.at[c, q], s2r.at[c, q], second_hop[q])

    def step0(c):
        send0(c).wait_recv()
        kept[c] = kept[c] + in0[c]

    def step1(c):
        for q in range(2):
            send1(c, q).wait_recv()
            kept[c, q, 0:2] = kept[c, q, 0:2] + in1[c, q]

    def step2(c):
        for q in range(2):
            send2(c, q).wait_recv()
            kept[c, q, 0] = kept[c, q, 0] + in2[c, q]

    def start1(c):
        send1(c, 0).start()
        send1(c, 1).start()

    def start2(c):
        send2(c, 0).start()
        send2(c, 1).start()

    def expert(c, e):
        out = jnp.dot(hv[e, :, 0:ff], wb[c % depth, e], preferred_element_type=F32)
        out = out.astype(BF16).astype(F32)
        ob[:, e] = out.reshape(nd, SLOT, width)

    def gated(d, o):
        r = jnp.dot(gv[d], o, preferred_element_type=F32)
        return r[0:rows] + r[rows:2 * rows] + r[2 * rows:3 * rows]

    def chunk(c, carry):
        for e0 in range(0, n_exp, GROUP):
            for e in range(e0, e0 + GROUP):
                wcopy(c, e).wait()
            for e in range(e0, e0 + GROUP):
                expert(c, e)

            @pl.when(c + depth < n_chunks)
            def _():
                for e in range(e0, e0 + GROUP):
                    wcopy(c + depth, e).start()

            if e0 == 0:
                step0(c - 1)
                start1(c - 1)

                @pl.when(c == early)
                def _():
                    for i in range(early - 2):
                        step1(i)
                        start2(i)

        dcopy(c).start()
        reduce_start(c, lambda d: ob[d].reshape(n_exp * SLOT, width).astype(BF16))

        @pl.when(c >= 2)
        def _():
            step1(c - 2)
            start2(c - 2)
        return carry

    def reduce_start(c, rows_of):
        chips = (own_c, xn_c, yn_c, dg_c)
        where = ((0, 0), (2, 1), (1, 2), (3, 3))
        for chip, (p0, p1) in zip(chips, where):
            d = 2 * chip + 1 - core
            r = gated(d, rows_of(d))
            snd[c, 0, p0] = r[:, 0:hw]
            snd[c, 1, p1] = r[:, hw:width]
        for chip, (p0, p1) in zip(chips, where):
            d = 2 * chip + core
            r = gated(d, rows_of(d))
            kept[c, 0, p0] = r[:, 0:hw]
            kept[c, 1, p1] = r[:, hw:width]

        send0(c).start()

    pl.semaphore_wait(barrier, 3)
    gcopy.wait()
    for c in range(early):
        cols = slice(ff + c * width, ff + (c + 1) * width)
        reduce_start(c, lambda d: hv[:, pl.ds(pl.multiple_of(d * SLOT, SLOT), SLOT), cols].reshape(n_exp * SLOT, width))
    for c in range(early + 1, early + depth):
        for e in range(n_exp):
            wcopy(c, e).start()
    for c in range(early):
        dcopy(c).start()
    for c in range(early - 1):
        step0(c)
        start1(c)
    lax.fori_loop(early, n_chunks, chunk, 0)

    def shared(c):
        dcopy(c).wait()
        cols = pl.ds(pl.multiple_of(c * width, width), width)
        s = jnp.dot(hsh_ref[...], sdb[c], preferred_element_type=F32).astype(BF16)
        y_ref[:, cols] = s

    def shared_range(lo, hi):
        def body(c, carry):
            shared(c)
            return carry
        lax.fori_loop(lo, hi, body, 0)

    def finish_range(lo, hi):
        def body(c, carry):
            step2(c)
            for q in range(2):
                cols = pl.ds(pl.multiple_of(c * width + q * hw, hw), hw)
                y_ref[:, cols] = (y_ref[:, cols].astype(F32) + kept[c, q, 0]).astype(BF16)
            return carry
        lax.fori_loop(lo, hi, body, 0)

    last = n_chunks - 1
    scopy.wait()
    shared_range(0, 3)
    step0(last)
    start1(last)
    shared_range(3, n_chunks)
    step1(last - 1)
    start2(last - 1)
    finish_range(0, last - 1)
    cut = (last - 1) * width
    ycopies = [pltpu.make_async_copy(y_ref.at[:, a:b], y_hbm.at[:, a:b], ysem.at[i])
               for i, (a, b) in enumerate(((0, cut), (cut, n_chunks * width)))]
    ycopies[0].start()
    step1(last)
    start2(last)
    finish_range(last - 1, n_chunks)
    ycopies[1].start()

    def drain(c, carry):
        send0(c).wait_send()
        for q in range(2):
            send1(c, q).wait_send()
            send2(c, q).wait_send()
        return carry

    lax.fori_loop(0, n_chunks, drain, 0)
    for c in ycopies:
        c.wait()


def down_call(h, g, hsh, w2, sd):
    n_exp, full, _ = h.shape
    ff = w2.shape[1]
    nd, rows3, width_g = g.shape
    rows = rows3 // 3
    d_model = w2.shape[2]
    width = CHUNK
    n_chunks = d_model // width
    depth = 3
    hw = width // 2
    any_spec = pl.BlockSpec(memory_space=pl.ANY)
    vmem = pl.BlockSpec(memory_space=pltpu.VMEM)
    dma = pltpu.SemaphoreType.DMA
    return pl.pallas_call(
        down_kernel,
        out_shape=jax.ShapeDtypeStruct((rows, d_model), BF16),
        in_specs=[vmem] + [any_spec] * 4,
        out_specs=pl.BlockSpec(memory_space=pltpu.HBM),
        scratch_shapes=[
            pltpu.VMEM(hsh.shape, BF16),
            pltpu.VMEM((rows, d_model), BF16),
            pltpu.VMEM((nd, rows3, width_g), BF16),
            pltpu.VMEM((depth, n_exp, ff, width), BF16),
            pltpu.VMEM((n_chunks, sd.shape[0], width), BF16),
            pltpu.VMEM((nd, n_exp, SLOT, width), F32),
            pltpu.VMEM((n_chunks, 2, 4, rows, hw), F32),
            pltpu.VMEM((n_chunks, 2, 4, rows, hw), F32),
            pltpu.VMEM((n_chunks, 2, 4, rows, hw), F32),
            pltpu.VMEM((n_chunks, 2, 2, rows, hw), F32),
            pltpu.VMEM((n_chunks, 2, rows, hw), F32),
            dma(()), dma((2,)), dma(()), dma((depth, n_exp)), dma((n_chunks,)),
            dma((n_chunks,)), dma((n_chunks,)),
            dma((n_chunks, 2)), dma((n_chunks, 2)), dma((n_chunks, 2)), dma((n_chunks, 2)),
        ],
        compiler_params=pltpu.CompilerParams(
            collective_id=1, has_side_effects=True, vmem_limit_bytes=55_000_000),
        name="down_reduce",
    )(pltpu.with_memory_space_constraint(h, pltpu.VMEM), g, hsh, w2, sd)


def solution(mesh):
    nd = mesh.shape["ep"]

    def device_fn(x, route, gates, w_gate, w_up, w_down, sg, su, sd):
        xg, hsh, cnt, g, pre1, pre3 = gather_call(x, route.T, gates.T, sg, su, w_gate, w_up, nd)
        h = hidden_call(cnt, xg, w_gate, w_up, w_down, pre1, pre3)
        return down_call(h.reshape(h.shape[0], -1, h.shape[3]), g, hsh, w_down, sd)

    tok = P(("dp", "ep"), None)
    exp = P("ep", None, None)
    rep = P(None, None)
    return jax.shard_map(device_fn, mesh=mesh, in_specs=(tok, tok, tok, exp, exp, exp, rep, rep, rep),
                         out_specs=tok, check_vma=False)
```

```python
import functools

import jax
import jax.numpy as jnp
from jax import lax
from jax.experimental import pallas as pl
from jax.experimental.pallas import tpu as pltpu
from jax.sharding import PartitionSpec as P

MESH = pl.DeviceIdType.MESH
CAP = 36
SLOT = 40
VMEM_LIMIT = 67_000_000
H_BYTES = 10_500_000
CHUNK = 256
GROUP = 4
EARLY = 1
PRE = 2
PRE_BYTES = 23_500_000
BF16 = jnp.bfloat16
F32 = jnp.float32


def neighbours():
    me = lax.axis_index("ep")
    core = me % 2
    xb = (me // 2) % 2
    yb = me // 4
    sib = me + 1 - 2 * core
    xn = me + 2 - 4 * xb
    yn = me + 4 - 8 * yb
    dg = yn + 2 - 4 * xb
    return me, core, sib, xn, yn, dg


def rcopy(src, dst, send, recv, dev):
    return pltpu.make_async_remote_copy(
        src_ref=src, dst_ref=dst, send_sem=send, recv_sem=recv,
        device_id={"ep": dev}, device_id_type=MESH)


def gather_kernel(x_hbm, route_hbm, gate_hbm, sg_hbm, su_hbm, w1_hbm, w3_hbm, w2_hbm,
                  xg_hbm, hsh_hbm, cnt_hbm, g_hbm, pre1, pre3, pre2,
                  x_ref, route_ref, gate_ref, land, meta_s, bg, bu, metal, stage, hsh, gv, cntv,
                  isem, wsem, osem, psem, p2sem, gsem, hsem, csem,
                  sx_s, sx_r, sy_s, sy_r, f_s, f_r, ss_s, ss_r, m_s, m_r):
    me, core, sib, xn, yn, dg = neighbours()
    sxn = xn + 1 - 2 * core
    syn = yn + 1 - 2 * core
    sdg = dg + 1 - 2 * core
    nd = land.shape[0]
    rows, d_model = x_ref.shape
    half = rows // 2
    ring = bg.shape[0]
    width = bg.shape[2]
    n_chunks = sg_hbm.shape[1] // width
    n_all = 8 * nd

    ins = [pltpu.make_async_copy(src, dst, isem.at[i]) for i, (src, dst) in enumerate(
        ((route_hbm, route_ref), (gate_hbm, gate_ref), (x_hbm, x_ref)))]
    for c in ins:
        c.start()
    barrier = pltpu.get_barrier_semaphore()
    for r in range(1, nd):
        pl.semaphore_signal(barrier, inc=1, device_id={"ep": (me + r) % nd}, device_id_type=MESH)

    def wcopy(i):
        cols = pl.ds(pl.multiple_of(i * width, width), width)
        slot = i % ring
        return (pltpu.make_async_copy(sg_hbm.at[:, cols], bg.at[slot], wsem.at[0, slot]),
                pltpu.make_async_copy(su_hbm.at[:, cols], bu.at[slot], wsem.at[1, slot]))

    for i in range(ring):
        for c in wcopy(i):
            c.start()

    def pcopy(e):
        return (pltpu.make_async_copy(w1_hbm.at[e], pre1.at[e], psem.at[0, e]),
                pltpu.make_async_copy(w3_hbm.at[e], pre3.at[e], psem.at[1, e]))

    def prefetch(e):
        for c in pcopy(e):
            c.start()

    ins[0].wait()
    ins[1].wait()
    ids = lax.broadcasted_iota(jnp.int32, (n_all, rows), 0)
    mask = jnp.zeros((n_all, rows), F32)
    gmap = jnp.zeros((n_all, rows), F32)
    for k in range(route_ref.shape[0]):
        eq = route_ref[k:k + 1, :] == ids
        mask = mask + jnp.where(eq, 1.0, 0.0)
        gmap = gmap + jnp.where(eq, gate_ref[k:k + 1, :], 0.0)
    before = (lax.broadcasted_iota(jnp.int32, (rows, rows), 0)
              < lax.broadcasted_iota(jnp.int32, (rows, rows), 1))
    rank = jnp.dot(mask.astype(BF16), jnp.where(before, 1.0, 0.0).astype(BF16), preferred_element_type=F32)
    rank = jnp.where(mask > 0.0, rank, -1.0)
    fill = jnp.zeros((n_all, 128 - rows), F32)
    rank = jnp.concatenate([rank, fill - 1.0], axis=1)
    gmap = jnp.concatenate([gmap, fill], axis=1)
    for j in range(nd):
        meta_s[j, 0:8, :] = rank[8 * j:8 * j + 8]
        meta_s[j, 8:16, :] = gmap[8 * j:8 * j + 8]
    metal[me] = meta_s[me]

    def hs(h):
        return pl.ds(h * half, half)

    pl.semaphore_wait(barrier, nd - 1)
    metas = []
    for r in range(1, nd):
        dst = (me + r) % nd
        c = rcopy(meta_s.at[dst], metal.at[me], m_s.at[r - 1], m_r.at[r - 1], dst)
        c.start()
        metas.append(c)
    ins[2].wait()
    own_x = [rcopy(x_ref.at[hs(h)], land.at[me, hs(h)], sx_s.at[h], sx_r.at[h], xn) for h in range(2)]
    own_y = [rcopy(x_ref.at[hs(h)], land.at[me, hs(h)], sy_s.at[h], sy_r.at[h], yn) for h in range(2)]
    own_s = rcopy(x_ref, land.at[me], ss_s.at[0], ss_r.at[0], sib)
    own_x[0].start()
    own_y[1].start()
    own_x[1].start()
    own_y[0].start()
    own_s.start()

    def shared_range(lo, hi):
        def body(i, carry):
            for c in wcopy(i):
                c.wait()
            a = jnp.dot(x_ref[...], bg[i % ring], preferred_element_type=F32)
            b = jnp.dot(x_ref[...], bu[i % ring], preferred_element_type=F32)
            cols = pl.ds(pl.multiple_of(i * width, width), width)
            hsh[:, cols] = (jax.nn.silu(a) * b).astype(BF16)

            @pl.when(i + ring < n_chunks)
            def _():
                for c in wcopy(i + ring):
                    c.start()
            return carry
        lax.fori_loop(lo, hi, body, 0)

    shared_range(0, n_chunks - 6)
    prefetch(0)

    for c in metas:
        c.wait_recv()

    for d in range(nd):
        n = jnp.sum(jnp.where(metal[d, 0:8, :] >= 0.0, 1.0, 0.0), axis=1, keepdims=True)
        cntv[d] = jnp.broadcast_to(n, (8, 128)).astype(jnp.int32)
    ccopy = pltpu.make_async_copy(cntv, cnt_hbm, csem)
    ccopy.start()

    def pick(d, x_rows, k):
        buf = k % 2
        if k >= 2:
            outs[k - 2].wait()
        slot = lax.broadcasted_iota(jnp.int32, (SLOT, rows), 0).astype(F32)
        sel = jnp.concatenate(
            [jnp.where(metal[d, e:e + 1, 0:rows] == slot, 1.0, 0.0) for e in range(8)], axis=0).astype(BF16)
        for c0 in range(0, d_model, 512):
            r = jnp.dot(sel, x_rows[:, c0:c0 + 512], preferred_element_type=F32)
            stage[buf, :, :, c0:c0 + 512] = r.astype(BF16).reshape(8, SLOT, 512)
        c = pltpu.make_async_copy(stage.at[buf], xg_hbm.at[:, d], osem.at[k])
        c.start()
        outs.append(c)

    outs = []
    pick(me, x_ref, 0)
    own_s.wait_recv()
    pick(sib, land.at[sib], 1)

    own_x[0].wait_recv()
    fy = rcopy(land.at[xn, hs(0)], land.at[xn, hs(0)], f_s.at[0], f_r.at[0], yn)
    fy.start()
    sx0 = rcopy(land.at[xn, hs(0)], land.at[xn, hs(0)], ss_s.at[1], ss_r.at[1], sib)
    sx0.start()
    own_y[1].wait_recv()
    fx = rcopy(land.at[yn, hs(1)], land.at[yn, hs(1)], f_s.at[1], f_r.at[1], xn)
    fx.start()
    sy1 = rcopy(land.at[yn, hs(1)], land.at[yn, hs(1)], ss_s.at[2], ss_r.at[2], sib)
    sy1.start()

    shared_range(n_chunks - 6, n_chunks)
    for e in range(1, pre1.shape[0]):
        prefetch(e)
    p2copy = pltpu.make_async_copy(w2_hbm.at[:, :, pl.ds(0, pre2.shape[2])], pre2, p2sem)
    p2copy.start()
    hcopy = pltpu.make_async_copy(hsh, hsh_hbm, hsem)
    hcopy.start()

    width_g = 8 * SLOT
    lane = lax.broadcasted_iota(jnp.int32, (8, width_g), 1)
    sel = jnp.where(lane // SLOT == lax.broadcasted_iota(jnp.int32, (8, width_g), 0), 1.0, 0.0)
    slot_id = (lax.broadcasted_iota(jnp.int32, (rows, width_g), 1) % SLOT).astype(F32)

    def spread(v):
        return lax.dot_general(v, sel, (((0,), (0,)), ((), ())), preferred_element_type=F32)[:rows]

    def gate_body(d, carry):
        rk = metal[d, 0:8, :]
        gt = metal[d, 8:16, :]
        hi = gt.astype(BF16).astype(F32)
        mid = (gt - hi).astype(BF16).astype(F32)
        lo = gt - hi - mid
        eq = spread(rk) == slot_id
        for q, part in enumerate((hi, mid, lo)):
            gv[d, q * rows:(q + 1) * rows, :] = jnp.where(eq, spread(part), 0.0).astype(BF16)
        return carry

    lax.fori_loop(0, nd, gate_body, 0)
    gcopy = pltpu.make_async_copy(gv, g_hbm, gsem)
    gcopy.start()

    own_x[1].wait_recv()
    sx1 = rcopy(land.at[xn, hs(1)], land.at[xn, hs(1)], ss_s.at[3], ss_r.at[3], sib)
    sx1.start()
    own_y[0].wait_recv()
    sy0 = rcopy(land.at[yn, hs(0)], land.at[yn, hs(0)], ss_s.at[4], ss_r.at[4], sib)
    sy0.start()
    pick(xn, land.at[xn], 2)
    pick(yn, land.at[yn], 3)
    sx0.wait_recv()
    sx1.wait_recv()
    pick(sxn, land.at[sxn], 4)
    sy1.wait_recv()
    sy0.wait_recv()
    pick(syn, land.at[syn], 5)

    fy.wait_recv()
    sd0 = rcopy(land.at[dg, hs(0)], land.at[dg, hs(0)], ss_s.at[5], ss_r.at[5], sib)
    sd0.start()
    fx.wait_recv()
    sd1 = rcopy(land.at[dg, hs(1)], land.at[dg, hs(1)], ss_s.at[6], ss_r.at[6], sib)
    sd1.start()
    pick(dg, land.at[dg], 6)
    sd0.wait_recv()
    sd1.wait_recv()
    pick(sdg, land.at[sdg], 7)
    for c in own_x + own_y + [own_s, fy, fx, sx0, sx1, sy0, sy1, sd0, sd1] + metas:
        c.wait_send()
    for c in outs[6:] + [ccopy, hcopy, gcopy, p2copy]:
        c.wait()
    for e in range(pre1.shape[0]):
        for c in pcopy(e):
            c.wait()


def gather_call(x, route, gates, sg, su, w1, w3, w2, nd):
    rows, d_model = x.shape
    ff = sg.shape[1]
    width = 256
    ring = 8
    any_spec = pl.BlockSpec(memory_space=pl.ANY)
    vmem = pl.BlockSpec(memory_space=pltpu.VMEM)
    dma = pltpu.SemaphoreType.DMA
    return pl.pallas_call(
        gather_kernel,
        out_shape=(
            jax.ShapeDtypeStruct((8, nd, SLOT, d_model), BF16),
            jax.ShapeDtypeStruct((rows, ff), BF16),
            jax.ShapeDtypeStruct((nd, 8, 128), jnp.int32),
            jax.ShapeDtypeStruct((nd, 3 * rows, 8 * SLOT), BF16),
            pltpu.VMEM((PRE,) + w1.shape[1:], BF16),
            pltpu.VMEM((PRE,) + w3.shape[1:], BF16),
            pltpu.VMEM(w2.shape[:2] + (EARLY * CHUNK,), BF16),
        ),
        in_specs=[any_spec] * 8,
        out_specs=(pl.BlockSpec(memory_space=pltpu.HBM),) * 4 + (vmem, vmem, vmem),
        scratch_shapes=[
            pltpu.VMEM(x.shape, BF16),
            pltpu.VMEM(route.shape, jnp.int32),
            pltpu.VMEM(gates.shape, F32),
            pltpu.VMEM((nd, rows, d_model), BF16),
            pltpu.VMEM((nd, 16, 128), F32),
            pltpu.VMEM((ring, d_model, width), BF16),
            pltpu.VMEM((ring, d_model, width), BF16),
            pltpu.VMEM((nd, 16, 128), F32),
            pltpu.VMEM((2, 8, SLOT, d_model), BF16),
            pltpu.VMEM((rows, ff), BF16),
            pltpu.VMEM((nd, 3 * rows, 8 * SLOT), BF16),
            pltpu.VMEM((nd, 8, 128), jnp.int32),
            dma((3,)), dma((2, ring)),
            dma((8,)), dma((2, PRE)), dma(()), dma(()), dma(()), dma(()),
            dma((2,)), dma((2,)), dma((2,)), dma((2,)), dma((2,)), dma((2,)),
            dma((7,)), dma((7,)), dma((7,)), dma((7,)),
        ],
        compiler_params=pltpu.CompilerParams(
            collective_id=0, has_side_effects=True, vmem_limit_bytes=29_500_000),
        name="gather_shared",
    )(x, route, gates, sg, su, w1, w3, w2)


FEW = 16


def hidden_kernel(cnt_hbm, xg_hbm, w1_hbm, w3_hbm, pre1, pre3, pre2, h_ref,
                  cnt, wb1, wb3, xfew, xall, csem, wsem, xsem):
    n_exp, d_model, ff = w1_hbm.shape
    nd = cnt.shape[0]
    depth = wb1.shape[0]
    first = pre1.shape[0]
    bounds = [(c, min(256, ff - c)) for c in range(0, ff, 256)]
    cut = 3 * 256
    groups = ((0, cut, bounds[:3]), (cut, ff - cut, bounds[3:]))

    def wcopy(e, slot, j):
        c0, w, _ = groups[j]
        return (pltpu.make_async_copy(w1_hbm.at[e, :, c0:c0 + w], wb1.at[slot, :, c0:c0 + w], wsem.at[slot, 0, j]),
                pltpu.make_async_copy(w3_hbm.at[e, :, c0:c0 + w], wb3.at[slot, :, c0:c0 + w], wsem.at[slot, 1, j]))

    def few(e):
        top = cnt[0, e, 0]
        for d in range(1, nd):
            top = jnp.maximum(top, cnt[d, e, 0])
        return top <= FEW

    def few_copy(e):
        return pltpu.make_async_copy(xg_hbm.at[e, :, pl.ds(0, FEW)], xfew.at[e % 2], xsem.at[e % 2])

    def all_copy(e):
        return pltpu.make_async_copy(xg_hbm.at[e], xall.at[e % 2], xsem.at[e % 2])

    def rows_start(e):
        @pl.when(few(e))
        def _():
            few_copy(e).start()

        @pl.when(jnp.logical_not(few(e)))
        def _():
            all_copy(e).start()

    ccopy = pltpu.make_async_copy(cnt_hbm, cnt, csem)
    ccopy.start()
    for e in range(first, first + depth):
        for j in range(len(groups)):
            for c in wcopy(e, e % depth, j):
                c.start()
    ccopy.wait()
    rows_start(0)
    rows_start(1)
    for e in range(n_exp):
        h_ref[e, :, FEW:SLOT, :] = jnp.zeros((nd, SLOT - FEW, h_ref.shape[3]), BF16)

    def hidden(rows_ref, up, gate, c0, w):
        m = rows_ref.shape[0] * rows_ref.shape[1]
        a = jnp.dot(rows_ref[...].reshape(m, d_model), gate[:, c0:c0 + w], preferred_element_type=F32)
        b = jnp.dot(rows_ref[...].reshape(m, d_model), up[:, c0:c0 + w], preferred_element_type=F32)
        return (jax.nn.silu(a) * b).astype(BF16).reshape(rows_ref.shape[0], rows_ref.shape[1], w)

    def down(e, slots):
        rows = h_ref[e, :, 0:slots, 0:ff].reshape(nd * slots, ff)
        for c0 in range(0, pre2.shape[2], 256):
            out = jnp.dot(rows, pre2[e, :, c0:c0 + 256], preferred_element_type=F32)
            h_ref[e, :, 0:slots, ff + c0:ff + c0 + 256] = out.astype(BF16).reshape(nd, slots, 256)

    def expert(e, gate, up, wait, refill):
        small = few(e)

        @pl.when(small)
        def _():
            few_copy(e).wait()
            for j, (_, _, cols) in enumerate(groups):
                wait(j)
                for c0, w in cols:
                    h_ref[e, :, 0:FEW, c0:c0 + w] = hidden(xfew.at[e % 2], up, gate, c0, w)
                refill(j)
            down(e, FEW)

        @pl.when(jnp.logical_not(small))
        def _():
            all_copy(e).wait()
            for j, (_, _, cols) in enumerate(groups):
                wait(j)
                for c0, w in cols:
                    h_ref[e, :, :, c0:c0 + w] = hidden(xall.at[e % 2], up, gate, c0, w)
                refill(j)
            down(e, SLOT)

        @pl.when(e + 2 < n_exp)
        def _():
            rows_start(e + 2)

    def early(e, carry):
        expert(e, pre1.at[e], pre3.at[e], lambda j: None, lambda j: None)
        return carry

    def late(e, carry):
        slot = e % depth

        def wait(j):
            for c in wcopy(e, slot, j):
                c.wait()

        def refill(j):
            @pl.when(e + depth < n_exp)
            def _():
                for c in wcopy(e + depth, slot, j):
                    c.start()

        expert(e, wb1.at[slot], wb3.at[slot], wait, refill)
        return carry

    lax.fori_loop(0, first, early, 0)
    lax.fori_loop(first, n_exp, late, 0)


def hidden_call(cnt, xg, w1, w3, pre1, pre3, pre2):
    n_exp, d_model, ff = w1.shape
    nd = cnt.shape[0]
    depth = 2
    any_spec = pl.BlockSpec(memory_space=pl.ANY)
    vmem = pl.BlockSpec(memory_space=pltpu.VMEM)
    dma = pltpu.SemaphoreType.DMA
    return pl.pallas_call(
        hidden_kernel,
        out_shape=pltpu.VMEM((n_exp, nd, SLOT, ff + EARLY * CHUNK), BF16),
        in_specs=[any_spec] * 4 + [vmem] * 3,
        out_specs=vmem,
        scratch_shapes=[
            pltpu.SMEM(cnt.shape, jnp.int32),
            pltpu.VMEM((depth, d_model, ff), BF16),
            pltpu.VMEM((depth, d_model, ff), BF16),
            pltpu.VMEM((2, nd, FEW, d_model), BF16),
            pltpu.VMEM((2, nd, SLOT, d_model), BF16),
            dma(()), dma((depth, 2, 2)), dma((2,)),
        ],
        compiler_params=pltpu.CompilerParams(vmem_limit_bytes=29_500_000),
        name="routed_hidden",
    )(cnt, xg, w1, w3, pltpu.with_memory_space_constraint(pre1, pltpu.VMEM),
      pltpu.with_memory_space_constraint(pre3, pltpu.VMEM),
      pltpu.with_memory_space_constraint(pre2, pltpu.VMEM))


def down_kernel(hv, g_hbm, hsh_hbm, w2_hbm, sd_hbm, y_hbm,
                hsh_ref, y_ref, gv, wb, sdb, ob, snd, kept, in0, in1, in2,
                isem, ysem, gsem, wsem, dsem, s0s, s0r, s1s, s1r, s2s, s2r):
    me, core, sib, xn, yn, dg = neighbours()
    n_exp, full, _ = hv.shape
    ff = w2_hbm.shape[1]
    nd = gv.shape[0]
    rows = gv.shape[1] // 3
    n_chunks = snd.shape[0]
    width = wb.shape[3]
    depth = wb.shape[0]
    hw = width // 2

    barrier = pltpu.get_barrier_semaphore()
    for dev in (sib, xn, yn):
        pl.semaphore_signal(barrier, inc=1, device_id={"ep": dev}, device_id_type=MESH)

    def wcopy(c, e):
        cols = pl.ds(pl.multiple_of(c * width, width), width)
        slot = c % depth
        return pltpu.make_async_copy(w2_hbm.at[e, :, cols], wb.at[slot, e], wsem.at[slot, e])

    def dcopy(c):
        cols = pl.ds(pl.multiple_of(c * width, width), width)
        return pltpu.make_async_copy(sd_hbm.at[:, cols], sdb.at[c], dsem.at[c])

    gcopy = pltpu.make_async_copy(g_hbm, gv, gsem)
    early = (hv.shape[2] - ff) // width
    gcopy.start()
    for e in range(n_exp):
        wcopy(early, e).start()
    scopy = pltpu.make_async_copy(hsh_hbm, hsh_ref, isem)
    scopy.start()

    own_c, xn_c, yn_c, dg_c = me // 2, xn // 2, yn // 2, dg // 2
    orders = ((own_c, yn_c, xn_c, dg_c), (own_c, xn_c, yn_c, dg_c))
    first_hop = (xn, yn)
    second_hop = (yn, xn)

    def send0(c):
        return rcopy(snd.at[c], in0.at[c], s0s.at[c], s0r.at[c], sib)

    def send1(c, q):
        return rcopy(kept.at[c, q, pl.ds(2, 2)], in1.at[c, q], s1s.at[c, q], s1r.at[c, q], first_hop[q])

    def send2(c, q):
        return rcopy(kept.at[c, q, 1], in2.at[c, q], s2s.at[c, q], s2r.at[c, q], second_hop[q])

    def step0(c):
        send0(c).wait_recv()
        kept[c] = kept[c] + in0[c]

    def step1(c):
        for q in range(2):
            send1(c, q).wait_recv()
            kept[c, q, 0:2] = kept[c, q, 0:2] + in1[c, q]

    def step2(c):
        for q in range(2):
            send2(c, q).wait_recv()
            kept[c, q, 0] = kept[c, q, 0] + in2[c, q]

    def start1(c):
        send1(c, 0).start()
        send1(c, 1).start()

    def start2(c):
        send2(c, 0).start()
        send2(c, 1).start()

    def expert(c, e):
        out = jnp.dot(hv[e, :, 0:ff], wb[c % depth, e], preferred_element_type=F32)
        out = out.astype(BF16).astype(F32)
        ob[:, e] = out.reshape(nd, SLOT, width)

    def gated(d, o):
        r = jnp.dot(gv[d], o, preferred_element_type=F32)
        return r[0:rows] + r[rows:2 * rows] + r[2 * rows:3 * rows]

    def chunk(c, carry):
        for e0 in range(0, n_exp, GROUP):
            for e in range(e0, e0 + GROUP):
                wcopy(c, e).wait()
            for e in range(e0, e0 + GROUP):
                expert(c, e)

            @pl.when(c + depth < n_chunks)
            def _():
                for e in range(e0, e0 + GROUP):
                    wcopy(c + depth, e).start()

            if e0 == 0:
                step0(c - 1)
                start1(c - 1)

                @pl.when(c == early)
                def _():
                    for i in range(early - 2):
                        step1(i)
                        start2(i)

        dcopy(c).start()
        reduce_start(c, lambda d: ob[d].reshape(n_exp * SLOT, width).astype(BF16))

        @pl.when(c >= 2)
        def _():
            step1(c - 2)
            start2(c - 2)
        return carry

    def reduce_start(c, rows_of):
        chips = (own_c, xn_c, yn_c, dg_c)
        where = ((0, 0), (2, 1), (1, 2), (3, 3))
        for chip, (p0, p1) in zip(chips, where):
            d = 2 * chip + 1 - core
            r = gated(d, rows_of(d))
            snd[c, 0, p0] = r[:, 0:hw]
            snd[c, 1, p1] = r[:, hw:width]
        for chip, (p0, p1) in zip(chips, where):
            d = 2 * chip + core
            r = gated(d, rows_of(d))
            kept[c, 0, p0] = r[:, 0:hw]
            kept[c, 1, p1] = r[:, hw:width]

        send0(c).start()

    pl.semaphore_wait(barrier, 3)
    gcopy.wait()
    for c in range(early):
        cols = slice(ff + c * width, ff + (c + 1) * width)
        reduce_start(c, lambda d: hv[:, pl.ds(pl.multiple_of(d * SLOT, SLOT), SLOT), cols].reshape(n_exp * SLOT, width))
    for c in range(early + 1, early + depth):
        for e in range(n_exp):
            wcopy(c, e).start()
    for c in range(early):
        dcopy(c).start()
    for c in range(early - 1):
        step0(c)
        start1(c)
    lax.fori_loop(early, n_chunks, chunk, 0)

    def shared(c):
        dcopy(c).wait()
        cols = pl.ds(pl.multiple_of(c * width, width), width)
        s = jnp.dot(hsh_ref[...], sdb[c], preferred_element_type=F32).astype(BF16)
        y_ref[:, cols] = s

    def shared_range(lo, hi):
        def body(c, carry):
            shared(c)
            return carry
        lax.fori_loop(lo, hi, body, 0)

    def finish_range(lo, hi):
        def body(c, carry):
            step2(c)
            for q in range(2):
                cols = pl.ds(pl.multiple_of(c * width + q * hw, hw), hw)
                y_ref[:, cols] = (y_ref[:, cols].astype(F32) + kept[c, q, 0]).astype(BF16)
            return carry
        lax.fori_loop(lo, hi, body, 0)

    last = n_chunks - 1
    scopy.wait()
    shared_range(0, 3)
    step0(last)
    start1(last)
    shared_range(3, n_chunks)
    step1(last - 1)
    start2(last - 1)
    finish_range(0, last - 1)
    cut = (last - 1) * width
    ycopies = [pltpu.make_async_copy(y_ref.at[:, a:b], y_hbm.at[:, a:b], ysem.at[i])
               for i, (a, b) in enumerate(((0, cut), (cut, n_chunks * width)))]
    ycopies[0].start()
    step1(last)
    start2(last)
    finish_range(last - 1, n_chunks)
    ycopies[1].start()

    def drain(c, carry):
        send0(c).wait_send()
        for q in range(2):
            send1(c, q).wait_send()
            send2(c, q).wait_send()
        return carry

    lax.fori_loop(0, n_chunks, drain, 0)
    for c in ycopies:
        c.wait()


def down_call(h, g, hsh, w2, sd):
    n_exp, full, _ = h.shape
    ff = w2.shape[1]
    nd, rows3, width_g = g.shape
    rows = rows3 // 3
    d_model = w2.shape[2]
    width = CHUNK
    n_chunks = d_model // width
    depth = 3
    hw = width // 2
    any_spec = pl.BlockSpec(memory_space=pl.ANY)
    vmem = pl.BlockSpec(memory_space=pltpu.VMEM)
    dma = pltpu.SemaphoreType.DMA
    return pl.pallas_call(
        down_kernel,
        out_shape=jax.ShapeDtypeStruct((rows, d_model), BF16),
        in_specs=[vmem] + [any_spec] * 4,
        out_specs=pl.BlockSpec(memory_space=pltpu.HBM),
        scratch_shapes=[
            pltpu.VMEM(hsh.shape, BF16),
            pltpu.VMEM((rows, d_model), BF16),
            pltpu.VMEM((nd, rows3, width_g), BF16),
            pltpu.VMEM((depth, n_exp, ff, width), BF16),
            pltpu.VMEM((n_chunks, sd.shape[0], width), BF16),
            pltpu.VMEM((nd, n_exp, SLOT, width), F32),
            pltpu.VMEM((n_chunks, 2, 4, rows, hw), F32),
            pltpu.VMEM((n_chunks, 2, 4, rows, hw), F32),
            pltpu.VMEM((n_chunks, 2, 4, rows, hw), F32),
            pltpu.VMEM((n_chunks, 2, 2, rows, hw), F32),
            pltpu.VMEM((n_chunks, 2, rows, hw), F32),
            dma(()), dma((2,)), dma(()), dma((depth, n_exp)), dma((n_chunks,)),
            dma((n_chunks,)), dma((n_chunks,)),
            dma((n_chunks, 2)), dma((n_chunks, 2)), dma((n_chunks, 2)), dma((n_chunks, 2)),
        ],
        compiler_params=pltpu.CompilerParams(
            collective_id=1, has_side_effects=True, vmem_limit_bytes=55_000_000),
        name="down_reduce",
    )(pltpu.with_memory_space_constraint(h, pltpu.VMEM), g, hsh, w2, sd)


def solution(mesh):
    nd = mesh.shape["ep"]

    def device_fn(x, route, gates, w_gate, w_up, w_down, sg, su, sd):
        xg, hsh, cnt, g, *pre = gather_call(x, route.T, gates.T, sg, su, w_gate, w_up, w_down, nd)
        h = hidden_call(cnt, xg, w_gate, w_up, *pre)
        return down_call(h.reshape(h.shape[0], -1, h.shape[3]), g, hsh, w_down, sd)

    tok = P(("dp", "ep"), None)
    exp = P("ep", None, None)
    rep = P(None, None)
    return jax.shard_map(device_fn, mesh=mesh, in_specs=(tok, tok, tok, exp, exp, exp, rep, rep, rep),
                         out_specs=tok, check_vma=False)
```

```python
import functools

import jax
import jax.numpy as jnp
from jax import lax
from jax.experimental import pallas as pl
from jax.experimental.pallas import tpu as pltpu
from jax.sharding import PartitionSpec as P

MESH = pl.DeviceIdType.MESH
CAP = 36
SLOT = 40
VMEM_LIMIT = 67_000_000
H_BYTES = 10_500_000
CHUNK = 256
GROUP = 8
EARLY = 1
PRE = 2
PRE_BYTES = 23_500_000
BF16 = jnp.bfloat16
F32 = jnp.float32


def neighbours():
    me = lax.axis_index("ep")
    core = me % 2
    xb = (me // 2) % 2
    yb = me // 4
    sib = me + 1 - 2 * core
    xn = me + 2 - 4 * xb
    yn = me + 4 - 8 * yb
    dg = yn + 2 - 4 * xb
    return me, core, sib, xn, yn, dg


def rcopy(src, dst, send, recv, dev):
    return pltpu.make_async_remote_copy(
        src_ref=src, dst_ref=dst, send_sem=send, recv_sem=recv,
        device_id={"ep": dev}, device_id_type=MESH)


def gather_kernel(x_hbm, route_hbm, gate_hbm, sg_hbm, su_hbm, w1_hbm, w3_hbm, w2_hbm,
                  xg_hbm, hsh_hbm, cnt_hbm, g_hbm, pre1, pre3, pre2,
                  x_ref, route_ref, gate_ref, land, meta_s, bg, bu, metal, stage, hsh, gv, cntv,
                  isem, wsem, osem, psem, p2sem, gsem, hsem, csem,
                  sx_s, sx_r, sy_s, sy_r, f_s, f_r, ss_s, ss_r, m_s, m_r):
    me, core, sib, xn, yn, dg = neighbours()
    sxn = xn + 1 - 2 * core
    syn = yn + 1 - 2 * core
    sdg = dg + 1 - 2 * core
    nd = land.shape[0]
    rows, d_model = x_ref.shape
    half = rows // 2
    ring = bg.shape[0]
    width = bg.shape[2]
    n_chunks = sg_hbm.shape[1] // width
    n_all = 8 * nd

    ins = [pltpu.make_async_copy(src, dst, isem.at[i]) for i, (src, dst) in enumerate(
        ((route_hbm, route_ref), (gate_hbm, gate_ref), (x_hbm, x_ref)))]
    for c in ins:
        c.start()
    barrier = pltpu.get_barrier_semaphore()
    for r in range(1, nd):
        pl.semaphore_signal(barrier, inc=1, device_id={"ep": (me + r) % nd}, device_id_type=MESH)

    def wcopy(i):
        cols = pl.ds(pl.multiple_of(i * width, width), width)
        slot = i % ring
        return (pltpu.make_async_copy(sg_hbm.at[:, cols], bg.at[slot], wsem.at[0, slot]),
                pltpu.make_async_copy(su_hbm.at[:, cols], bu.at[slot], wsem.at[1, slot]))

    for i in range(ring):
        for c in wcopy(i):
            c.start()

    def pcopy(e):
        return (pltpu.make_async_copy(w1_hbm.at[e], pre1.at[e], psem.at[0, e]),
                pltpu.make_async_copy(w3_hbm.at[e], pre3.at[e], psem.at[1, e]))

    def prefetch(e):
        for c in pcopy(e):
            c.start()

    ins[0].wait()
    ins[1].wait()
    ids = lax.broadcasted_iota(jnp.int32, (n_all, rows), 0)
    mask = jnp.zeros((n_all, rows), F32)
    gmap = jnp.zeros((n_all, rows), F32)
    for k in range(route_ref.shape[0]):
        eq = route_ref[k:k + 1, :] == ids
        mask = mask + jnp.where(eq, 1.0, 0.0)
        gmap = gmap + jnp.where(eq, gate_ref[k:k + 1, :], 0.0)
    before = (lax.broadcasted_iota(jnp.int32, (rows, rows), 0)
              < lax.broadcasted_iota(jnp.int32, (rows, rows), 1))
    rank = jnp.dot(mask.astype(BF16), jnp.where(before, 1.0, 0.0).astype(BF16), preferred_element_type=F32)
    rank = jnp.where(mask > 0.0, rank, -1.0)
    fill = jnp.zeros((n_all, 128 - rows), F32)
    rank = jnp.concatenate([rank, fill - 1.0], axis=1)
    gmap = jnp.concatenate([gmap, fill], axis=1)
    for j in range(nd):
        meta_s[j, 0:8, :] = rank[8 * j:8 * j + 8]
        meta_s[j, 8:16, :] = gmap[8 * j:8 * j + 8]
    metal[me] = meta_s[me]

    def hs(h):
        return pl.ds(h * half, half)

    pl.semaphore_wait(barrier, nd - 1)
    metas = []
    for r in range(1, nd):
        dst = (me + r) % nd
        c = rcopy(meta_s.at[dst], metal.at[me], m_s.at[r - 1], m_r.at[r - 1], dst)
        c.start()
        metas.append(c)
    ins[2].wait()
    own_x = [rcopy(x_ref.at[hs(h)], land.at[me, hs(h)], sx_s.at[h], sx_r.at[h], xn) for h in range(2)]
    own_y = [rcopy(x_ref.at[hs(h)], land.at[me, hs(h)], sy_s.at[h], sy_r.at[h], yn) for h in range(2)]
    own_s = rcopy(x_ref, land.at[me], ss_s.at[0], ss_r.at[0], sib)
    own_x[0].start()
    own_y[1].start()
    own_x[1].start()
    own_y[0].start()
    own_s.start()

    def shared_range(lo, hi):
        def body(i, carry):
            for c in wcopy(i):
                c.wait()
            a = jnp.dot(x_ref[...], bg[i % ring], preferred_element_type=F32)
            b = jnp.dot(x_ref[...], bu[i % ring], preferred_element_type=F32)
            cols = pl.ds(pl.multiple_of(i * width, width), width)
            hsh[:, cols] = (jax.nn.silu(a) * b).astype(BF16)

            @pl.when(i + ring < n_chunks)
            def _():
                for c in wcopy(i + ring):
                    c.start()
            return carry
        lax.fori_loop(lo, hi, body, 0)

    shared_range(0, n_chunks - 6)
    prefetch(0)

    for c in metas:
        c.wait_recv()

    for d in range(nd):
        n = jnp.sum(jnp.where(metal[d, 0:8, :] >= 0.0, 1.0, 0.0), axis=1, keepdims=True)
        cntv[d] = jnp.broadcast_to(n, (8, 128)).astype(jnp.int32)
    ccopy = pltpu.make_async_copy(cntv, cnt_hbm, csem)
    ccopy.start()

    def pick(d, x_rows, k):
        buf = k % 2
        if k >= 2:
            outs[k - 2].wait()
        slot = lax.broadcasted_iota(jnp.int32, (SLOT, rows), 0).astype(F32)
        sel = jnp.concatenate(
            [jnp.where(metal[d, e:e + 1, 0:rows] == slot, 1.0, 0.0) for e in range(8)], axis=0).astype(BF16)
        for c0 in range(0, d_model, 512):
            r = jnp.dot(sel, x_rows[:, c0:c0 + 512], preferred_element_type=F32)
            stage[buf, :, :, c0:c0 + 512] = r.astype(BF16).reshape(8, SLOT, 512)
        c = pltpu.make_async_copy(stage.at[buf], xg_hbm.at[:, d], osem.at[k])
        c.start()
        outs.append(c)

    outs = []
    pick(me, x_ref, 0)
    own_s.wait_recv()
    pick(sib, land.at[sib], 1)

    own_x[0].wait_recv()
    fy = rcopy(land.at[xn, hs(0)], land.at[xn, hs(0)], f_s.at[0], f_r.at[0], yn)
    fy.start()
    sx0 = rcopy(land.at[xn, hs(0)], land.at[xn, hs(0)], ss_s.at[1], ss_r.at[1], sib)
    sx0.start()
    own_y[1].wait_recv()
    fx = rcopy(land.at[yn, hs(1)], land.at[yn, hs(1)], f_s.at[1], f_r.at[1], xn)
    fx.start()
    sy1 = rcopy(land.at[yn, hs(1)], land.at[yn, hs(1)], ss_s.at[2], ss_r.at[2], sib)
    sy1.start()

    shared_range(n_chunks - 6, n_chunks)
    for e in range(1, pre1.shape[0]):
        prefetch(e)
    p2copy = pltpu.make_async_copy(w2_hbm.at[:, :, pl.ds(0, pre2.shape[2])], pre2, p2sem)
    p2copy.start()
    hcopy = pltpu.make_async_copy(hsh, hsh_hbm, hsem)
    hcopy.start()

    width_g = 8 * SLOT
    lane = lax.broadcasted_iota(jnp.int32, (8, width_g), 1)
    sel = jnp.where(lane // SLOT == lax.broadcasted_iota(jnp.int32, (8, width_g), 0), 1.0, 0.0)
    slot_id = (lax.broadcasted_iota(jnp.int32, (rows, width_g), 1) % SLOT).astype(F32)

    def spread(v):
        return lax.dot_general(v, sel, (((0,), (0,)), ((), ())), preferred_element_type=F32)[:rows]

    def gate_body(d, carry):
        rk = metal[d, 0:8, :]
        gt = metal[d, 8:16, :]
        hi = gt.astype(BF16).astype(F32)
        mid = (gt - hi).astype(BF16).astype(F32)
        lo = gt - hi - mid
        eq = spread(rk) == slot_id
        for q, part in enumerate((hi, mid, lo)):
            gv[d, q * rows:(q + 1) * rows, :] = jnp.where(eq, spread(part), 0.0).astype(BF16)
        return carry

    lax.fori_loop(0, nd, gate_body, 0)
    gcopy = pltpu.make_async_copy(gv, g_hbm, gsem)
    gcopy.start()

    own_x[1].wait_recv()
    sx1 = rcopy(land.at[xn, hs(1)], land.at[xn, hs(1)], ss_s.at[3], ss_r.at[3], sib)
    sx1.start()
    own_y[0].wait_recv()
    sy0 = rcopy(land.at[yn, hs(0)], land.at[yn, hs(0)], ss_s.at[4], ss_r.at[4], sib)
    sy0.start()
    pick(xn, land.at[xn], 2)
    pick(yn, land.at[yn], 3)
    sx0.wait_recv()
    sx1.wait_recv()
    pick(sxn, land.at[sxn], 4)
    sy1.wait_recv()
    sy0.wait_recv()
    pick(syn, land.at[syn], 5)

    fy.wait_recv()
    sd0 = rcopy(land.at[dg, hs(0)], land.at[dg, hs(0)], ss_s.at[5], ss_r.at[5], sib)
    sd0.start()
    fx.wait_recv()
    sd1 = rcopy(land.at[dg, hs(1)], land.at[dg, hs(1)], ss_s.at[6], ss_r.at[6], sib)
    sd1.start()
    pick(dg, land.at[dg], 6)
    sd0.wait_recv()
    sd1.wait_recv()
    pick(sdg, land.at[sdg], 7)
    for c in own_x + own_y + [own_s, fy, fx, sx0, sx1, sy0, sy1, sd0, sd1] + metas:
        c.wait_send()
    for c in outs[6:] + [ccopy, hcopy, gcopy, p2copy]:
        c.wait()
    for e in range(pre1.shape[0]):
        for c in pcopy(e):
            c.wait()


def gather_call(x, route, gates, sg, su, w1, w3, w2, nd):
    rows, d_model = x.shape
    ff = sg.shape[1]
    width = 256
    ring = 8
    any_spec = pl.BlockSpec(memory_space=pl.ANY)
    vmem = pl.BlockSpec(memory_space=pltpu.VMEM)
    dma = pltpu.SemaphoreType.DMA
    return pl.pallas_call(
        gather_kernel,
        out_shape=(
            jax.ShapeDtypeStruct((8, nd, SLOT, d_model), BF16),
            jax.ShapeDtypeStruct((rows, ff), BF16),
            jax.ShapeDtypeStruct((nd, 8, 128), jnp.int32),
            jax.ShapeDtypeStruct((nd, 3 * rows, 8 * SLOT), BF16),
            pltpu.VMEM((PRE,) + w1.shape[1:], BF16),
            pltpu.VMEM((PRE,) + w3.shape[1:], BF16),
            pltpu.VMEM(w2.shape[:2] + (EARLY * CHUNK,), BF16),
        ),
        in_specs=[any_spec] * 8,
        out_specs=(pl.BlockSpec(memory_space=pltpu.HBM),) * 4 + (vmem, vmem, vmem),
        scratch_shapes=[
            pltpu.VMEM(x.shape, BF16),
            pltpu.VMEM(route.shape, jnp.int32),
            pltpu.VMEM(gates.shape, F32),
            pltpu.VMEM((nd, rows, d_model), BF16),
            pltpu.VMEM((nd, 16, 128), F32),
            pltpu.VMEM((ring, d_model, width), BF16),
            pltpu.VMEM((ring, d_model, width), BF16),
            pltpu.VMEM((nd, 16, 128), F32),
            pltpu.VMEM((2, 8, SLOT, d_model), BF16),
            pltpu.VMEM((rows, ff), BF16),
            pltpu.VMEM((nd, 3 * rows, 8 * SLOT), BF16),
            pltpu.VMEM((nd, 8, 128), jnp.int32),
            dma((3,)), dma((2, ring)),
            dma((8,)), dma((2, PRE)), dma(()), dma(()), dma(()), dma(()),
            dma((2,)), dma((2,)), dma((2,)), dma((2,)), dma((2,)), dma((2,)),
            dma((7,)), dma((7,)), dma((7,)), dma((7,)),
        ],
        compiler_params=pltpu.CompilerParams(
            collective_id=0, has_side_effects=True, vmem_limit_bytes=29_500_000),
        name="gather_shared",
    )(x, route, gates, sg, su, w1, w3, w2)


FEW = 16


def hidden_kernel(cnt_hbm, xg_hbm, w1_hbm, w3_hbm, in1, in3, pre2, h_ref, pre1, pre3,
                  cnt, wb1, wb3, xfew, xall, csem, wsem, xsem):
    n_exp, d_model, ff = w1_hbm.shape
    nd = cnt.shape[0]
    depth = wb1.shape[0]
    first = pre1.shape[0]
    bounds = [(c, min(256, ff - c)) for c in range(0, ff, 256)]
    cut = 3 * 256
    groups = ((0, cut, bounds[:3]), (cut, ff - cut, bounds[3:]))

    def wcopy(e, late, j):
        c0, w, _ = groups[j]
        d1, d3 = (wb1, wb3) if late else (pre1, pre3)
        slot = e % depth
        sem = slot + depth if late else slot
        return (pltpu.make_async_copy(w1_hbm.at[e, :, c0:c0 + w], d1.at[slot, :, c0:c0 + w], wsem.at[sem, 0, j]),
                pltpu.make_async_copy(w3_hbm.at[e, :, c0:c0 + w], d3.at[slot, :, c0:c0 + w], wsem.at[sem, 1, j]))

    def few(e):
        top = cnt[0, e, 0]
        for d in range(1, nd):
            top = jnp.maximum(top, cnt[d, e, 0])
        return top <= FEW

    def few_copy(e):
        return pltpu.make_async_copy(xg_hbm.at[e, :, pl.ds(0, FEW)], xfew.at[e % 2], xsem.at[e % 2])

    def all_copy(e):
        return pltpu.make_async_copy(xg_hbm.at[e], xall.at[e % 2], xsem.at[e % 2])

    def rows_start(e):
        @pl.when(few(e))
        def _():
            few_copy(e).start()

        @pl.when(jnp.logical_not(few(e)))
        def _():
            all_copy(e).start()

    ccopy = pltpu.make_async_copy(cnt_hbm, cnt, csem)
    ccopy.start()
    for e in range(first, first + depth):
        for j in range(len(groups)):
            for c in wcopy(e, True, j):
                c.start()
    ccopy.wait()
    rows_start(0)
    rows_start(1)
    for e in range(n_exp):
        h_ref[e, :, FEW:SLOT, :] = jnp.zeros((nd, SLOT - FEW, h_ref.shape[3]), BF16)

    def hidden(rows_ref, up, gate, c0, w):
        m = rows_ref.shape[0] * rows_ref.shape[1]
        a = jnp.dot(rows_ref[...].reshape(m, d_model), gate[:, c0:c0 + w], preferred_element_type=F32)
        b = jnp.dot(rows_ref[...].reshape(m, d_model), up[:, c0:c0 + w], preferred_element_type=F32)
        return (jax.nn.silu(a) * b).astype(BF16).reshape(rows_ref.shape[0], rows_ref.shape[1], w)

    def down(e, slots):
        rows = h_ref[e, :, 0:slots, 0:ff].reshape(nd * slots, ff)
        for c0 in range(0, pre2.shape[2], 256):
            out = jnp.dot(rows, pre2[e, :, c0:c0 + 256], preferred_element_type=F32)
            h_ref[e, :, 0:slots, ff + c0:ff + c0 + 256] = out.astype(BF16).reshape(nd, slots, 256)

    def expert(e, gate, up, wait, refill):
        small = few(e)

        @pl.when(small)
        def _():
            few_copy(e).wait()
            for j, (_, _, cols) in enumerate(groups):
                wait(j)
                for c0, w in cols:
                    h_ref[e, :, 0:FEW, c0:c0 + w] = hidden(xfew.at[e % 2], up, gate, c0, w)
                refill(j)
            down(e, FEW)

        @pl.when(jnp.logical_not(small))
        def _():
            all_copy(e).wait()
            for j, (_, _, cols) in enumerate(groups):
                wait(j)
                for c0, w in cols:
                    h_ref[e, :, :, c0:c0 + w] = hidden(xall.at[e % 2], up, gate, c0, w)
                refill(j)
            down(e, SLOT)

        @pl.when(e + 2 < n_exp)
        def _():
            rows_start(e + 2)

    def stretch(start, late):
        def body(k, carry):
            e = start + k
            d1, d3 = (wb1, wb3) if late else (pre1, pre3)

            def wait(j):
                @pl.when(e >= first)
                def _():
                    for c in wcopy(e, late, j):
                        c.wait()

            def refill(j):
                @pl.when(e + 2 * depth < n_exp)
                def _():
                    for c in wcopy(e + 2 * depth, late, j):
                        c.start()

            expert(e, d1.at[k], d3.at[k], wait, refill)
            return carry

        lax.fori_loop(0, depth, body, 0)

    def both(i, carry):
        stretch(2 * depth * i, False)
        stretch(2 * depth * i + depth, True)
        return carry

    lax.fori_loop(0, n_exp // (2 * depth), both, 0)


def hidden_call(cnt, xg, w1, w3, pre1, pre3, pre2):
    n_exp, d_model, ff = w1.shape
    nd = cnt.shape[0]
    depth = 2
    any_spec = pl.BlockSpec(memory_space=pl.ANY)
    vmem = pl.BlockSpec(memory_space=pltpu.VMEM)
    dma = pltpu.SemaphoreType.DMA
    return pl.pallas_call(
        hidden_kernel,
        out_shape=(pltpu.VMEM((n_exp, nd, SLOT, ff + EARLY * CHUNK), BF16),
                   pltpu.VMEM(pre1.shape, BF16), pltpu.VMEM(pre3.shape, BF16)),
        input_output_aliases={4: 1, 5: 2},
        in_specs=[any_spec] * 4 + [vmem] * 3,
        out_specs=(vmem,) * 3,
        scratch_shapes=[
            pltpu.SMEM(cnt.shape, jnp.int32),
            pltpu.VMEM((depth, d_model, ff), BF16),
            pltpu.VMEM((depth, d_model, ff), BF16),
            pltpu.VMEM((2, nd, FEW, d_model), BF16),
            pltpu.VMEM((2, nd, SLOT, d_model), BF16),
            dma(()), dma((2 * depth, 2, 2)), dma((2,)),
        ],
        compiler_params=pltpu.CompilerParams(vmem_limit_bytes=29_500_000),
        name="routed_hidden",
    )(cnt, xg, w1, w3, pltpu.with_memory_space_constraint(pre1, pltpu.VMEM),
      pltpu.with_memory_space_constraint(pre3, pltpu.VMEM),
      pltpu.with_memory_space_constraint(pre2, pltpu.VMEM))[0]


def down_kernel(hv, g_hbm, hsh_hbm, w2_hbm, sd_hbm, y_hbm,
                hsh_ref, y_ref, gv, wb, sdb, ob, snd, kept, in0, in1, in2,
                isem, ysem, gsem, wsem, dsem, s0s, s0r, s1s, s1r, s2s, s2r):
    me, core, sib, xn, yn, dg = neighbours()
    n_exp, full, _ = hv.shape
    ff = w2_hbm.shape[1]
    nd = gv.shape[0]
    rows = gv.shape[1] // 3
    n_chunks = snd.shape[0]
    width = wb.shape[3]
    depth = wb.shape[0]
    hw = width // 2

    barrier = pltpu.get_barrier_semaphore()
    for dev in (sib, xn, yn):
        pl.semaphore_signal(barrier, inc=1, device_id={"ep": dev}, device_id_type=MESH)

    def wcopy(c, e):
        cols = pl.ds(pl.multiple_of(c * width, width), width)
        slot = c % depth
        return pltpu.make_async_copy(w2_hbm.at[e, :, cols], wb.at[slot, e], wsem.at[slot, e])

    def dcopy(c):
        cols = pl.ds(pl.multiple_of(c * width, width), width)
        return pltpu.make_async_copy(sd_hbm.at[:, cols], sdb.at[c], dsem.at[c])

    gcopy = pltpu.make_async_copy(g_hbm, gv, gsem)
    early = (hv.shape[2] - ff) // width
    gcopy.start()
    for e in range(n_exp):
        wcopy(early, e).start()
    scopy = pltpu.make_async_copy(hsh_hbm, hsh_ref, isem)
    scopy.start()

    own_c, xn_c, yn_c, dg_c = me // 2, xn // 2, yn // 2, dg // 2
    orders = ((own_c, yn_c, xn_c, dg_c), (own_c, xn_c, yn_c, dg_c))
    first_hop = (xn, yn)
    second_hop = (yn, xn)

    def send0(c):
        return rcopy(snd.at[c], in0.at[c], s0s.at[c], s0r.at[c], sib)

    def send1(c, q):
        return rcopy(kept.at[c, q, pl.ds(2, 2)], in1.at[c, q], s1s.at[c, q], s1r.at[c, q], first_hop[q])

    def send2(c, q):
        return rcopy(kept.at[c, q, 1], in2.at[c, q], s2s.at[c, q], s2r.at[c, q], second_hop[q])

    def step0(c):
        send0(c).wait_recv()
        kept[c] = kept[c] + in0[c]

    def step1(c):
        for q in range(2):
            send1(c, q).wait_recv()
            kept[c, q, 0:2] = kept[c, q, 0:2] + in1[c, q]

    def step2(c):
        for q in range(2):
            send2(c, q).wait_recv()
            kept[c, q, 0] = kept[c, q, 0] + in2[c, q]

    def start1(c):
        send1(c, 0).start()
        send1(c, 1).start()

    def start2(c):
        send2(c, 0).start()
        send2(c, 1).start()

    def expert(c, e):
        out = jnp.dot(hv[e, :, 0:ff], wb[c % depth, e], preferred_element_type=F32)
        out = out.astype(BF16).astype(F32)
        ob[:, e] = out.reshape(nd, SLOT, width)

    def gated(d, o):
        r = jnp.dot(gv[d], o, preferred_element_type=F32)
        return r[0:rows] + r[rows:2 * rows] + r[2 * rows:3 * rows]

    def chunk(c, carry):
        for e0 in range(0, n_exp, GROUP):
            for e in range(e0, e0 + GROUP):
                wcopy(c, e).wait()
            for e in range(e0, e0 + GROUP):
                expert(c, e)

            @pl.when(c + depth < n_chunks)
            def _():
                for e in range(e0, e0 + GROUP):
                    wcopy(c + depth, e).start()

            if e0 == 0:
                step0(c - 1)
                start1(c - 1)

                @pl.when(c == early)
                def _():
                    for i in range(early - 2):
                        step1(i)
                        start2(i)

        dcopy(c).start()
        reduce_start(c, lambda d: ob[d].reshape(n_exp * SLOT, width).astype(BF16))

        @pl.when(c >= 2)
        def _():
            step1(c - 2)
            start2(c - 2)
        return carry

    def reduce_start(c, rows_of):
        chips = (own_c, xn_c, yn_c, dg_c)
        where = ((0, 0), (2, 1), (1, 2), (3, 3))
        for chip, (p0, p1) in zip(chips, where):
            d = 2 * chip + 1 - core
            r = gated(d, rows_of(d))
            snd[c, 0, p0] = r[:, 0:hw]
            snd[c, 1, p1] = r[:, hw:width]
        for chip, (p0, p1) in zip(chips, where):
            d = 2 * chip + core
            r = gated(d, rows_of(d))
            kept[c, 0, p0] = r[:, 0:hw]
            kept[c, 1, p1] = r[:, hw:width]

        send0(c).start()

    pl.semaphore_wait(barrier, 3)
    gcopy.wait()
    for c in range(early):
        cols = slice(ff + c * width, ff + (c + 1) * width)
        reduce_start(c, lambda d: hv[:, pl.ds(pl.multiple_of(d * SLOT, SLOT), SLOT), cols].reshape(n_exp * SLOT, width))
    for c in range(early + 1, early + depth):
        for e in range(n_exp):
            wcopy(c, e).start()
    for c in range(early):
        dcopy(c).start()
    for c in range(early - 1):
        step0(c)
        start1(c)
    lax.fori_loop(early, n_chunks, chunk, 0)

    def shared(c):
        dcopy(c).wait()
        cols = pl.ds(pl.multiple_of(c * width, width), width)
        s = jnp.dot(hsh_ref[...], sdb[c], preferred_element_type=F32).astype(BF16)
        y_ref[:, cols] = s

    def shared_range(lo, hi):
        def body(c, carry):
            shared(c)
            return carry
        lax.fori_loop(lo, hi, body, 0)

    def finish_range(lo, hi):
        def body(c, carry):
            step2(c)
            for q in range(2):
                cols = pl.ds(pl.multiple_of(c * width + q * hw, hw), hw)
                y_ref[:, cols] = (y_ref[:, cols].astype(F32) + kept[c, q, 0]).astype(BF16)
            return carry
        lax.fori_loop(lo, hi, body, 0)

    last = n_chunks - 1
    scopy.wait()
    shared_range(0, 3)
    step0(last)
    start1(last)
    shared_range(3, n_chunks)
    step1(last - 1)
    start2(last - 1)
    finish_range(0, last - 1)
    cut = (last - 1) * width
    ycopies = [pltpu.make_async_copy(y_ref.at[:, a:b], y_hbm.at[:, a:b], ysem.at[i])
               for i, (a, b) in enumerate(((0, cut), (cut, n_chunks * width)))]
    ycopies[0].start()
    step1(last)
    start2(last)
    finish_range(last - 1, n_chunks)
    ycopies[1].start()

    def drain(c, carry):
        send0(c).wait_send()
        for q in range(2):
            send1(c, q).wait_send()
            send2(c, q).wait_send()
        return carry

    lax.fori_loop(0, n_chunks, drain, 0)
    for c in ycopies:
        c.wait()


def down_call(h, g, hsh, w2, sd):
    n_exp, full, _ = h.shape
    ff = w2.shape[1]
    nd, rows3, width_g = g.shape
    rows = rows3 // 3
    d_model = w2.shape[2]
    width = CHUNK
    n_chunks = d_model // width
    depth = 3
    hw = width // 2
    any_spec = pl.BlockSpec(memory_space=pl.ANY)
    vmem = pl.BlockSpec(memory_space=pltpu.VMEM)
    dma = pltpu.SemaphoreType.DMA
    return pl.pallas_call(
        down_kernel,
        out_shape=jax.ShapeDtypeStruct((rows, d_model), BF16),
        in_specs=[vmem] + [any_spec] * 4,
        out_specs=pl.BlockSpec(memory_space=pltpu.HBM),
        scratch_shapes=[
            pltpu.VMEM(hsh.shape, BF16),
            pltpu.VMEM((rows, d_model), BF16),
            pltpu.VMEM((nd, rows3, width_g), BF16),
            pltpu.VMEM((depth, n_exp, ff, width), BF16),
            pltpu.VMEM((n_chunks, sd.shape[0], width), BF16),
            pltpu.VMEM((nd, n_exp, SLOT, width), F32),
            pltpu.VMEM((n_chunks, 2, 4, rows, hw), F32),
            pltpu.VMEM((n_chunks, 2, 4, rows, hw), F32),
            pltpu.VMEM((n_chunks, 2, 4, rows, hw), F32),
            pltpu.VMEM((n_chunks, 2, 2, rows, hw), F32),
            pltpu.VMEM((n_chunks, 2, rows, hw), F32),
            dma(()), dma((2,)), dma(()), dma((depth, n_exp)), dma((n_chunks,)),
            dma((n_chunks,)), dma((n_chunks,)),
            dma((n_chunks, 2)), dma((n_chunks, 2)), dma((n_chunks, 2)), dma((n_chunks, 2)),
        ],
        compiler_params=pltpu.CompilerParams(
            collective_id=1, has_side_effects=True, vmem_limit_bytes=55_000_000),
        name="down_reduce",
    )(pltpu.with_memory_space_constraint(h, pltpu.VMEM), g, hsh, w2, sd)


def solution(mesh):
    nd = mesh.shape["ep"]

    def device_fn(x, route, gates, w_gate, w_up, w_down, sg, su, sd):
        xg, hsh, cnt, g, *pre = gather_call(x, route.T, gates.T, sg, su, w_gate, w_up, w_down, nd)
        h = hidden_call(cnt, xg, w_gate, w_up, *pre)
        return down_call(h.reshape(h.shape[0], -1, h.shape[3]), g, hsh, w_down, sd)

    tok = P(("dp", "ep"), None)
    exp = P("ep", None, None)
    rep = P(None, None)
    return jax.shard_map(device_fn, mesh=mesh, in_specs=(tok, tok, tok, exp, exp, exp, rep, rep, rep),
                         out_specs=tok, check_vma=False)
```

```python
import functools

import jax
import jax.numpy as jnp
from jax import lax
from jax.experimental import pallas as pl
from jax.experimental.pallas import tpu as pltpu
from jax.sharding import PartitionSpec as P

MESH = pl.DeviceIdType.MESH
CAP = 36
SLOT = 40
VMEM_LIMIT = 67_000_000
H_BYTES = 10_500_000
CHUNK = 256
GROUP = 8
EARLY = 1
PRE = 2
PRE_BYTES = 23_500_000
BF16 = jnp.bfloat16
F32 = jnp.float32


def neighbours():
    me = lax.axis_index("ep")
    core = me % 2
    xb = (me // 2) % 2
    yb = me // 4
    sib = me + 1 - 2 * core
    xn = me + 2 - 4 * xb
    yn = me + 4 - 8 * yb
    dg = yn + 2 - 4 * xb
    return me, core, sib, xn, yn, dg


def rcopy(src, dst, send, recv, dev):
    return pltpu.make_async_remote_copy(
        src_ref=src, dst_ref=dst, send_sem=send, recv_sem=recv,
        device_id={"ep": dev}, device_id_type=MESH)


def gather_kernel(x_hbm, route_hbm, gate_hbm, sg_hbm, su_hbm, w1_hbm, w3_hbm, w2_hbm,
                  xg_hbm, hsh_hbm, cnt_hbm, g_hbm, pre1, pre3, pre2,
                  x_ref, route_ref, gate_ref, land, meta_s, bg, bu, metal, stage, hsh, gv, cntv,
                  isem, wsem, osem, psem, p2sem, gsem, hsem, csem,
                  sx_s, sx_r, sy_s, sy_r, f_s, f_r, ss_s, ss_r, m_s, m_r):
    me, core, sib, xn, yn, dg = neighbours()
    sxn = xn + 1 - 2 * core
    syn = yn + 1 - 2 * core
    sdg = dg + 1 - 2 * core
    nd = land.shape[0]
    rows, d_model = x_ref.shape
    half = rows // 2
    ring = bg.shape[0]
    width = bg.shape[2]
    n_chunks = sg_hbm.shape[1] // width
    n_all = 8 * nd

    ins = [pltpu.make_async_copy(src, dst, isem.at[i]) for i, (src, dst) in enumerate(
        ((route_hbm, route_ref), (gate_hbm, gate_ref), (x_hbm, x_ref)))]
    for c in ins:
        c.start()
    barrier = pltpu.get_barrier_semaphore()
    for r in range(1, nd):
        pl.semaphore_signal(barrier, inc=1, device_id={"ep": (me + r) % nd}, device_id_type=MESH)

    def wcopy(i):
        cols = pl.ds(pl.multiple_of(i * width, width), width)
        slot = i % ring
        return (pltpu.make_async_copy(sg_hbm.at[:, cols], bg.at[slot], wsem.at[0, slot]),
                pltpu.make_async_copy(su_hbm.at[:, cols], bu.at[slot], wsem.at[1, slot]))

    for i in range(ring):
        for c in wcopy(i):
            c.start()

    def pcopy(e):
        return (pltpu.make_async_copy(w1_hbm.at[e], pre1.at[e], psem.at[0, e]),
                pltpu.make_async_copy(w3_hbm.at[e], pre3.at[e], psem.at[1, e]))

    def prefetch(e):
        for c in pcopy(e):
            c.start()

    ins[0].wait()
    ins[1].wait()
    ids = lax.broadcasted_iota(jnp.int32, (n_all, rows), 0)
    mask = jnp.zeros((n_all, rows), F32)
    gmap = jnp.zeros((n_all, rows), F32)
    for k in range(route_ref.shape[0]):
        eq = route_ref[k:k + 1, :] == ids
        mask = mask + jnp.where(eq, 1.0, 0.0)
        gmap = gmap + jnp.where(eq, gate_ref[k:k + 1, :], 0.0)
    before = (lax.broadcasted_iota(jnp.int32, (rows, rows), 0)
              < lax.broadcasted_iota(jnp.int32, (rows, rows), 1))
    rank = jnp.dot(mask.astype(BF16), jnp.where(before, 1.0, 0.0).astype(BF16), preferred_element_type=F32)
    rank = jnp.where(mask > 0.0, rank, -1.0)
    fill = jnp.zeros((n_all, 128 - rows), F32)
    rank = jnp.concatenate([rank, fill - 1.0], axis=1)
    gmap = jnp.concatenate([gmap, fill], axis=1)
    for j in range(nd):
        meta_s[j, 0:8, :] = rank[8 * j:8 * j + 8]
        meta_s[j, 8:16, :] = gmap[8 * j:8 * j + 8]
    metal[me] = meta_s[me]

    def hs(h):
        return pl.ds(h * half, half)

    pl.semaphore_wait(barrier, nd - 1)
    metas = []
    for r in range(1, nd):
        dst = (me + r) % nd
        c = rcopy(meta_s.at[dst], metal.at[me], m_s.at[r - 1], m_r.at[r - 1], dst)
        c.start()
        metas.append(c)
    ins[2].wait()
    own_x = [rcopy(x_ref.at[hs(h)], land.at[me, hs(h)], sx_s.at[h], sx_r.at[h], xn) for h in range(2)]
    own_y = [rcopy(x_ref.at[hs(h)], land.at[me, hs(h)], sy_s.at[h], sy_r.at[h], yn) for h in range(2)]
    own_s = rcopy(x_ref, land.at[me], ss_s.at[0], ss_r.at[0], sib)
    own_x[0].start()
    own_y[1].start()
    own_x[1].start()
    own_y[0].start()
    own_s.start()

    def shared_range(lo, hi):
        def body(i, carry):
            for c in wcopy(i):
                c.wait()
            a = jnp.dot(x_ref[...], bg[i % ring], preferred_element_type=F32)
            b = jnp.dot(x_ref[...], bu[i % ring], preferred_element_type=F32)
            cols = pl.ds(pl.multiple_of(i * width, width), width)
            hsh[:, cols] = (jax.nn.silu(a) * b).astype(BF16)

            @pl.when(i + ring < n_chunks)
            def _():
                for c in wcopy(i + ring):
                    c.start()
            return carry
        lax.fori_loop(lo, hi, body, 0)

    shared_range(0, n_chunks - 6)
    prefetch(0)

    for c in metas:
        c.wait_recv()

    for d in range(nd):
        n = jnp.sum(jnp.where(metal[d, 0:8, :] >= 0.0, 1.0, 0.0), axis=1, keepdims=True)
        cntv[d] = jnp.broadcast_to(n, (8, 128)).astype(jnp.int32)
    ccopy = pltpu.make_async_copy(cntv, cnt_hbm, csem)
    ccopy.start()

    def pick(d, x_rows, k):
        buf = k % 2
        if k >= 2:
            outs[k - 2].wait()
        slot = lax.broadcasted_iota(jnp.int32, (SLOT, rows), 0).astype(F32)
        sel = jnp.concatenate(
            [jnp.where(metal[d, e:e + 1, 0:rows] == slot, 1.0, 0.0) for e in range(8)], axis=0).astype(BF16)
        for c0 in range(0, d_model, 512):
            r = jnp.dot(sel, x_rows[:, c0:c0 + 512], preferred_element_type=F32)
            stage[buf, :, :, c0:c0 + 512] = r.astype(BF16).reshape(8, SLOT, 512)
        c = pltpu.make_async_copy(stage.at[buf], xg_hbm.at[:, d], osem.at[k])
        c.start(priority=1)
        outs.append(c)

    outs = []
    pick(me, x_ref, 0)
    own_s.wait_recv()
    pick(sib, land.at[sib], 1)

    own_x[0].wait_recv()
    fy = rcopy(land.at[xn, hs(0)], land.at[xn, hs(0)], f_s.at[0], f_r.at[0], yn)
    fy.start()
    sx0 = rcopy(land.at[xn, hs(0)], land.at[xn, hs(0)], ss_s.at[1], ss_r.at[1], sib)
    sx0.start()
    own_y[1].wait_recv()
    fx = rcopy(land.at[yn, hs(1)], land.at[yn, hs(1)], f_s.at[1], f_r.at[1], xn)
    fx.start()
    sy1 = rcopy(land.at[yn, hs(1)], land.at[yn, hs(1)], ss_s.at[2], ss_r.at[2], sib)
    sy1.start()

    shared_range(n_chunks - 6, n_chunks)
    for e in range(1, pre1.shape[0]):
        prefetch(e)
    p2copy = pltpu.make_async_copy(w2_hbm.at[:, :, pl.ds(0, pre2.shape[2])], pre2, p2sem)
    p2copy.start()
    hcopy = pltpu.make_async_copy(hsh, hsh_hbm, hsem)
    hcopy.start()

    width_g = 8 * SLOT
    lane = lax.broadcasted_iota(jnp.int32, (8, width_g), 1)
    sel = jnp.where(lane // SLOT == lax.broadcasted_iota(jnp.int32, (8, width_g), 0), 1.0, 0.0)
    slot_id = (lax.broadcasted_iota(jnp.int32, (rows, width_g), 1) % SLOT).astype(F32)

    def spread(v):
        return lax.dot_general(v, sel, (((0,), (0,)), ((), ())), preferred_element_type=F32)[:rows]

    def gate_body(d, carry):
        rk = metal[d, 0:8, :]
        gt = metal[d, 8:16, :]
        hi = gt.astype(BF16).astype(F32)
        mid = (gt - hi).astype(BF16).astype(F32)
        lo = gt - hi - mid
        eq = spread(rk) == slot_id
        for q, part in enumerate((hi, mid, lo)):
            gv[d, q * rows:(q + 1) * rows, :] = jnp.where(eq, spread(part), 0.0).astype(BF16)
        return carry

    lax.fori_loop(0, nd, gate_body, 0)
    gcopy = pltpu.make_async_copy(gv, g_hbm, gsem)
    gcopy.start()

    own_x[1].wait_recv()
    sx1 = rcopy(land.at[xn, hs(1)], land.at[xn, hs(1)], ss_s.at[3], ss_r.at[3], sib)
    sx1.start()
    own_y[0].wait_recv()
    sy0 = rcopy(land.at[yn, hs(0)], land.at[yn, hs(0)], ss_s.at[4], ss_r.at[4], sib)
    sy0.start()
    pick(xn, land.at[xn], 2)
    pick(yn, land.at[yn], 3)
    sx0.wait_recv()
    sx1.wait_recv()
    pick(sxn, land.at[sxn], 4)
    sy1.wait_recv()
    sy0.wait_recv()
    pick(syn, land.at[syn], 5)

    fy.wait_recv()
    sd0 = rcopy(land.at[dg, hs(0)], land.at[dg, hs(0)], ss_s.at[5], ss_r.at[5], sib)
    sd0.start()
    fx.wait_recv()
    sd1 = rcopy(land.at[dg, hs(1)], land.at[dg, hs(1)], ss_s.at[6], ss_r.at[6], sib)
    sd1.start()
    pick(dg, land.at[dg], 6)
    sd0.wait_recv()
    sd1.wait_recv()
    pick(sdg, land.at[sdg], 7)
    for c in own_x + own_y + [own_s, fy, fx, sx0, sx1, sy0, sy1, sd0, sd1] + metas:
        c.wait_send()
    for c in outs[6:] + [ccopy, hcopy, gcopy, p2copy]:
        c.wait()
    for e in range(pre1.shape[0]):
        for c in pcopy(e):
            c.wait()


def gather_call(x, route, gates, sg, su, w1, w3, w2, nd):
    rows, d_model = x.shape
    ff = sg.shape[1]
    width = 256
    ring = 8
    any_spec = pl.BlockSpec(memory_space=pl.ANY)
    vmem = pl.BlockSpec(memory_space=pltpu.VMEM)
    dma = pltpu.SemaphoreType.DMA
    return pl.pallas_call(
        gather_kernel,
        out_shape=(
            jax.ShapeDtypeStruct((8, nd, SLOT, d_model), BF16),
            jax.ShapeDtypeStruct((rows, ff), BF16),
            jax.ShapeDtypeStruct((nd, 8, 128), jnp.int32),
            jax.ShapeDtypeStruct((nd, 3 * rows, 8 * SLOT), BF16),
            pltpu.VMEM((PRE,) + w1.shape[1:], BF16),
            pltpu.VMEM((PRE,) + w3.shape[1:], BF16),
            pltpu.VMEM(w2.shape[:2] + (EARLY * CHUNK,), BF16),
        ),
        in_specs=[any_spec] * 8,
        out_specs=(pl.BlockSpec(memory_space=pltpu.HBM),) * 4 + (vmem, vmem, vmem),
        scratch_shapes=[
            pltpu.VMEM(x.shape, BF16),
            pltpu.VMEM(route.shape, jnp.int32),
            pltpu.VMEM(gates.shape, F32),
            pltpu.VMEM((nd, rows, d_model), BF16),
            pltpu.VMEM((nd, 16, 128), F32),
            pltpu.VMEM((ring, d_model, width), BF16),
            pltpu.VMEM((ring, d_model, width), BF16),
            pltpu.VMEM((nd, 16, 128), F32),
            pltpu.VMEM((2, 8, SLOT, d_model), BF16),
            pltpu.VMEM((rows, ff), BF16),
            pltpu.VMEM((nd, 3 * rows, 8 * SLOT), BF16),
            pltpu.VMEM((nd, 8, 128), jnp.int32),
            dma((3,)), dma((2, ring)),
            dma((8,)), dma((2, PRE)), dma(()), dma(()), dma(()), dma(()),
            dma((2,)), dma((2,)), dma((2,)), dma((2,)), dma((2,)), dma((2,)),
            dma((7,)), dma((7,)), dma((7,)), dma((7,)),
        ],
        compiler_params=pltpu.CompilerParams(
            collective_id=0, has_side_effects=True, vmem_limit_bytes=29_500_000),
        name="gather_shared",
    )(x, route, gates, sg, su, w1, w3, w2)


FEW = 16


def hidden_kernel(cnt_hbm, xg_hbm, w1_hbm, w3_hbm, in1, in3, pre2, h_ref, pre1, pre3,
                  cnt, wb1, wb3, xfew, xall, csem, wsem, xsem):
    n_exp, d_model, ff = w1_hbm.shape
    nd = cnt.shape[0]
    depth = wb1.shape[0]
    first = pre1.shape[0]
    bounds = [(c, min(256, ff - c)) for c in range(0, ff, 256)]
    cut = 3 * 256
    groups = ((0, cut, bounds[:3]), (cut, ff - cut, bounds[3:]))

    def wcopy(e, late, j):
        c0, w, _ = groups[j]
        d1, d3 = (wb1, wb3) if late else (pre1, pre3)
        slot = e % depth
        sem = slot + depth if late else slot
        return (pltpu.make_async_copy(w1_hbm.at[e, :, c0:c0 + w], d1.at[slot, :, c0:c0 + w], wsem.at[sem, 0, j]),
                pltpu.make_async_copy(w3_hbm.at[e, :, c0:c0 + w], d3.at[slot, :, c0:c0 + w], wsem.at[sem, 1, j]))

    def few(e):
        top = cnt[0, e, 0]
        for d in range(1, nd):
            top = jnp.maximum(top, cnt[d, e, 0])
        return top <= FEW

    def few_copy(e):
        return pltpu.make_async_copy(xg_hbm.at[e, :, pl.ds(0, FEW)], xfew.at[e % 2], xsem.at[e % 2])

    def all_copy(e):
        return pltpu.make_async_copy(xg_hbm.at[e], xall.at[e % 2], xsem.at[e % 2])

    def rows_start(e):
        @pl.when(few(e))
        def _():
            few_copy(e).start(priority=1)

        @pl.when(jnp.logical_not(few(e)))
        def _():
            all_copy(e).start(priority=1)

    ccopy = pltpu.make_async_copy(cnt_hbm, cnt, csem)
    ccopy.start()
    for e in range(first, first + depth):
        for j in range(len(groups)):
            for c in wcopy(e, True, j):
                c.start()
    ccopy.wait()
    rows_start(0)
    rows_start(1)
    for e in range(n_exp):
        h_ref[e, :, FEW:SLOT, :] = jnp.zeros((nd, SLOT - FEW, h_ref.shape[3]), BF16)

    def hidden(rows_ref, up, gate, c0, w):
        m = rows_ref.shape[0] * rows_ref.shape[1]
        a = jnp.dot(rows_ref[...].reshape(m, d_model), gate[:, c0:c0 + w], preferred_element_type=F32)
        b = jnp.dot(rows_ref[...].reshape(m, d_model), up[:, c0:c0 + w], preferred_element_type=F32)
        return (jax.nn.silu(a) * b).astype(BF16).reshape(rows_ref.shape[0], rows_ref.shape[1], w)

    def down(e, slots):
        rows = h_ref[e, :, 0:slots, 0:ff].reshape(nd * slots, ff)
        for c0 in range(0, pre2.shape[2], 256):
            out = jnp.dot(rows, pre2[e, :, c0:c0 + 256], preferred_element_type=F32)
            h_ref[e, :, 0:slots, ff + c0:ff + c0 + 256] = out.astype(BF16).reshape(nd, slots, 256)

    def expert(e, gate, up, wait, refill):
        small = few(e)

        @pl.when(small)
        def _():
            few_copy(e).wait()
            for j, (_, _, cols) in enumerate(groups):
                wait(j)
                for c0, w in cols:
                    h_ref[e, :, 0:FEW, c0:c0 + w] = hidden(xfew.at[e % 2], up, gate, c0, w)
                refill(j)
            down(e, FEW)

        @pl.when(jnp.logical_not(small))
        def _():
            all_copy(e).wait()
            for j, (_, _, cols) in enumerate(groups):
                wait(j)
                for c0, w in cols:
                    h_ref[e, :, :, c0:c0 + w] = hidden(xall.at[e % 2], up, gate, c0, w)
                refill(j)
            down(e, SLOT)

        @pl.when(e + 2 < n_exp)
        def _():
            rows_start(e + 2)

    def stretch(start, late):
        def body(k, carry):
            e = start + k
            d1, d3 = (wb1, wb3) if late else (pre1, pre3)

            def wait(j):
                @pl.when(e >= first)
                def _():
                    for c in wcopy(e, late, j):
                        c.wait()

            def refill(j):
                @pl.when(e + 2 * depth < n_exp)
                def _():
                    for c in wcopy(e + 2 * depth, late, j):
                        c.start()

            expert(e, d1.at[k], d3.at[k], wait, refill)
            return carry

        lax.fori_loop(0, depth, body, 0)

    def both(i, carry):
        stretch(2 * depth * i, False)
        stretch(2 * depth * i + depth, True)
        return carry

    lax.fori_loop(0, n_exp // (2 * depth), both, 0)


def hidden_call(cnt, xg, w1, w3, pre1, pre3, pre2):
    n_exp, d_model, ff = w1.shape
    nd = cnt.shape[0]
    depth = 2
    any_spec = pl.BlockSpec(memory_space=pl.ANY)
    vmem = pl.BlockSpec(memory_space=pltpu.VMEM)
    dma = pltpu.SemaphoreType.DMA
    return pl.pallas_call(
        hidden_kernel,
        out_shape=(pltpu.VMEM((n_exp, nd, SLOT, ff + EARLY * CHUNK), BF16),
                   pltpu.VMEM(pre1.shape, BF16), pltpu.VMEM(pre3.shape, BF16)),
        input_output_aliases={4: 1, 5: 2},
        in_specs=[any_spec] * 4 + [vmem] * 3,
        out_specs=(vmem,) * 3,
        scratch_shapes=[
            pltpu.SMEM(cnt.shape, jnp.int32),
            pltpu.VMEM((depth, d_model, ff), BF16),
            pltpu.VMEM((depth, d_model, ff), BF16),
            pltpu.VMEM((2, nd, FEW, d_model), BF16),
            pltpu.VMEM((2, nd, SLOT, d_model), BF16),
            dma(()), dma((2 * depth, 2, 2)), dma((2,)),
        ],
        compiler_params=pltpu.CompilerParams(vmem_limit_bytes=29_500_000),
        name="routed_hidden",
    )(cnt, xg, w1, w3, pltpu.with_memory_space_constraint(pre1, pltpu.VMEM),
      pltpu.with_memory_space_constraint(pre3, pltpu.VMEM),
      pltpu.with_memory_space_constraint(pre2, pltpu.VMEM))[0]


def down_kernel(hv, g_hbm, hsh_hbm, w2_hbm, sd_hbm, y_hbm,
                hsh_ref, y_ref, gv, wb, sdb, ob, snd, kept, in0, in1, in2,
                isem, ysem, gsem, wsem, dsem, s0s, s0r, s1s, s1r, s2s, s2r):
    me, core, sib, xn, yn, dg = neighbours()
    n_exp, full, _ = hv.shape
    ff = w2_hbm.shape[1]
    nd = gv.shape[0]
    rows = gv.shape[1] // 3
    n_chunks = snd.shape[0]
    width = wb.shape[3]
    depth = wb.shape[0]
    hw = width // 2

    barrier = pltpu.get_barrier_semaphore()
    for dev in (sib, xn, yn):
        pl.semaphore_signal(barrier, inc=1, device_id={"ep": dev}, device_id_type=MESH)

    def wcopy(c, e):
        cols = pl.ds(pl.multiple_of(c * width, width), width)
        slot = c % depth
        return pltpu.make_async_copy(w2_hbm.at[e, :, cols], wb.at[slot, e], wsem.at[slot, e])

    def dcopy(c):
        cols = pl.ds(pl.multiple_of(c * width, width), width)
        return pltpu.make_async_copy(sd_hbm.at[:, cols], sdb.at[c], dsem.at[c])

    gcopy = pltpu.make_async_copy(g_hbm, gv, gsem)
    early = (hv.shape[2] - ff) // width
    gcopy.start()
    for e in range(n_exp):
        wcopy(early, e).start()
    scopy = pltpu.make_async_copy(hsh_hbm, hsh_ref, isem)
    scopy.start()

    own_c, xn_c, yn_c, dg_c = me // 2, xn // 2, yn // 2, dg // 2
    orders = ((own_c, yn_c, xn_c, dg_c), (own_c, xn_c, yn_c, dg_c))
    first_hop = (xn, yn)
    second_hop = (yn, xn)

    def send0(c):
        return rcopy(snd.at[c], in0.at[c], s0s.at[c], s0r.at[c], sib)

    def send1(c, q):
        return rcopy(kept.at[c, q, pl.ds(2, 2)], in1.at[c, q], s1s.at[c, q], s1r.at[c, q], first_hop[q])

    def send2(c, q):
        return rcopy(kept.at[c, q, 1], in2.at[c, q], s2s.at[c, q], s2r.at[c, q], second_hop[q])

    def step0(c):
        send0(c).wait_recv()
        kept[c] = kept[c] + in0[c]

    def step1(c):
        for q in range(2):
            send1(c, q).wait_recv()
            kept[c, q, 0:2] = kept[c, q, 0:2] + in1[c, q]

    def step2(c):
        for q in range(2):
            send2(c, q).wait_recv()
            kept[c, q, 0] = kept[c, q, 0] + in2[c, q]

    def start1(c):
        send1(c, 0).start()
        send1(c, 1).start()

    def start2(c):
        send2(c, 0).start()
        send2(c, 1).start()

    def expert(c, e):
        out = jnp.dot(hv[e, :, 0:ff], wb[c % depth, e], preferred_element_type=F32)
        out = out.astype(BF16).astype(F32)
        ob[:, e] = out.reshape(nd, SLOT, width)

    def gated(d, o):
        r = jnp.dot(gv[d], o, preferred_element_type=F32)
        return r[0:rows] + r[rows:2 * rows] + r[2 * rows:3 * rows]

    def chunk(c, carry):
        for e0 in range(0, n_exp, GROUP):
            for e in range(e0, e0 + GROUP):
                wcopy(c, e).wait()
            for e in range(e0, e0 + GROUP):
                expert(c, e)

            @pl.when(c + depth < n_chunks)
            def _():
                for e in range(e0, e0 + GROUP):
                    wcopy(c + depth, e).start()

            if e0 == 0:
                step0(c - 1)
                start1(c - 1)

                @pl.when(c == early)
                def _():
                    for i in range(early - 2):
                        step1(i)
                        start2(i)

        dcopy(c).start()
        reduce_start(c, lambda d: ob[d].reshape(n_exp * SLOT, width).astype(BF16))

        @pl.when(c >= 2)
        def _():
            step1(c - 2)
            start2(c - 2)
        return carry

    def reduce_start(c, rows_of):
        chips = (own_c, xn_c, yn_c, dg_c)
        where = ((0, 0), (2, 1), (1, 2), (3, 3))
        for chip, (p0, p1) in zip(chips, where):
            d = 2 * chip + 1 - core
            r = gated(d, rows_of(d))
            snd[c, 0, p0] = r[:, 0:hw]
            snd[c, 1, p1] = r[:, hw:width]
        for chip, (p0, p1) in zip(chips, where):
            d = 2 * chip + core
            r = gated(d, rows_of(d))
            kept[c, 0, p0] = r[:, 0:hw]
            kept[c, 1, p1] = r[:, hw:width]

        send0(c).start()

    pl.semaphore_wait(barrier, 3)
    gcopy.wait()
    for c in range(early):
        cols = slice(ff + c * width, ff + (c + 1) * width)
        reduce_start(c, lambda d: hv[:, pl.ds(pl.multiple_of(d * SLOT, SLOT), SLOT), cols].reshape(n_exp * SLOT, width))
    for c in range(early + 1, early + depth):
        for e in range(n_exp):
            wcopy(c, e).start()
    for c in range(early):
        dcopy(c).start()
    for c in range(early - 1):
        step0(c)
        start1(c)
    lax.fori_loop(early, n_chunks, chunk, 0)

    def shared(c):
        dcopy(c).wait()
        cols = pl.ds(pl.multiple_of(c * width, width), width)
        s = jnp.dot(hsh_ref[...], sdb[c], preferred_element_type=F32).astype(BF16)
        y_ref[:, cols] = s

    def shared_range(lo, hi):
        def body(c, carry):
            shared(c)
            return carry
        lax.fori_loop(lo, hi, body, 0)

    def finish_range(lo, hi):
        def body(c, carry):
            step2(c)
            for q in range(2):
                cols = pl.ds(pl.multiple_of(c * width + q * hw, hw), hw)
                y_ref[:, cols] = (y_ref[:, cols].astype(F32) + kept[c, q, 0]).astype(BF16)
            return carry
        lax.fori_loop(lo, hi, body, 0)

    last = n_chunks - 1
    scopy.wait()
    shared_range(0, 3)
    step0(last)
    start1(last)
    shared_range(3, n_chunks)
    step1(last - 1)
    start2(last - 1)
    finish_range(0, last - 1)
    cut = (last - 1) * width
    ycopies = [pltpu.make_async_copy(y_ref.at[:, a:b], y_hbm.at[:, a:b], ysem.at[i])
               for i, (a, b) in enumerate(((0, cut), (cut, n_chunks * width)))]
    ycopies[0].start()
    step1(last)
    start2(last)
    finish_range(last - 1, n_chunks)
    ycopies[1].start()

    def drain(c, carry):
        send0(c).wait_send()
        for q in range(2):
            send1(c, q).wait_send()
            send2(c, q).wait_send()
        return carry

    lax.fori_loop(0, n_chunks, drain, 0)
    for c in ycopies:
        c.wait()


def down_call(h, g, hsh, w2, sd):
    n_exp, full, _ = h.shape
    ff = w2.shape[1]
    nd, rows3, width_g = g.shape
    rows = rows3 // 3
    d_model = w2.shape[2]
    width = CHUNK
    n_chunks = d_model // width
    depth = 3
    hw = width // 2
    any_spec = pl.BlockSpec(memory_space=pl.ANY)
    vmem = pl.BlockSpec(memory_space=pltpu.VMEM)
    dma = pltpu.SemaphoreType.DMA
    return pl.pallas_call(
        down_kernel,
        out_shape=jax.ShapeDtypeStruct((rows, d_model), BF16),
        in_specs=[vmem] + [any_spec] * 4,
        out_specs=pl.BlockSpec(memory_space=pltpu.HBM),
        scratch_shapes=[
            pltpu.VMEM(hsh.shape, BF16),
            pltpu.VMEM((rows, d_model), BF16),
            pltpu.VMEM((nd, rows3, width_g), BF16),
            pltpu.VMEM((depth, n_exp, ff, width), BF16),
            pltpu.VMEM((n_chunks, sd.shape[0], width), BF16),
            pltpu.VMEM((nd, n_exp, SLOT, width), F32),
            pltpu.VMEM((n_chunks, 2, 4, rows, hw), F32),
            pltpu.VMEM((n_chunks, 2, 4, rows, hw), F32),
            pltpu.VMEM((n_chunks, 2, 4, rows, hw), F32),
            pltpu.VMEM((n_chunks, 2, 2, rows, hw), F32),
            pltpu.VMEM((n_chunks, 2, rows, hw), F32),
            dma(()), dma((2,)), dma(()), dma((depth, n_exp)), dma((n_chunks,)),
            dma((n_chunks,)), dma((n_chunks,)),
            dma((n_chunks, 2)), dma((n_chunks, 2)), dma((n_chunks, 2)), dma((n_chunks, 2)),
        ],
        compiler_params=pltpu.CompilerParams(
            collective_id=1, has_side_effects=True, vmem_limit_bytes=55_000_000),
        name="down_reduce",
    )(pltpu.with_memory_space_constraint(h, pltpu.VMEM), g, hsh, w2, sd)


def solution(mesh):
    nd = mesh.shape["ep"]

    def device_fn(x, route, gates, w_gate, w_up, w_down, sg, su, sd):
        xg, hsh, cnt, g, *pre = gather_call(x, route.T, gates.T, sg, su, w_gate, w_up, w_down, nd)
        h = hidden_call(cnt, xg, w_gate, w_up, *pre)
        return down_call(h.reshape(h.shape[0], -1, h.shape[3]), g, hsh, w_down, sd)

    tok = P(("dp", "ep"), None)
    exp = P("ep", None, None)
    rep = P(None, None)
    return jax.shard_map(device_fn, mesh=mesh, in_specs=(tok, tok, tok, exp, exp, exp, rep, rep, rep),
                         out_specs=tok, check_vma=False)
```
